64 devices in a mesh: dp: 4 (over x, y), tp: 16 (over z, core).
Axes of the slice: x: 2, y: 2, z: 8, core: 2. Of those that a mesh axis runs over, the one named last changes fastest.
The devices are a block of a 4x4x8 slice.
Arguments:
- layer_in: bfloat16 [16384, 1024], P(('dp', 'tp')), parts along dimension 0
- resid_mid: bfloat16 [16384, 1024], P(('dp', 'tp')), parts along dimension 0
- grad_out: bfloat16 [16384, 1024], P(('dp', 'tp')), parts along dimension 0
- ln1_gain: float32 [1024], replicated
- ln2_gain: float32 [1024], replicated
- w_qkv: bfloat16 [1024, 3072], P(None, 'tp')
- w_out: bfloat16 [16, 64, 1024], P('tp')
- w_fc1: bfloat16 [1024, 4096], P(None, 'tp')
- w_fc2: bfloat16 [4096, 1024], P('tp')
Outputs:
- output 1: bfloat16 [16384, 1024], P(('dp', 'tp')), parts along dimension 0
- output 2: bfloat16 [4096, 3072], P('dp', 'tp'), parts along dimension 0
- output 3: bfloat16 [64, 64, 1024], P(('dp', 'tp')), parts along dimension 0
- output 4: bfloat16 [4096, 4096], P('dp', 'tp'), parts along dimension 0
- output 5: bfloat16 [16384, 1024], P(('dp', 'tp')), parts along dimension 0
There are 4 independent parts. The reference program is written for one: setup_inputs(seed, part) draws one part's arguments, and reference() takes and returns one part's arrays. A program takes and returns all parts, laid end to end along the dimension named above; an argument that names none is the same for every part.
All inputs are finite; a program needn't handle non-finite values.
Results may differ from the reference program's by a relative error of at most 0.0175564.
Values are sent between devices in bfloat16 or wider.
A program may use at most 768 MiB of HBM per device.

```python
import jax
import jax.numpy as jnp
from jax import lax

D = 1024
HEADS = 16
HEAD = 64
FF = 4096
TOKENS = 4096
LN_EPS = 1e-5
GELU_COEF = 0.044715
GELU_SCALE = 0.7978845608028654


def ln_forward(rows):
    row_mean = jnp.mean(rows, axis=-1, keepdims=True)
    centered = rows - row_mean
    row_rstd = lax.rsqrt(jnp.mean(centered * centered, axis=-1, keepdims=True) + LN_EPS)
    return centered * row_rstd, row_rstd


def ln_backward(x_hat, row_rstd, ln_gain, grad_norm):
    grad_hat = grad_norm * ln_gain
    proj_one = jnp.mean(grad_hat, axis=-1, keepdims=True)
    proj_two = jnp.mean(grad_hat * x_hat, axis=-1, keepdims=True)
    return row_rstd * (grad_hat - proj_one - x_hat * proj_two)


def gelu_pair(pre_act):
    tanh_val = jnp.tanh(GELU_SCALE * (pre_act + GELU_COEF * pre_act * pre_act * pre_act))
    gelu_val = 0.5 * pre_act * (1.0 + tanh_val)
    gelu_der = 0.5 * (1.0 + tanh_val) + 0.5 * pre_act * (1.0 - tanh_val * tanh_val) * GELU_SCALE * (1.0 + 3.0 * GELU_COEF * pre_act * pre_act)
    return gelu_val, gelu_der


def head_grads(head_args):
    qkv_head, grad_attn = head_args
    q_rows = qkv_head[0]
    k_rows = qkv_head[1]
    v_rows = qkv_head[2]
    score_scale = HEAD ** -0.5
    scores = jnp.dot(q_rows, k_rows.T, preferred_element_type=jnp.float32) * score_scale
    causal = jnp.arange(TOKENS)[:, None] >= jnp.arange(TOKENS)[None, :]
    attn_prob = jax.nn.softmax(jnp.where(causal, scores, -1e30), axis=-1)
    prob_low = attn_prob.astype(jnp.bfloat16)
    attn_out = jnp.dot(prob_low, v_rows, preferred_element_type=jnp.float32).astype(jnp.bfloat16)
    grad_v = jnp.dot(prob_low.T, grad_attn, preferred_element_type=jnp.float32).astype(jnp.bfloat16)
    grad_prob = jnp.dot(grad_attn, v_rows.T, preferred_element_type=jnp.float32)
    row_dot = jnp.sum(attn_prob * grad_prob, axis=-1, keepdims=True)
    grad_score = (attn_prob * (grad_prob - row_dot) * score_scale).astype(jnp.bfloat16)
    grad_q = jnp.dot(grad_score, k_rows, preferred_element_type=jnp.float32).astype(jnp.bfloat16)
    grad_k = jnp.dot(grad_score.T, q_rows, preferred_element_type=jnp.float32).astype(jnp.bfloat16)
    return attn_out, jnp.stack([grad_q, grad_k, grad_v])


def setup_inputs(seed: int = 0, part: int = 0) -> dict:
    part_keys = jax.random.split(jax.random.fold_in(jax.random.key(seed), part), 3)
    shared_keys = jax.random.split(jax.random.key(seed + 1), 6)
    col_kind = (jnp.arange(3 * D) // HEAD) % 3
    qk_scale = jnp.where(col_kind < 2, 1.6, 1.0)
    return {
        'layer_in': jax.random.normal(part_keys[0], (TOKENS, D), jnp.float32).astype(jnp.bfloat16),
        'resid_mid': jax.random.normal(part_keys[1], (TOKENS, D), jnp.float32).astype(jnp.bfloat16),
        'grad_out': jax.random.normal(part_keys[2], (TOKENS, D), jnp.float32).astype(jnp.bfloat16),
        'ln1_gain': 1.0 + 0.25 * jax.random.normal(shared_keys[0], (D,), jnp.float32),
        'ln2_gain': 1.0 + 0.25 * jax.random.normal(shared_keys[1], (D,), jnp.float32),
        'w_qkv': (jax.random.normal(shared_keys[2], (D, 3 * D), jnp.float32) * qk_scale * D ** -0.5).astype(jnp.bfloat16),
        'w_out': (jax.random.normal(shared_keys[3], (HEADS, HEAD, D), jnp.float32) * D ** -0.5).astype(jnp.bfloat16),
        'w_fc1': (jax.random.normal(shared_keys[4], (D, FF), jnp.float32) * D ** -0.5).astype(jnp.bfloat16),
        'w_fc2': (jax.random.normal(shared_keys[5], (FF, D), jnp.float32) * FF ** -0.5).astype(jnp.bfloat16),
    }


def reference(layer_in, resid_mid, grad_out, ln1_gain, ln2_gain, w_qkv, w_out, w_fc1, w_fc2):
    mid_hat, mid_rstd = ln_forward(resid_mid.astype(jnp.float32))
    ln2_out = (mid_hat * ln2_gain).astype(jnp.bfloat16)
    pre_act = jnp.dot(ln2_out, w_fc1, preferred_element_type=jnp.float32)
    gelu_val, gelu_der = gelu_pair(pre_act)
    act_low = gelu_val.astype(jnp.bfloat16)
    grad_wfc2 = jnp.dot(act_low.T, grad_out, preferred_element_type=jnp.float32).astype(jnp.bfloat16)
    grad_act = jnp.dot(grad_out, w_fc2.T, preferred_element_type=jnp.float32)
    grad_pre = (grad_act * gelu_der).astype(jnp.bfloat16)
    grad_wfc1 = jnp.dot(ln2_out.T, grad_pre, preferred_element_type=jnp.float32).astype(jnp.bfloat16)
    grad_norm2 = jnp.dot(grad_pre, w_fc1.T, preferred_element_type=jnp.float32)
    grad_mid = grad_out.astype(jnp.float32) + ln_backward(mid_hat, mid_rstd, ln2_gain, grad_norm2)
    grad_mid_low = grad_mid.astype(jnp.bfloat16)
    in_hat, in_rstd = ln_forward(layer_in.astype(jnp.float32))
    ln1_out = (in_hat * ln1_gain).astype(jnp.bfloat16)
    qkv_rows = jnp.dot(ln1_out, w_qkv, preferred_element_type=jnp.float32).astype(jnp.bfloat16)
    qkv_heads = qkv_rows.reshape(TOKENS, HEADS, 3, HEAD).transpose(1, 2, 0, 3)
    grad_attn = jnp.dot(grad_mid_low, w_out.reshape(D, D).T, preferred_element_type=jnp.float32).astype(jnp.bfloat16)
    grad_attn_heads = grad_attn.reshape(TOKENS, HEADS, HEAD).transpose(1, 0, 2)
    attn_heads, grad_qkv_heads = lax.map(head_grads, (qkv_heads, grad_attn_heads))
    attn_out = attn_heads.transpose(1, 0, 2).reshape(TOKENS, D)
    grad_qkv = grad_qkv_heads.transpose(2, 0, 1, 3).reshape(TOKENS, 3 * D)
    grad_wout = jnp.dot(attn_out.T, grad_mid_low, preferred_element_type=jnp.float32).astype(jnp.bfloat16).reshape(HEADS, HEAD, D)
    grad_wqkv = jnp.dot(ln1_out.T, grad_qkv, preferred_element_type=jnp.float32).astype(jnp.bfloat16)
    grad_norm1 = jnp.dot(grad_qkv, w_qkv.T, preferred_element_type=jnp.float32)
    grad_in = (grad_mid + ln_backward(in_hat, in_rstd, ln1_gain, grad_norm1)).astype(jnp.bfloat16)
    return (grad_in, grad_wqkv, grad_wout, grad_wfc1, grad_wfc2)
```

```python
import functools

import jax
import jax.numpy as jnp
from jax import lax
from jax.experimental import pallas as pl
from jax.experimental.pallas import tpu as pltpu
from jax.sharding import PartitionSpec as P

LN_EPS = 1e-5
GELU_COEF = 0.044715
GELU_SCALE = 0.7978845608028654
QB = 256
TK = 512
NEG = -1e30
F32 = jnp.float32
BF16 = jnp.bfloat16


def ln_forward(rows):
    row_mean = jnp.mean(rows, axis=-1, keepdims=True)
    centered = rows - row_mean
    row_rstd = lax.rsqrt(jnp.mean(centered * centered, axis=-1, keepdims=True) + LN_EPS)
    return centered * row_rstd, row_rstd


def ln_backward(x_hat, row_rstd, ln_gain, grad_norm):
    grad_hat = grad_norm * ln_gain
    proj_one = jnp.mean(grad_hat, axis=-1, keepdims=True)
    proj_two = jnp.mean(grad_hat * x_hat, axis=-1, keepdims=True)
    return row_rstd * (grad_hat - proj_one - x_hat * proj_two)


def gelu_pair(pre_act):
    tanh_val = jnp.tanh(GELU_SCALE * (pre_act + GELU_COEF * pre_act * pre_act * pre_act))
    gelu_val = 0.5 * pre_act * (1.0 + tanh_val)
    gelu_der = 0.5 * (1.0 + tanh_val) + 0.5 * pre_act * (1.0 - tanh_val * tanh_val) * GELU_SCALE * (1.0 + 3.0 * GELU_COEF * pre_act * pre_act)
    return gelu_val, gelu_der


def dot_nt(a, b):
    return lax.dot_general(a, b, (((1,), (1,)), ((), ())), preferred_element_type=F32)


def dot_nn(a, b):
    return lax.dot_general(a, b, (((1,), (0,)), ((), ())), preferred_element_type=F32)


def keep_mask(first_key, first_query):
    key = first_key + lax.broadcasted_iota(jnp.int32, (TK, QB), 0)
    query = first_query + lax.broadcasted_iota(jnp.int32, (TK, QB), 1)
    return key <= query


def fwd_block(i, q_ref, kv_ref, kvt_ref, ot_ref, lse_ref, head):
    rows = pl.ds(pl.multiple_of(i * QB, QB), QB)
    queries = q_ref[rows, :]

    def tile(t, carry, masked):
        top, total, acc = carry
        keys = pl.ds(pl.multiple_of(t * TK, TK), TK)
        s = dot_nt(kv_ref[keys, :], queries)
        if masked:
            s = jnp.where(keep_mask(t * TK, i * QB), s, NEG)
        new_top = jnp.maximum(top, jnp.max(s, axis=0, keepdims=True))
        p = jnp.exp(s - new_top)
        scale = jnp.exp(top - new_top)
        total = total * scale + jnp.sum(p, axis=0, keepdims=True)
        acc = acc * scale + dot_nn(kvt_ref[head:, keys], p.astype(BF16))
        return new_top, total, acc

    init = (jnp.full((1, QB), NEG, F32), jnp.zeros((1, QB), F32), jnp.zeros((head, QB), F32))
    last = lax.div(i, TK // QB)
    carry = lax.fori_loop(0, last, lambda t, c: tile(t, c, False), init)
    top, total, acc = tile(last, carry, True)
    ot_ref[:, rows] = acc / total
    lse_ref[:, rows] = top + jnp.log(total)


def bwd_block(i, q_ref, do_ref, kv_ref, kvt_ref, ot_ref, lse_ref, dq_ref, dkv_ref, head):
    rows = pl.ds(pl.multiple_of(i * QB, QB), QB)
    grads = do_ref[rows, :]
    both = jnp.concatenate([q_ref[rows, :], grads], axis=0)
    lse = lse_ref[:, rows]
    grads_t = jnp.transpose(grads.astype(F32))[head:]
    row_dot = jnp.sum(grads_t * ot_ref[:, rows], axis=0, keepdims=True)

    def tile(t, dqt, masked):
        keys = pl.ds(pl.multiple_of(t * TK, TK), TK)
        sr = dot_nt(kv_ref[keys, :], both)
        p = jnp.exp(sr[:, :QB] - lse)
        if masked:
            p = jnp.where(keep_mask(t * TK, i * QB), p, 0.0)
        ds = (p * (sr[:, QB:] - row_dot)).astype(BF16)
        dkv_ref[keys, :] += dot_nn(jnp.concatenate([ds, p.astype(BF16)], axis=1), both)
        return dqt + dot_nn(kvt_ref[:head, keys], ds)

    last = lax.div(i, TK // QB)
    dqt = lax.fori_loop(0, last, lambda t, c: tile(t, c, False), jnp.zeros((head, QB), F32))
    dqt = tile(last, dqt, True) * (head ** -0.5)
    dqt = jnp.concatenate([dqt, jnp.zeros_like(dqt)], axis=0)
    dq_ref[rows, :] = jnp.transpose(dqt).astype(BF16)


def attention_forward(q_pad, kv, kvt):
    tokens, wide = q_pad.shape
    head = wide // 2

    def kernel(q_ref, kv_ref, kvt_ref, ot_ref, lse_ref):
        def step(i, _):
            fwd_block(i, q_ref, kv_ref, kvt_ref, ot_ref, lse_ref, head)
            return 0
        lax.fori_loop(0, tokens // QB, step, 0)

    flops = 2 * tokens * tokens * wide
    return pl.pallas_call(
        kernel,
        out_shape=(jax.ShapeDtypeStruct((head, tokens), F32), jax.ShapeDtypeStruct((1, tokens), F32)),
        compiler_params=pltpu.CompilerParams(vmem_limit_bytes=48 * 1024 * 1024),
        cost_estimate=pl.CostEstimate(flops=8 * flops, bytes_accessed=4 * tokens * wide, transcendentals=tokens * tokens // 2),
    )(q_pad, kv, kvt)


def attention_backward(q_pad, do_pad, kv, kvt, out_t, lse):
    tokens, wide = q_pad.shape
    head = wide // 2

    def kernel(q_ref, do_ref, kv_ref, kvt_ref, ot_ref, lse_ref, dq_ref, dkv_ref, acc_ref):
        acc_ref[...] = jnp.zeros_like(acc_ref)

        def step(i, _):
            bwd_block(i, q_ref, do_ref, kv_ref, kvt_ref, ot_ref, lse_ref, dq_ref, acc_ref, head)
            return 0
        lax.fori_loop(0, tokens // QB, step, 0)
        dkv_ref[...] = acc_ref[...].astype(BF16)

    flops = 4 * tokens * tokens * wide
    return pl.pallas_call(
        kernel,
        out_shape=(jax.ShapeDtypeStruct((tokens, wide), BF16), jax.ShapeDtypeStruct((tokens, wide), BF16)),
        scratch_shapes=[pltpu.VMEM((tokens, wide), F32)],
        compiler_params=pltpu.CompilerParams(vmem_limit_bytes=48 * 1024 * 1024),
        cost_estimate=pl.CostEstimate(flops=8 * flops, bytes_accessed=6 * tokens * wide, transcendentals=tokens * tokens // 2),
    )(q_pad, do_pad, kv, kvt, out_t, lse)


def solution(mesh):
    row_spec = P(('dp', 'tp'), None)
    in_specs = (row_spec, row_spec, row_spec, P(None), P(None), P(None, 'tp'), P('tp', None, None), P(None, 'tp'), P('tp', None))
    out_specs = (row_spec, P('dp', 'tp'), P(('dp', 'tp'), None, None), P('dp', 'tp'), P(('dp', 'tp'), None))

    def device_step(in_rows, mid_rows, gout_rows, ln1_gain, ln2_gain, wqkv_loc, wout_loc, wfc1_loc, wfc2_loc):
        head, width = wout_loc.shape[1:]
        wqkv_pad = jnp.concatenate([wqkv_loc[:, :head], jnp.zeros_like(wqkv_loc[:, :head]), wqkv_loc[:, head:]], axis=1)
        wout_pad = jnp.concatenate([jnp.zeros_like(wout_loc[0]), wout_loc[0]], axis=0)
        mid_hat, mid_rstd = ln_forward(mid_rows.astype(F32))
        ln2_loc = (mid_hat * ln2_gain).astype(BF16)
        ln2_all = lax.all_gather(ln2_loc, 'tp', axis=0, tiled=True)
        gout_all = lax.all_gather(gout_rows, 'tp', axis=0, tiled=True)
        in_hat, in_rstd = ln_forward(in_rows.astype(F32))
        ln1_loc = (in_hat * ln1_gain).astype(BF16)
        ln1_all = lax.all_gather(ln1_loc, 'tp', axis=0, tiled=True)
        pre_act = jnp.dot(ln2_all, wfc1_loc, preferred_element_type=F32)
        gelu_val, gelu_der = gelu_pair(pre_act)
        act_low = gelu_val.astype(BF16)
        grad_wfc2 = jnp.einsum('tf,tm->fm', act_low, gout_all, preferred_element_type=F32).astype(BF16)
        grad_act = jnp.einsum('tm,fm->tf', gout_all, wfc2_loc, preferred_element_type=F32)
        grad_pre = (grad_act * gelu_der).astype(BF16)
        grad_wfc1 = jnp.einsum('tm,tf->mf', ln2_all, grad_pre, preferred_element_type=F32).astype(BF16)
        norm2_part = jnp.einsum('tf,mf->tm', grad_pre, wfc1_loc, preferred_element_type=F32).astype(BF16)
        grad_norm2 = lax.psum_scatter(norm2_part, 'tp', scatter_dimension=0, tiled=True)
        grad_mid = gout_rows.astype(F32) + ln_backward(mid_hat, mid_rstd, ln2_gain, grad_norm2.astype(F32))
        qkv_pad = jnp.dot(ln1_all, wqkv_pad, preferred_element_type=F32).astype(BF16)
        q_pad = qkv_pad[:, :2 * head] * jnp.asarray(head ** -0.5, BF16)
        kv = qkv_pad[:, 2 * head:]
        kvt = kv.T
        out_t, lse = attention_forward(q_pad, kv, kvt)
        grad_mid_all = lax.all_gather(grad_mid.astype(BF16), 'tp', axis=0, tiled=True)
        do_pad = jnp.einsum('tm,dm->td', grad_mid_all, wout_pad, preferred_element_type=F32).astype(BF16)
        dq_pad, dkv = attention_backward(q_pad, do_pad, kv, kvt, out_t, lse)
        grad_wout = jnp.dot(out_t.astype(BF16), grad_mid_all, preferred_element_type=F32).astype(BF16)[None]
        grad_qkv = jnp.concatenate([dq_pad, dkv], axis=1)
        grad_wqkv = jnp.einsum('tm,tc->mc', ln1_all, grad_qkv, preferred_element_type=F32).astype(BF16)
        grad_wqkv = jnp.concatenate([grad_wqkv[:, :head], grad_wqkv[:, 2 * head:]], axis=1)
        norm1_part = jnp.einsum('tc,mc->tm', grad_qkv, wqkv_pad, preferred_element_type=F32).astype(BF16)
        grad_norm1 = lax.psum_scatter(norm1_part, 'tp', scatter_dimension=0, tiled=True)
        grad_in = (grad_mid + ln_backward(in_hat, in_rstd, ln1_gain, grad_norm1.astype(F32))).astype(BF16)
        return grad_in, grad_wqkv, grad_wout, grad_wfc1, grad_wfc2

    return jax.shard_map(device_step, mesh=mesh, in_specs=in_specs, out_specs=out_specs, check_vma=False)
```

```python
import jax
import jax.numpy as jnp
from jax import lax
from jax.experimental import pallas as pl
from jax.experimental.pallas import tpu as pltpu
from jax.sharding import PartitionSpec as P

LN_EPS = 1e-5
GELU_COEF = 0.044715
GELU_SCALE = 0.7978845608028654
NEG = -1e30
F32 = jnp.float32
BF16 = jnp.bfloat16
MESH = pl.DeviceIdType.MESH
SIGN = (1, -1)
N2, DY, N1, EG = 0, 1, 2, 3


def ln_forward(rows):
    row_mean = jnp.mean(rows, axis=-1, keepdims=True)
    centered = rows - row_mean
    row_rstd = lax.rsqrt(jnp.mean(centered * centered, axis=-1, keepdims=True) + LN_EPS)
    return centered * row_rstd, row_rstd


def ln_backward(x_hat, row_rstd, ln_gain, grad_norm):
    grad_hat = grad_norm * ln_gain
    proj_one = jnp.mean(grad_hat, axis=-1, keepdims=True)
    proj_two = jnp.mean(grad_hat * x_hat, axis=-1, keepdims=True)
    return row_rstd * (grad_hat - proj_one - x_hat * proj_two)


def gelu_pair(pre_act):
    tanh_val = jnp.tanh(GELU_SCALE * (pre_act + GELU_COEF * pre_act * pre_act * pre_act))
    gelu_val = 0.5 * pre_act * (1.0 + tanh_val)
    gelu_der = 0.5 * (1.0 + tanh_val) + 0.5 * pre_act * (1.0 - tanh_val * tanh_val) * GELU_SCALE * (1.0 + 3.0 * GELU_COEF * pre_act * pre_act)
    return gelu_val, gelu_der


def dot_nt(a, b):
    return lax.dot_general(a, b, (((1,), (1,)), ((), ())), preferred_element_type=F32)


def dot_nn(a, b):
    return lax.dot_general(a, b, (((1,), (0,)), ((), ())), preferred_element_type=F32)


def ds_of(index, size):
    return pl.ds(pl.multiple_of(index * size, size), size)


def keep_mask(first_key, first_query, shape):
    key = first_key + lax.broadcasted_iota(jnp.int32, shape, 0)
    query = first_query + lax.broadcasted_iota(jnp.int32, shape, 1)
    return key <= query


def layer_kernel(chips, x_ref, h_ref, g_ref, gain1_ref, gain2_ref, wqkv_ref, wo_ref, w1_ref, w2_ref,
                 dx_ref, dwqkv_ref, dwo_ref, dw1_ref, dw2_ref,
                 n2_all, dy_all, n1_all, part, dbuf, rbuf, q_all, do_all, kv_all, kvt_all, ot_all, lse_all,
                 dq_all, dkv_acc, dw1t_acc, dw2_acc, dwo_acc, dwqkvt_acc, dh1,
                 ag_send, ag_recv, dd_send, dd_recv, rs_send, rs_recv, dx_send, dx_recv):
    me = lax.axis_index('tp')
    z, c = lax.div(me, 2), lax.rem(me, 2)
    half_ring = chips // 2
    last_u = 2 * half_ring
    R, width = x_ref.shape
    H = R // 2
    head = dwo_ref.shape[1]
    blocks = 2 * chips
    keys_per = 2 * R
    full = (n2_all, dy_all, n1_all, dy_all)

    def chip_at(offset):
        return lax.rem(z + offset + 2 * chips, chips)

    nbr = tuple(2 * chip_at(s) + c for s in SIGN)
    partner = 2 * z + 1 - c

    def half_rows(chip, core, h):
        return ds_of(2 * (2 * chip + core) + h, H)

    def block_rows(block):
        return ds_of(block, R)

    def ag_copy(a, d, s, h, src=None):
        dst = full[a].at[half_rows(chip_at(-SIGN[d] * (s - 1)), c, h)]
        return pltpu.make_async_remote_copy(dst if src is None else src, dst, ag_send.at[a, d, s - 1, h],
                                            ag_recv.at[a, d, s - 1, h], device_id={'tp': nbr[d]}, device_id_type=MESH)

    def ag_arrived(a, d, s, h):
        dst = full[a].at[half_rows(chip_at(-SIGN[d] * s), c, h)]
        pltpu.make_async_remote_copy(dst, dst, ag_send.at[a, d, s - 1, h],
                                     ag_recv.at[a, d, s - 1, h], device_id={'tp': nbr[d]}, device_id_type=MESH).wait_recv()

    def dd_copy(a, j, chip, core, h, src=None):
        dst = full[a].at[half_rows(chip, core, h)]
        return pltpu.make_async_remote_copy(dst if src is None else src, dst, dd_send.at[a, j, h], dd_recv.at[a, j, h],
                                            device_id={'tp': partner}, device_id_type=MESH)

    def slot_of(step, d):
        return jnp.where(step == 0, 0, jnp.minimum(2 * step - 1 + d, chips - 1))

    def chip_of_slot(j):
        away = lax.div(j + 1, 2)
        return chip_at(jnp.where(lax.rem(j, 2) == 1, -away, away))

    def dx_copy(r, j):
        chip = chip_of_slot(j)
        return pltpu.make_async_remote_copy(part.at[block_rows(2 * chip + 1 - c)], dbuf.at[chip], dx_send.at[r, j],
                                            dx_recv.at[r, j], device_id={'tp': partner}, device_id_type=MESH)

    def rs_copy(r, d, s, h):
        src = part.at[half_rows(chip_at(SIGN[d] * (half_ring - s + 1)), c, h)]
        return pltpu.make_async_remote_copy(src, rbuf.at[d, s - 1, h], rs_send.at[r, d, s - 1, h],
                                            rs_recv.at[r, d, s - 1, h], device_id={'tp': nbr[d]}, device_id_type=MESH)

    def ag_begin(a, src=None):
        for h in (0, 1):
            part_src = None if src is None else src.at[pl.ds(h * H, H)]
            for d in (0, 1):
                ag_copy(a, d, 1, h, part_src).start()
            dd_copy(a, 0, z, c, h, part_src).start()

    def ag_sent(a):
        for h in (0, 1):
            for d in (0, 1):
                for s in range(1, half_ring + 1):
                    if s < half_ring or h == d:
                        ag_copy(a, d, s, h).wait_send()
            for j in range(chips):
                dd_copy(a, j, chip_of_slot(j), c, h).wait_send()

    def ag_loop(arrays, before, compute, after):
        def body(u, carry):
            step, h = lax.div(u, 2), lax.rem(u, 2)
            s = step + 1

            @pl.when(u < last_u)
            def _():
                for a in arrays:
                    for d in (0, 1):
                        @pl.when((s < half_ring) | (h == d))
                        def _():
                            ag_arrived(a, d, s, h)

                            @pl.when((s < half_ring - 1) | ((s == half_ring - 1) & (h == d)))
                            def _():
                                ag_copy(a, d, s + 1, h).start()
                            dd_copy(a, slot_of(s, d), chip_at(-SIGN[d] * s), c, h).start()
            before(u)

            def one(sub, carry):
                chip = chip_at((2 * sub - 1) * step)
                core = jnp.where(h == 0, c, 1 - c)

                @pl.when(h == 1)
                def _():
                    for a in arrays:
                        for g in (0, 1):
                            dd_copy(a, slot_of(step, sub), chip, 1 - c, g).wait_recv()
                compute(2 * chip + core)
                return carry
            lax.fori_loop(0, jnp.where((step == 0) | (step == half_ring), 1, 2), one, 0)
            after(u)
            return carry
        lax.fori_loop(0, last_u + 2, body, 0)

    def rs_begin(r):
        for d in (0, 1):
            rs_copy(r, d, 1, d).start()
            rs_copy(r, d, 2, 1 - d).start()

    def rs_tick(r, u):
        s = 1 + lax.div(u, 2)
        odd = lax.rem(u, 2)
        for d in (0, 1):
            h = jnp.where(odd == 1, d, 1 - d)
            rs_copy(r, d, s, h).wait_recv()
            rows = half_rows(chip_at(SIGN[d] * (half_ring - s)), c, h)
            part[rows, :] = (part[rows, :].astype(F32) + rbuf[d, s - 1, h].astype(F32)).astype(BF16)
        for d in (0, 1):
            rs_copy(r, d, s + 1, jnp.where(odd == 1, d, 1 - d)).start()

    def rs_last(r, h):
        for d in (0, 1):
            rs_copy(r, d, half_ring, h).wait_recv()
        own = part[half_rows(z, c, h), :].astype(F32)
        return own + rbuf[0, half_ring - 1, h].astype(F32) + rbuf[1, half_ring - 1, h].astype(F32)

    def rs_sent(r):
        for d in (0, 1):
            for h in (0, 1):
                for s in range(1, half_ring + 1):
                    if s > 1 or h == d:
                        rs_copy(r, d, s, h).wait_send()
        for j in range(chips):
            dx_copy(r, j).wait_send()

    def join_partner(r, j):
        dx_copy(r, j).wait_recv()
        chip = chip_of_slot(j)
        rows = block_rows(2 * chip + c)
        part[rows, :] = (part[rows, :].astype(F32) + dbuf[chip].astype(F32)).astype(BF16)

    def mlp(block):
        rows = block_rows(block)
        n2, dy = n2_all[rows, :], dy_all[rows, :]
        gelu_val, gelu_der = gelu_pair(dot_nn(n2, w1_ref[...]))
        grad_pre = dot_nt(dy, w2_ref[...]) * gelu_der
        dw2_acc[...] += dot_nn(jnp.transpose(gelu_val).astype(BF16), dy)
        dw1t_acc[...] += dot_nn(jnp.transpose(grad_pre).astype(BF16), n2)
        part[rows, :] = dot_nt(grad_pre.astype(BF16), w1_ref[...]).astype(BF16)

    def qkv(block):
        rows = block_rows(block)
        cols = dot_nn(n1_all[rows, :], wqkv_ref[...])
        q_all[rows, :] = cols[:, :2 * head].astype(BF16) * jnp.asarray(head ** -0.5, BF16)
        kv_all[rows, :] = cols[:, 2 * head:].astype(BF16)
        kvt_all[:, rows] = jnp.transpose(cols[:, 2 * head:]).astype(BF16)

    def attend(i):
        rows = block_rows(i)
        queries = q_all[rows, :]

        def tile(t, carry, masked):
            top, total, acc = carry
            keys = ds_of(t, keys_per)
            s = dot_nt(kv_all[keys, :], queries)
            if masked:
                s = jnp.where(keep_mask(t * keys_per, i * R, s.shape), s, NEG)
            new_top = jnp.maximum(top, jnp.max(s, axis=0, keepdims=True))
            p = jnp.exp(s - new_top)
            scale = jnp.exp(top - new_top)
            total = total * scale + jnp.sum(p, axis=0, keepdims=True)
            acc = acc * scale + dot_nn(kvt_all[head:, keys], p.astype(BF16))
            return new_top, total, acc

        init = (jnp.full((1, R), NEG, F32), jnp.zeros((1, R), F32), jnp.zeros((head, R), F32))
        last = lax.div(i, 2)
        top, total, acc = tile(last, lax.fori_loop(0, last, lambda t, k: tile(t, k, False), init), True)
        ot_all[:, rows] = acc / total
        lse_all[:, rows] = top + jnp.log(total)

    def attend_grad(i):
        rows = block_rows(i)
        e_rows = dy_all[rows, :]
        grads_wide = dot_nt(e_rows, wo_ref[...])
        grads = grads_wide.astype(BF16)
        grads_t = jnp.transpose(grads.astype(F32))[head:]
        out_t = ot_all[:, rows]
        dwo_acc[...] += dot_nn(out_t.astype(BF16), e_rows)
        row_dot = jnp.sum(grads_t * out_t, axis=0, keepdims=True)
        both = jnp.concatenate([q_all[rows, :], grads], axis=0)
        lse = lse_all[:, rows]

        def tile(t, dqt, masked):
            keys = ds_of(t, keys_per)
            sr = dot_nt(kv_all[keys, :], both)
            p = jnp.exp(sr[:, :R] - lse)
            if masked:
                p = jnp.where(keep_mask(t * keys_per, i * R, p.shape), p, 0.0)
            ds = (p * (sr[:, R:] - row_dot)).astype(BF16)
            dkv_acc[keys, :] += dot_nn(jnp.concatenate([ds, p.astype(BF16)], axis=1), both)
            return dqt + dot_nn(kvt_all[:head, keys], ds)

        last = lax.div(i, 2)
        dqt = lax.fori_loop(0, last, lambda t, k: tile(t, k, False), jnp.zeros((head, R), F32))
        dqt = tile(last, dqt, True) * (head ** -0.5)
        dq_all[rows, :] = jnp.transpose(jnp.concatenate([dqt, jnp.zeros_like(dqt)], axis=0)).astype(BF16)

    def grad_cols(block):
        rows = block_rows(block)
        return jnp.concatenate([dq_all[rows, :], dkv_acc[rows, :].astype(BF16)], axis=1)

    def nothing(u):
        del u

    barrier = pltpu.get_barrier_semaphore()
    for peer in nbr + (partner,):
        pl.semaphore_signal(barrier, inc=1, device_id={'tp': peer}, device_id_type=MESH)
    pl.semaphore_wait(barrier, 3)
    ag_begin(DY, g_ref)

    def norm_rows(k, carry):
        piece = H // 2
        src = ds_of(k, piece)
        dst = ds_of((2 * z + c) * 4 + k, piece)
        for raw, gain, out in ((h_ref, gain2_ref, n2_all), (x_ref, gain1_ref, n1_all)):
            out[dst, :] = (ln_forward(raw[src, :].astype(F32))[0] * gain[...]).astype(BF16)
        dy_all[dst, :] = g_ref[src, :]
        return carry
    lax.fori_loop(0, 4, norm_rows, 0)
    for acc in (dw1t_acc, dw2_acc):
        acc[...] = jnp.zeros_like(acc)
    ag_begin(N2)
    for acc in (dwo_acc, dwqkvt_acc, dkv_acc):
        acc[...] = jnp.zeros_like(acc)

    def send_partner(u):
        step = lax.div(u, 2)

        @pl.when((lax.rem(u, 2) == 0) & (u > 0))
        def _():
            dx_copy(0, slot_of(step - 1, 0)).start()

            @pl.when(step > 1)
            def _():
                dx_copy(0, slot_of(step - 1, 1)).start()

    def begin_n1(u):
        @pl.when(u == last_u - 3)
        def _():
            ag_begin(N1)

    ag_loop((DY, N2), send_partner, mlp, begin_n1)

    dx_pending = slot_of(half_ring, 0)

    def join_first(u):
        @pl.when(u == 0)
        def _():
            dx_copy(0, dx_pending).start()

        @pl.when((u > 0) & (u <= chips))
        def _():
            join_partner(0, chips - u)

    def begin_rs(u):
        @pl.when(u == last_u - 2)
        def _():
            ag_sent(N2)
            ag_sent(DY)
            rs_begin(0)

    ag_loop((N1,), join_first, qkv, begin_rs)

    def forward_pair(u, carry):
        @pl.when(u <= last_u - 3)
        def _():
            rs_tick(0, u)

        def one(k, carry):
            attend(jnp.where(k == 0, blocks - u, u - 1))
            return carry
        return lax.fori_loop(0, 2, one, carry)
    lax.fori_loop(1, chips + 1, forward_pair, 0)

    for h in (0, 1):
        rows = pl.ds(h * H, H)
        mid_hat, mid_rstd = ln_forward(h_ref[rows, :].astype(F32))
        grad = g_ref[rows, :].astype(F32) + ln_backward(mid_hat, mid_rstd, gain2_ref[...], rs_last(0, h))
        dh1[rows, :] = grad
        dy_all[half_rows(z, c, h), :] = grad.astype(BF16)
    rs_sent(0)
    ag_begin(EG)

    ag_loop((EG,), nothing, attend_grad, nothing)

    def share(k, carry):
        j = chips - 1 - k
        chip = chip_of_slot(j)
        for core in (1 - c, c):
            block = 2 * chip + core
            part[block_rows(block), :] = dot_nt(grad_cols(block), wqkv_ref[...]).astype(BF16)
        dx_copy(1, j).start()

        @pl.when(k > 0)
        def _():
            join_partner(1, j + 1)

        @pl.when(k == 3)
        def _():
            rs_begin(1)
        return carry
    lax.fori_loop(0, chips, share, 0)
    join_partner(1, 0)

    def weight_block(u, carry):
        @pl.when(u <= last_u - 3)
        def _():
            rs_tick(1, u)
        block = u - 1
        cols_t = jnp.transpose(grad_cols(block).astype(F32)).astype(BF16)
        dwqkvt_acc[...] += dot_nn(cols_t, n1_all[block_rows(block), :])
        return carry
    lax.fori_loop(1, blocks + 1, weight_block, 0)

    dw2_ref[...] = dw2_acc[...].astype(BF16)
    dw1_ref[...] = jnp.transpose(dw1t_acc[...]).astype(BF16)
    dwo_ref[0] = dwo_acc[...].astype(BF16)
    dwqkv_t = jnp.concatenate([dwqkvt_acc[:head, :], dwqkvt_acc[2 * head:, :], jnp.zeros((head, width), F32)], axis=0)
    dwqkv_ref[...] = jnp.transpose(dwqkv_t)[:, :3 * head].astype(BF16)

    for h in (0, 1):
        rows = pl.ds(h * H, H)
        in_hat, in_rstd = ln_forward(x_ref[rows, :].astype(F32))
        dx_ref[rows, :] = (dh1[rows, :] + ln_backward(in_hat, in_rstd, gain1_ref[...], rs_last(1, h))).astype(BF16)
    rs_sent(1)
    ag_sent(N1)
    ag_sent(EG)


def solution(mesh):
    chips = mesh.shape['tp'] // 2
    row_spec = P(('dp', 'tp'), None)
    in_specs = (row_spec, row_spec, row_spec, P(None), P(None), P(None, 'tp'), P('tp', None, None), P(None, 'tp'), P('tp', None))
    out_specs = (row_spec, P('dp', 'tp'), P(('dp', 'tp'), None, None), P('dp', 'tp'), P(('dp', 'tp'), None))

    def device_step(in_rows, mid_rows, gout_rows, ln1_gain, ln2_gain, wqkv_loc, wout_loc, wfc1_loc, wfc2_loc):
        R, width = in_rows.shape
        head = wout_loc.shape[1]
        hidden = wfc1_loc.shape[1]
        tokens = 2 * chips * R
        half_ring = chips // 2
        wqkv_pad = jnp.concatenate([wqkv_loc[:, :head], jnp.zeros_like(wqkv_loc[:, :head]), wqkv_loc[:, head:]], axis=1)
        wout_pad = jnp.concatenate([jnp.zeros_like(wout_loc[0]), wout_loc[0]], axis=0)
        vm = pltpu.VMEM
        dma = pltpu.SemaphoreType.DMA
        scratch = [
            vm((tokens, width), BF16), vm((tokens, width), BF16), vm((tokens, width), BF16), vm((tokens, width), BF16),
            vm((chips, R, width), BF16), vm((2, half_ring, 2, R // 2, width), BF16),
            vm((tokens, 2 * head), BF16), vm((8, 128), BF16), vm((tokens, 2 * head), BF16), vm((2 * head, tokens), BF16),
            vm((head, tokens), F32), vm((1, tokens), F32),
            vm((tokens, 2 * head), BF16), vm((tokens, 2 * head), F32),
            vm((hidden, width), F32), vm((hidden, width), F32), vm((head, width), F32), vm((4 * head, width), F32), vm((R, width), F32),
            dma((4, 2, half_ring, 2)), dma((4, 2, half_ring, 2)), dma((4, chips, 2)), dma((4, chips, 2)),
            dma((2, 2, half_ring, 2)), dma((2, 2, half_ring, 2)), dma((2, chips)), dma((2, chips)),
        ]
        return pl.pallas_call(
            lambda *refs: layer_kernel(chips, *refs),
            out_shape=(
                jax.ShapeDtypeStruct((R, width), BF16), jax.ShapeDtypeStruct((width, 3 * head), BF16),
                jax.ShapeDtypeStruct((1, head, width), BF16), jax.ShapeDtypeStruct((width, hidden), BF16),
                jax.ShapeDtypeStruct((hidden, width), BF16)),
            in_specs=[pl.BlockSpec(memory_space=pltpu.VMEM)] * 9,
            out_specs=tuple([pl.BlockSpec(memory_space=pltpu.VMEM)] * 5),
            scratch_shapes=scratch,
            compiler_params=pltpu.CompilerParams(collective_id=0, has_side_effects=True, vmem_limit_bytes=67043328),
        )(in_rows, mid_rows, gout_rows, ln1_gain[None], ln2_gain[None], wqkv_pad, wout_pad, wfc1_loc, wfc2_loc)

    return jax.shard_map(device_step, mesh=mesh, in_specs=in_specs, out_specs=out_specs, check_vma=False)
```

```python
import jax
import jax.numpy as jnp
from jax import lax
from jax.experimental import pallas as pl
from jax.experimental.pallas import tpu as pltpu
from jax.sharding import PartitionSpec as P

LN_EPS = 1e-5
GELU_COEF = 0.044715
GELU_SCALE = 0.7978845608028654
NEG = -1e30
F32 = jnp.float32
BF16 = jnp.bfloat16
MESH = pl.DeviceIdType.MESH
SIGN = (1, -1)
N2, DY, N1, EG = 0, 1, 2, 3


def ln_forward(rows):
    row_mean = jnp.mean(rows, axis=-1, keepdims=True)
    centered = rows - row_mean
    row_rstd = lax.rsqrt(jnp.mean(centered * centered, axis=-1, keepdims=True) + LN_EPS)
    return centered * row_rstd, row_rstd


def ln_backward(x_hat, row_rstd, ln_gain, grad_norm):
    grad_hat = grad_norm * ln_gain
    proj_one = jnp.mean(grad_hat, axis=-1, keepdims=True)
    proj_two = jnp.mean(grad_hat * x_hat, axis=-1, keepdims=True)
    return row_rstd * (grad_hat - proj_one - x_hat * proj_two)


def gelu_pair(pre_act):
    tanh_val = jnp.tanh(GELU_SCALE * (pre_act + GELU_COEF * pre_act * pre_act * pre_act))
    gelu_val = 0.5 * pre_act * (1.0 + tanh_val)
    gelu_der = 0.5 * (1.0 + tanh_val) + 0.5 * pre_act * (1.0 - tanh_val * tanh_val) * GELU_SCALE * (1.0 + 3.0 * GELU_COEF * pre_act * pre_act)
    return gelu_val, gelu_der


def dot_nt(a, b):
    return lax.dot_general(a, b, (((1,), (1,)), ((), ())), preferred_element_type=F32)


def dot_nn(a, b):
    return lax.dot_general(a, b, (((1,), (0,)), ((), ())), preferred_element_type=F32)


def ds_of(index, size):
    return pl.ds(pl.multiple_of(index * size, size), size)


def keep_mask(shape):
    return lax.broadcasted_iota(jnp.int32, shape, 0) <= lax.broadcasted_iota(jnp.int32, shape, 1)


def layer_kernel(chips, x_ref, h_ref, g_ref, gain1_ref, gain2_ref, wqkvt_ref, wo_ref, w1_ref, w2_ref,
                 dx_ref, dwqkvt_ref, dwo_ref, dw1_ref, dw2_ref,
                 n2_all, dy_all, n1_all, part, dbuf, rbuf, q_all, wot_pad, wqkvt_pad, kv_all, kvt_all, ot_all, lse_all,
                 dq_all, dkv_acc, dw1t_acc, dw2_acc, dwo_acc, dwqkvt_acc, dh1,
                 ag_send, ag_recv, dd_send, dd_recv, rs_send, rs_recv, dx_send, dx_recv):
    me = lax.axis_index('tp')
    z, c = lax.div(me, 2), lax.rem(me, 2)
    half_ring = chips // 2
    last_u = 2 * half_ring
    R, width = x_ref.shape
    H = R // 2
    head = dwo_ref.shape[1]
    pair = 2 * R
    full = (n2_all, dy_all, n1_all, dy_all)

    def chip_at(offset):
        return lax.rem(z + offset + 2 * chips, chips)

    nbr = tuple(2 * chip_at(s) + c for s in SIGN)
    partner = 2 * z + 1 - c

    def half_rows(chip, core, h):
        return ds_of(2 * (2 * chip + core) + h, H)

    def block_rows(block):
        return ds_of(block, R)

    def ag_copy(a, d, s, h, src=None):
        dst = full[a].at[half_rows(chip_at(-SIGN[d] * (s - 1)), c, h)]
        return pltpu.make_async_remote_copy(dst if src is None else src, dst, ag_send.at[a, d, s - 1, h],
                                            ag_recv.at[a, d, s - 1, h], device_id={'tp': nbr[d]}, device_id_type=MESH)

    def ag_arrived(a, d, s, h):
        dst = full[a].at[half_rows(chip_at(-SIGN[d] * s), c, h)]
        pltpu.make_async_remote_copy(dst, dst, ag_send.at[a, d, s - 1, h],
                                     ag_recv.at[a, d, s - 1, h], device_id={'tp': nbr[d]}, device_id_type=MESH).wait_recv()

    def dd_copy(a, j, chip, core, h, src=None):
        dst = full[a].at[half_rows(chip, core, h)]
        return pltpu.make_async_remote_copy(dst if src is None else src, dst, dd_send.at[a, j, h], dd_recv.at[a, j, h],
                                            device_id={'tp': partner}, device_id_type=MESH)

    def slot_of(step, d):
        return jnp.where(step == 0, 0, jnp.minimum(2 * step - 1 + d, chips - 1))

    def chip_of_slot(j):
        away = lax.div(j + 1, 2)
        return chip_at(jnp.where(lax.rem(j, 2) == 1, -away, away))

    def dx_copy(r, j):
        chip = chip_of_slot(j)
        return pltpu.make_async_remote_copy(part.at[block_rows(2 * chip + 1 - c)], dbuf.at[chip], dx_send.at[r, j],
                                            dx_recv.at[r, j], device_id={'tp': partner}, device_id_type=MESH)

    def rs_copy(r, d, s, h):
        src = part.at[half_rows(chip_at(SIGN[d] * (half_ring - s + 1)), c, h)]
        return pltpu.make_async_remote_copy(src, rbuf.at[d, s - 1, h], rs_send.at[r, d, s - 1, h],
                                            rs_recv.at[r, d, s - 1, h], device_id={'tp': nbr[d]}, device_id_type=MESH)

    def ag_begin(a, src=None):
        for h in (0, 1):
            part_src = None if src is None else src.at[pl.ds(h * H, H)]
            for d in (0, 1):
                ag_copy(a, d, 1, h, part_src).start()
            dd_copy(a, 0, z, c, h, part_src).start()

    def ag_sent(a):
        for h in (0, 1):
            for d in (0, 1):
                for s in range(1, half_ring + 1):
                    if s < half_ring or h == d:
                        ag_copy(a, d, s, h).wait_send()
            for j in range(chips):
                dd_copy(a, j, chip_of_slot(j), c, h).wait_send()

    def ag_loop(arrays, before, compute, after):
        def body(u, carry):
            step, h = lax.div(u, 2), lax.rem(u, 2)
            s = step + 1

            @pl.when(u < last_u)
            def _():
                for a in arrays:
                    for d in (0, 1):
                        @pl.when((s < half_ring) | (h == d))
                        def _():
                            ag_arrived(a, d, s, h)

                            @pl.when((s < half_ring - 1) | ((s == half_ring - 1) & (h == d)))
                            def _():
                                ag_copy(a, d, s + 1, h).start()
                            dd_copy(a, slot_of(s, d), chip_at(-SIGN[d] * s), c, h).start()
            before(u)

            @pl.when((h == 0) | ((step > 0) & (step < half_ring)))
            def _():
                chip = chip_at((2 * h - 1) * step)
                for a in arrays:
                    for g in (0, 1):
                        dd_copy(a, slot_of(step, h), chip, 1 - c, g).wait_recv()
                compute(chip)
            after(u)
            return carry
        lax.fori_loop(0, last_u + 1, body, 0)

    def rs_begin(r):
        for d in (0, 1):
            rs_copy(r, d, 1, d).start()
            rs_copy(r, d, 2, 1 - d).start()

    def rs_tick(r, u):
        s = 1 + lax.div(u, 2)
        odd = lax.rem(u, 2)
        for d in (0, 1):
            h = jnp.where(odd == 1, d, 1 - d)
            rs_copy(r, d, s, h).wait_recv()
            rows = half_rows(chip_at(SIGN[d] * (half_ring - s)), c, h)
            part[rows, :] = (part[rows, :].astype(F32) + rbuf[d, s - 1, h].astype(F32)).astype(BF16)
        for d in (0, 1):
            rs_copy(r, d, s + 1, jnp.where(odd == 1, d, 1 - d)).start()

    def rs_last(r, h):
        for d in (0, 1):
            rs_copy(r, d, half_ring, h).wait_recv()
        own = part[half_rows(z, c, h), :].astype(F32)
        return own + rbuf[0, half_ring - 1, h].astype(F32) + rbuf[1, half_ring - 1, h].astype(F32)

    def rs_sent(r):
        for d in (0, 1):
            for h in (0, 1):
                for s in range(1, half_ring + 1):
                    if s > 1 or h == d:
                        rs_copy(r, d, s, h).wait_send()
        for j in range(chips):
            dx_copy(r, j).wait_send()

    def join_partner(r, j):
        dx_copy(r, j).wait_recv()
        chip = chip_of_slot(j)
        rows = block_rows(2 * chip + c)
        part[rows, :] = (part[rows, :].astype(F32) + dbuf[chip].astype(F32)).astype(BF16)

    def mlp(chip):
        rows = ds_of(chip, pair)
        n2, dy = n2_all[rows, :], dy_all[rows, :]
        gelu_val, gelu_der = gelu_pair(dot_nn(n2, w1_ref[...]))
        grad_pre = dot_nt(dy, w2_ref[...]) * gelu_der
        dw2_acc[...] += dot_nn(jnp.transpose(gelu_val).astype(BF16), dy)
        dw1t_acc[...] += dot_nn(jnp.transpose(grad_pre).astype(BF16), n2)
        part[rows, :] = dot_nt(grad_pre.astype(BF16), w1_ref[...]).astype(BF16)

    def qkv(chip):
        rows = ds_of(chip, pair)
        cols = dot_nt(n1_all[rows, :], wqkvt_pad[...])
        q_all[rows, :] = cols[:, :2 * head].astype(BF16) * jnp.asarray(head ** -0.5, BF16)
        kv_all[rows, :] = cols[:, 2 * head:].astype(BF16)
        kvt_all[:, rows] = jnp.transpose(cols[:, 2 * head:]).astype(BF16)

    def attend(m):
        rows = ds_of(m, pair)
        queries = q_all[rows, :]

        def tile(t, carry, masked):
            top, total, acc = carry
            keys = ds_of(t, pair)
            s = dot_nt(kv_all[keys, :], queries)
            if masked:
                s = jnp.where(keep_mask(s.shape), s, NEG)
            new_top = jnp.maximum(top, jnp.max(s, axis=0, keepdims=True))
            p = jnp.exp(s - new_top)
            scale = jnp.exp(top - new_top)
            total = total * scale + jnp.sum(p, axis=0, keepdims=True)
            acc = acc * scale + dot_nn(kvt_all[head:, keys], p.astype(BF16))
            return new_top, total, acc

        init = (jnp.full((1, pair), NEG, F32), jnp.zeros((1, pair), F32), jnp.zeros((head, pair), F32))
        top, total, acc = tile(m, lax.fori_loop(0, m, lambda t, k: tile(t, k, False), init), True)
        ot_all[:, rows] = acc / total
        lse_all[:, rows] = top + jnp.log(total)

    def attend_grad(m):
        rows = ds_of(m, pair)
        e_rows = dy_all[rows, :]
        grads = dot_nt(e_rows, wot_pad[...]).astype(BF16)
        grads_t = jnp.transpose(grads.astype(F32))[head:]
        out_t = ot_all[:, rows]
        dwo_acc[...] += dot_nn(out_t.astype(BF16), e_rows)
        row_dot = jnp.sum(grads_t * out_t, axis=0, keepdims=True)
        both = jnp.concatenate([q_all[rows, :], grads], axis=0)
        lse = lse_all[:, rows]

        def tile(t, dqt, masked):
            keys = ds_of(t, pair)
            sr = dot_nt(kv_all[keys, :], both)
            p = jnp.exp(sr[:, :pair] - lse)
            if masked:
                p = jnp.where(keep_mask(p.shape), p, 0.0)
            ds = (p * (sr[:, pair:] - row_dot)).astype(BF16)
            dkv_acc[keys, :] += dot_nn(jnp.concatenate([ds, p.astype(BF16)], axis=1), both)
            return dqt + dot_nn(kvt_all[:head, keys], ds)

        dqt = lax.fori_loop(0, m, lambda t, k: tile(t, k, False), jnp.zeros((head, pair), F32))
        dqt = tile(m, dqt, True) * (head ** -0.5)
        dq_all[rows, :] = jnp.transpose(jnp.concatenate([dqt, jnp.zeros_like(dqt)], axis=0)).astype(BF16)

    def grad_cols(rows):
        return jnp.concatenate([dq_all[rows, :], dkv_acc[rows, :].astype(BF16)], axis=1)

    def nothing(u):
        del u

    barrier = pltpu.get_barrier_semaphore()
    for peer in nbr + (partner,):
        pl.semaphore_signal(barrier, inc=1, device_id={'tp': peer}, device_id_type=MESH)
    pl.semaphore_wait(barrier, 3)
    ag_begin(DY, g_ref)

    def norm_rows(k, carry):
        piece = H // 2
        src = ds_of(k, piece)
        dst = ds_of((2 * z + c) * 4 + k, piece)
        for raw, gain, out in ((h_ref, gain2_ref, n2_all), (x_ref, gain1_ref, n1_all)):
            out[dst, :] = (ln_forward(raw[src, :].astype(F32))[0] * gain[...]).astype(BF16)
        dy_all[dst, :] = g_ref[src, :]
        return carry
    lax.fori_loop(0, 4, norm_rows, 0)
    for acc in (dw1t_acc, dw2_acc):
        acc[...] = jnp.zeros_like(acc)
    ag_begin(N2)
    wot_pad[:head, :] = jnp.zeros((head, width), BF16)
    wot_pad[head:, :] = wo_ref[0]
    wqkvt_pad[:head, :] = wqkvt_ref[:head, :]
    wqkvt_pad[head:2 * head, :] = jnp.zeros((head, width), BF16)
    wqkvt_pad[2 * head:, :] = wqkvt_ref[head:, :]
    for acc in (dwo_acc, dwqkvt_acc, dkv_acc):
        acc[...] = jnp.zeros_like(acc)

    def send_partner(u):
        step, sub = lax.div(u - 1, 2), lax.rem(u - 1, 2)

        @pl.when((u > 0) & ((sub == 0) | (step > 0)))
        def _():
            dx_copy(0, slot_of(step, sub)).start()

    def begin_n1(u):
        @pl.when(u == last_u - 3)
        def _():
            ag_begin(N1)

    ag_loop((DY, N2), send_partner, mlp, begin_n1)

    dx_pending = slot_of(half_ring, 0)

    def join_first(u):
        @pl.when(u == 0)
        def _():
            dx_copy(0, dx_pending).start()

        @pl.when((u > 0) & (u <= chips))
        def _():
            join_partner(0, chips - u)

    def begin_rs(u):
        @pl.when(u == last_u - 3)
        def _():
            ag_sent(N2)
            ag_sent(DY)
            rs_begin(0)

    ag_loop((N1,), join_first, qkv, begin_rs)

    def forward_chip(u, carry):
        @pl.when(u <= last_u - 3)
        def _():
            rs_tick(0, u)

        attend(chips - u)
        return carry
    lax.fori_loop(1, chips + 1, forward_chip, 0)

    for h in (0, 1):
        rows = pl.ds(h * H, H)
        mid_hat, mid_rstd = ln_forward(h_ref[rows, :].astype(F32))
        grad = g_ref[rows, :].astype(F32) + ln_backward(mid_hat, mid_rstd, gain2_ref[...], rs_last(0, h))
        dh1[rows, :] = grad
        dy_all[half_rows(z, c, h), :] = grad.astype(BF16)
    rs_sent(0)
    ag_begin(EG)

    ag_loop((EG,), nothing, attend_grad, nothing)

    def share(k, carry):
        j = chips - 1 - k
        chip = chip_of_slot(j)
        for core in (1 - c, c):
            rows = block_rows(2 * chip + core)
            part[rows, :] = dot_nn(grad_cols(rows), wqkvt_pad[...]).astype(BF16)
        dx_copy(1, j).start()

        @pl.when(k > 0)
        def _():
            join_partner(1, j + 1)

        for first in (1, 2):
            @pl.when(k == 2 * first - 1)
            def _():
                for d in (0, 1):
                    rs_copy(1, d, first, d if first == 1 else 1 - d).start()
        return carry
    lax.fori_loop(0, chips, share, 0)
    join_partner(1, 0)

    def weight_block(u, carry):
        @pl.when(u <= last_u - 3)
        def _():
            rs_tick(1, u)
        rows = ds_of(u - 1, pair)
        cols_t = jnp.transpose(grad_cols(rows).astype(F32)).astype(BF16)
        dwqkvt_acc[...] += dot_nn(cols_t, n1_all[rows, :])
        return carry
    lax.fori_loop(1, chips + 1, weight_block, 0)

    dw2_ref[...] = dw2_acc[...].astype(BF16)
    dw1_ref[...] = jnp.transpose(dw1t_acc[...]).astype(BF16)
    dwo_ref[0] = dwo_acc[...].astype(BF16)
    dwqkvt_ref[:head, :] = dwqkvt_acc[:head, :].astype(BF16)
    dwqkvt_ref[head:, :] = dwqkvt_acc[2 * head:, :].astype(BF16)

    for h in (0, 1):
        rows = pl.ds(h * H, H)
        in_hat, in_rstd = ln_forward(x_ref[rows, :].astype(F32))
        dx_ref[rows, :] = (dh1[rows, :] + ln_backward(in_hat, in_rstd, gain1_ref[...], rs_last(1, h))).astype(BF16)
    rs_sent(1)
    ag_sent(N1)
    ag_sent(EG)


def hand_over(arrays):
    count = len(arrays)

    def kernel(*refs):
        ins, outs, held, sems = refs[:count], refs[count:2 * count], refs[2 * count:3 * count], refs[3 * count]
        reads = [pltpu.make_async_copy(ins[k], held[k], sems.at[0, k]) for k in range(count)]
        writes = [pltpu.make_async_copy(held[k], outs[k], sems.at[1, k]) for k in range(count)]
        for read in reads:
            read.start()
        for read, write in zip(reads, writes):
            read.wait()
            write.start()
        for write in writes:
            write.wait()

    return pl.pallas_call(
        kernel,
        out_shape=tuple(jax.ShapeDtypeStruct(a.shape, a.dtype) for a in arrays),
        in_specs=[pl.BlockSpec(memory_space=pl.ANY)] * count,
        out_specs=tuple([pl.BlockSpec(memory_space=pl.ANY)] * count),
        scratch_shapes=[pltpu.VMEM(a.shape, a.dtype) for a in arrays] + [pltpu.SemaphoreType.DMA((2, count))],
    )(*arrays)


def solution(mesh):
    chips = mesh.shape['tp'] // 2
    row_spec = P(('dp', 'tp'), None)
    in_specs = (row_spec, row_spec, row_spec, P(None), P(None), P(None, 'tp'), P('tp', None, None), P(None, 'tp'), P('tp', None))
    out_specs = (row_spec, P('dp', 'tp'), P(('dp', 'tp'), None, None), P('dp', 'tp'), P(('dp', 'tp'), None))

    def device_step(in_rows, mid_rows, gout_rows, ln1_gain, ln2_gain, wqkv_loc, wout_loc, wfc1_loc, wfc2_loc):
        R, width = in_rows.shape
        head = wout_loc.shape[1]
        hidden = wfc1_loc.shape[1]
        tokens = 2 * chips * R
        half_ring = chips // 2
        vm = pltpu.VMEM
        dma = pltpu.SemaphoreType.DMA
        scratch = [
            vm((tokens, width), BF16), vm((tokens, width), BF16), vm((tokens, width), BF16), vm((tokens, width), BF16),
            vm((chips, R, width), BF16), vm((2, half_ring, 2, R // 2, width), BF16),
            vm((tokens, 2 * head), BF16), vm((2 * head, width), BF16), vm((4 * head, width), BF16), vm((tokens, 2 * head), BF16), vm((2 * head, tokens), BF16),
            vm((head, tokens), F32), vm((1, tokens), F32),
            vm((tokens, 2 * head), BF16), vm((tokens, 2 * head), F32),
            vm((hidden, width), F32), vm((hidden, width), F32), vm((head, width), F32), vm((4 * head, width), F32), vm((R, width), F32),
            dma((4, 2, half_ring, 2)), dma((4, 2, half_ring, 2)), dma((4, chips, 2)), dma((4, chips, 2)),
            dma((2, 2, half_ring, 2)), dma((2, 2, half_ring, 2)), dma((2, chips)), dma((2, chips)),
        ]
        grads = pl.pallas_call(
            lambda *refs: layer_kernel(chips, *refs),
            out_shape=(
                jax.ShapeDtypeStruct((R, width), BF16), jax.ShapeDtypeStruct((3 * head, width), BF16),
                jax.ShapeDtypeStruct((1, head, width), BF16), jax.ShapeDtypeStruct((width, hidden), BF16),
                jax.ShapeDtypeStruct((hidden, width), BF16)),
            in_specs=[pl.BlockSpec(memory_space=pltpu.VMEM)] * 9,
            out_specs=tuple([pl.BlockSpec(memory_space=pltpu.VMEM)] * 5),
            scratch_shapes=scratch,
            compiler_params=pltpu.CompilerParams(collective_id=0, has_side_effects=True, vmem_limit_bytes=67043328),
        )(in_rows, mid_rows, gout_rows, ln1_gain[None], ln2_gain[None], wqkv_loc.T, wout_loc, wfc1_loc, wfc2_loc)
        grad_in, grad_wqkvt, grad_wout, grad_wfc1, grad_wfc2 = hand_over(grads)
        return grad_in, grad_wqkvt.T, grad_wout, grad_wfc1, grad_wfc2

    return jax.shard_map(device_step, mesh=mesh, in_specs=in_specs, out_specs=out_specs, check_vma=False)
```

```python
import jax
import jax.numpy as jnp
from jax import lax
from jax.experimental import pallas as pl
from jax.experimental.pallas import tpu as pltpu
from jax.sharding import PartitionSpec as P

LN_EPS = 1e-5
GELU_COEF = 0.044715
GELU_SCALE = 0.7978845608028654
NEG = -1e30
F32 = jnp.float32
BF16 = jnp.bfloat16
MESH = pl.DeviceIdType.MESH
SIGN = (1, -1)
N2, DY, N1, EG = 0, 1, 2, 3


def ln_forward(rows):
    row_mean = jnp.mean(rows, axis=-1, keepdims=True)
    centered = rows - row_mean
    row_rstd = lax.rsqrt(jnp.mean(centered * centered, axis=-1, keepdims=True) + LN_EPS)
    return centered * row_rstd, row_rstd


def ln_backward(x_hat, row_rstd, ln_gain, grad_norm):
    grad_hat = grad_norm * ln_gain
    proj_one = jnp.mean(grad_hat, axis=-1, keepdims=True)
    proj_two = jnp.mean(grad_hat * x_hat, axis=-1, keepdims=True)
    return row_rstd * (grad_hat - proj_one - x_hat * proj_two)


def gelu_pair(pre_act):
    tanh_val = jnp.tanh(GELU_SCALE * (pre_act + GELU_COEF * pre_act * pre_act * pre_act))
    gelu_val = 0.5 * pre_act * (1.0 + tanh_val)
    gelu_der = 0.5 * (1.0 + tanh_val) + 0.5 * pre_act * (1.0 - tanh_val * tanh_val) * GELU_SCALE * (1.0 + 3.0 * GELU_COEF * pre_act * pre_act)
    return gelu_val, gelu_der


def dot_nt(a, b):
    return lax.dot_general(a, b, (((1,), (1,)), ((), ())), preferred_element_type=F32)


def dot_nn(a, b):
    return lax.dot_general(a, b, (((1,), (0,)), ((), ())), preferred_element_type=F32)


def ds_of(index, size):
    return pl.ds(pl.multiple_of(index * size, size), size)


def keep_mask(shape):
    return lax.broadcasted_iota(jnp.int32, shape, 0) <= lax.broadcasted_iota(jnp.int32, shape, 1)


def layer_kernel(chips, x_ref, h_ref, g_ref, gain1_ref, gain2_ref, wqkvt_ref, wo_ref, w1_ref, w2_ref,
                 dx_ref, dwqkvt_ref, dwo_ref, dw1_ref, dw2_ref,
                 n2_all, dy_all, n1_all, part, dbuf, rbuf, q_all, wot_pad, wqkvt_pad, kv_all, kvt_all, ot_all, lse_all,
                 dq_all, dkv_acc, dw1t_acc, dw2_acc, dwo_acc, dwqkvt_acc, dh1,
                 ag_send, ag_recv, dd_send, dd_recv, rs_send, rs_recv, dx_send, dx_recv):
    me = lax.axis_index('tp')
    z, c = lax.div(me, 2), lax.rem(me, 2)
    half_ring = chips // 2
    last_u = 2 * half_ring
    R, width = x_ref.shape
    H = R // 2
    piece = R // 4
    head = dwo_ref.shape[1]
    pair = 2 * R
    full = (n2_all, dy_all, n1_all, dy_all)

    def chip_at(offset):
        return lax.rem(z + offset + 2 * chips, chips)

    nbr = tuple(2 * chip_at(s) + c for s in SIGN)
    partner = 2 * z + 1 - c

    def half_rows(chip, core, h):
        return ds_of(2 * (2 * chip + core) + h, H)

    def piece_rows(chip, core, q):
        return ds_of(4 * (2 * chip + core) + q, piece)

    def block_rows(block):
        return ds_of(block, R)

    def ag_copy(a, d, s, h, src=None):
        dst = full[a].at[half_rows(chip_at(-SIGN[d] * (s - 1)), c, h)]
        return pltpu.make_async_remote_copy(dst if src is None else src, dst, ag_send.at[a, d, s - 1, h],
                                            ag_recv.at[a, d, s - 1, h], device_id={'tp': nbr[d]}, device_id_type=MESH)

    def ag_arrived(a, d, s, h):
        dst = full[a].at[half_rows(chip_at(-SIGN[d] * s), c, h)]
        pltpu.make_async_remote_copy(dst, dst, ag_send.at[a, d, s - 1, h],
                                     ag_recv.at[a, d, s - 1, h], device_id={'tp': nbr[d]}, device_id_type=MESH).wait_recv()

    def dd_copy(a, j, chip, core, h, src=None):
        dst = full[a].at[half_rows(chip, core, h)]
        return pltpu.make_async_remote_copy(dst if src is None else src, dst, dd_send.at[a, j, h], dd_recv.at[a, j, h],
                                            device_id={'tp': partner}, device_id_type=MESH)

    def slot_of(step, d):
        return jnp.where(step == 0, 0, jnp.minimum(2 * step - 1 + d, chips - 1))

    def chip_of_slot(j):
        away = lax.div(j + 1, 2)
        return chip_at(jnp.where(lax.rem(j, 2) == 1, -away, away))

    def dx_copy(r, j):
        chip = chip_of_slot(j)
        return pltpu.make_async_remote_copy(part.at[block_rows(2 * chip + 1 - c)], dbuf.at[chip], dx_send.at[r, j],
                                            dx_recv.at[r, j], device_id={'tp': partner}, device_id_type=MESH)

    def rs_copy(r, d, s, h):
        src = part.at[piece_rows(chip_at(SIGN[d] * (half_ring - s + 1)), c, h)]
        return pltpu.make_async_remote_copy(src, rbuf.at[d, s - 1, h], rs_send.at[r, d, s - 1, h],
                                            rs_recv.at[r, d, s - 1, h], device_id={'tp': nbr[d]}, device_id_type=MESH)

    def ag_begin(a, src=None, halves=(0, 1)):
        for h in halves:
            part_src = None if src is None else src.at[pl.ds(h * H, H)]
            for d in (0, 1):
                ag_copy(a, d, 1, h, part_src).start()
            dd_copy(a, 0, z, c, h, part_src).start()

    def ag_sent(a):
        for h in (0, 1):
            for d in (0, 1):
                for s in range(1, half_ring + 1):
                    if s < half_ring or h == d:
                        ag_copy(a, d, s, h).wait_send()
            for j in range(chips):
                dd_copy(a, j, chip_of_slot(j), c, h).wait_send()

    def ag_loop(arrays, before, compute, after):
        def body(u, carry):
            step, h = lax.div(u, 2), lax.rem(u, 2)
            s = step + 1

            @pl.when(u < last_u)
            def _():
                for a in arrays:
                    for d in (0, 1):
                        @pl.when((s < half_ring) | (h == d))
                        def _():
                            ag_arrived(a, d, s, h)

                            @pl.when((s < half_ring - 1) | ((s == half_ring - 1) & (h == d)))
                            def _():
                                ag_copy(a, d, s + 1, h).start()
                            dd_copy(a, slot_of(s, d), chip_at(-SIGN[d] * s), c, h).start()
            before(u)

            @pl.when((h == 0) | ((step > 0) & (step < half_ring)))
            def _():
                chip = chip_at((2 * h - 1) * step)
                for a in arrays:
                    for g in (0, 1):
                        dd_copy(a, slot_of(step, h), chip, 1 - c, g).wait_recv()
                compute(chip)
            after(u)
            return carry
        lax.fori_loop(0, last_u + 1, body, 0)

    def rs_first(r, s):
        for d in (0, 1):
            for q in (0, 1):
                rs_copy(r, d, s, (2 * d + q + 2 * (s - 1)) % 4).start()

    def rs_tick(r, k):
        s = 2 + lax.div(k + 2, 4)
        place = lax.rem(k + 2, 4)
        swapped = lax.rem(place + 2, 4)
        rising = jnp.where(place == 3, 3, lax.rem(place + 2, 3))
        order = (jnp.where(s == half_ring, place, jnp.where(s == half_ring - 1, rising, swapped)), place)
        for d in (0, 1):
            q = order[d]
            rs_copy(r, d, s - 1, q).wait_recv()
            rows = piece_rows(chip_at(SIGN[d] * (half_ring - s + 1)), c, q)
            part[rows, :] = (part[rows, :].astype(F32) + rbuf[d, s - 2, q].astype(F32)).astype(BF16)
        for d in (0, 1):
            rs_copy(r, d, s, order[d]).start()

    def rs_ticks(r, u):
        @pl.when(u <= last_u - 3)
        def _():
            rs_tick(r, 2 * u - 2)
            rs_tick(r, 2 * u - 1)

    def rs_last(r, q):
        for d in (0, 1):
            rs_copy(r, d, half_ring, q).wait_recv()
        own = part[piece_rows(z, c, q), :].astype(F32)
        return own + rbuf[0, half_ring - 1, q].astype(F32) + rbuf[1, half_ring - 1, q].astype(F32)

    def rs_sent(r):
        for d in (0, 1):
            for q in range(4):
                for s in range(1, half_ring + 1):
                    if s > 1 or q // 2 == d:
                        rs_copy(r, d, s, q).wait_send()
        for j in range(chips):
            dx_copy(r, j).wait_send()

    def join_partner(r, j):
        dx_copy(r, j).wait_recv()
        chip = chip_of_slot(j)
        rows = block_rows(2 * chip + c)
        part[rows, :] = (part[rows, :].astype(F32) + dbuf[chip].astype(F32)).astype(BF16)

    def mlp(chip):
        rows = ds_of(chip, pair)
        n2, dy = n2_all[rows, :], dy_all[rows, :]
        gelu_val, gelu_der = gelu_pair(dot_nn(n2, w1_ref[...]))
        grad_pre = dot_nt(dy, w2_ref[...]) * gelu_der
        dw2_acc[...] += dot_nn(jnp.transpose(gelu_val).astype(BF16), dy)
        dw1t_acc[...] += dot_nn(jnp.transpose(grad_pre).astype(BF16), n2)
        part[rows, :] = dot_nt(grad_pre.astype(BF16), w1_ref[...]).astype(BF16)

    def qkv(chip):
        rows = ds_of(chip, pair)
        cols = dot_nt(n1_all[rows, :], wqkvt_pad[...])
        q_all[rows, :] = cols[:, :2 * head].astype(BF16) * jnp.asarray(head ** -0.5, BF16)
        kv_all[rows, :] = cols[:, 2 * head:].astype(BF16)
        kvt_all[:, rows] = jnp.transpose(cols[:, 2 * head:]).astype(BF16)

    def attend(m):
        rows = ds_of(m, pair)
        queries = q_all[rows, :]

        def tile(t, carry, masked):
            top, total, acc = carry
            keys = ds_of(t, pair)
            s = dot_nt(kv_all[keys, :], queries)
            if masked:
                s = jnp.where(keep_mask(s.shape), s, NEG)
            new_top = jnp.maximum(top, jnp.max(s, axis=0, keepdims=True))
            p = jnp.exp(s - new_top)
            scale = jnp.exp(top - new_top)
            total = total * scale + jnp.sum(p, axis=0, keepdims=True)
            acc = acc * scale + dot_nn(kvt_all[head:, keys], p.astype(BF16))
            return new_top, total, acc

        init = (jnp.full((1, pair), NEG, F32), jnp.zeros((1, pair), F32), jnp.zeros((head, pair), F32))
        top, total, acc = tile(m, lax.fori_loop(0, m, lambda t, k: tile(t, k, False), init), True)
        ot_all[:, rows] = acc / total
        lse_all[:, rows] = top + jnp.log(total)

    def attend_grad(m, h):
        rows = (half_rows(m, 0, h), half_rows(m, 1, h))
        e_rows = jnp.concatenate([dy_all[k, :] for k in rows], axis=0)
        grads = dot_nt(e_rows, wot_pad[...]).astype(BF16)
        grads_t = jnp.transpose(grads.astype(F32))[head:]
        out_t = jnp.concatenate([ot_all[:, k] for k in rows], axis=1)
        dwo_acc[...] += dot_nn(out_t.astype(BF16), e_rows)
        row_dot = jnp.sum(grads_t * out_t, axis=0, keepdims=True)
        both = jnp.concatenate([q_all[k, :] for k in rows] + [grads], axis=0)
        lse = jnp.concatenate([lse_all[:, k] for k in rows], axis=1)

        def tile(t, dqt, masked):
            keys = ds_of(t, pair)
            sr = dot_nt(kv_all[keys, :], both)
            p = jnp.exp(sr[:, :R] - lse)
            if masked:
                query = lax.broadcasted_iota(jnp.int32, p.shape, 1)
                query = jnp.where(query < H, query, query + H) + h * H
                p = jnp.where(lax.broadcasted_iota(jnp.int32, p.shape, 0) <= query, p, 0.0)
            ds = (p * (sr[:, R:] - row_dot)).astype(BF16)
            dkv_acc[keys, :] += dot_nn(jnp.concatenate([ds, p.astype(BF16)], axis=1), both)
            return dqt + dot_nn(kvt_all[:head, keys], ds)

        dqt = lax.fori_loop(0, m, lambda t, k: tile(t, k, False), jnp.zeros((head, R), F32))
        dqt = tile(m, dqt, True) * (head ** -0.5)
        dq = jnp.transpose(jnp.concatenate([dqt, jnp.zeros_like(dqt)], axis=0)).astype(BF16)
        dq_all[rows[0], :] = dq[:H]
        dq_all[rows[1], :] = dq[H:]

    def grad_cols(rows):
        return jnp.concatenate([dq_all[rows, :], dkv_acc[rows, :].astype(BF16)], axis=1)

    barrier = pltpu.get_barrier_semaphore()
    for peer in nbr + (partner,):
        pl.semaphore_signal(barrier, inc=1, device_id={'tp': peer}, device_id_type=MESH)
    pl.semaphore_wait(barrier, 3)
    ag_begin(DY, g_ref)

    def norm_rows(k, carry):
        src = ds_of(k, piece)
        dst = ds_of((2 * z + c) * 4 + k, piece)
        for raw, gain, out in ((h_ref, gain2_ref, n2_all), (x_ref, gain1_ref, n1_all)):
            out[dst, :] = (ln_forward(raw[src, :].astype(F32))[0] * gain[...]).astype(BF16)
        dy_all[dst, :] = g_ref[src, :]
        return carry
    lax.fori_loop(0, 4, norm_rows, 0)
    for acc in (dw1t_acc, dw2_acc):
        acc[...] = jnp.zeros_like(acc)
    ag_begin(N2)
    wot_pad[:head, :] = jnp.zeros((head, width), BF16)
    wot_pad[head:, :] = wo_ref[0]
    wqkvt_pad[:head, :] = wqkvt_ref[:head, :]
    wqkvt_pad[head:2 * head, :] = jnp.zeros((head, width), BF16)
    wqkvt_pad[2 * head:, :] = wqkvt_ref[head:, :]
    for acc in (dwo_acc, dwqkvt_acc, dkv_acc):
        acc[...] = jnp.zeros_like(acc)

    def send_partner(u):
        step, sub = lax.div(u - 1, 2), lax.rem(u - 1, 2)

        @pl.when((u > 0) & ((sub == 0) | (step > 0)))
        def _():
            dx_copy(0, slot_of(step, sub)).start()

    def begin_n1(u):
        @pl.when(u == last_u - 3)
        def _():
            ag_begin(N1)

    ag_loop((DY, N2), send_partner, mlp, begin_n1)

    dx_pending = slot_of(half_ring, 0)

    def join_first(u):
        @pl.when(u == 0)
        def _():
            dx_copy(0, dx_pending).start()

        @pl.when((u > 0) & (u <= chips))
        def _():
            join_partner(0, chips - u)

    def begin_rs(u):
        @pl.when(u == last_u - 3)
        def _():
            ag_sent(N2)
            ag_sent(DY)
            rs_first(0, 1)
            rs_first(0, 2)

    ag_loop((N1,), join_first, qkv, begin_rs)

    def forward_chip(u, carry):
        rs_ticks(0, u)
        attend(chips - u)
        return carry
    lax.fori_loop(1, chips + 1, forward_chip, 0)

    def middle_piece(q, carry):
        rows = ds_of(q, piece)
        mid_hat, mid_rstd = ln_forward(h_ref[rows, :].astype(F32))
        grad = g_ref[rows, :].astype(F32) + ln_backward(mid_hat, mid_rstd, gain2_ref[...], rs_last(0, q))
        dh1[rows, :] = grad
        dy_all[piece_rows(z, c, q), :] = grad.astype(BF16)
        for h in (0, 1):
            @pl.when(q == 2 * h + 1)
            def _():
                ag_begin(EG, halves=(h,))
        return carry
    lax.fori_loop(0, 4, middle_piece, 0)
    rs_sent(0)

    def backward_unit(v, carry):
        s, h = 1 + lax.div(v, 2), lax.rem(v, 2)

        @pl.when(v < last_u - 1)
        def _():
            for d in (0, 1):
                g = jnp.where(s == half_ring, d, h)
                ag_arrived(EG, d, s, g)

                @pl.when((s < half_ring - 1) | ((s == half_ring - 1) & (h == d)))
                def _():
                    ag_copy(EG, d, s + 1, h).start()
                dd_copy(EG, slot_of(s, d), chip_at(-SIGN[d] * s), c, g).start()

        def one(sub, carry):
            ends = (v == 0) | (v == last_u - 1)
            step = jnp.where(v == 0, 0, jnp.where(v == last_u - 1, half_ring, 1 + lax.div(v - 1, 2)))
            side = jnp.where(ends, 0, sub)
            g = jnp.where(ends, sub, lax.rem(v + 1, 2))
            chip = chip_at((2 * side - 1) * step)
            dd_copy(EG, slot_of(step, side), chip, 1 - c, g).wait_recv()
            attend_grad(chip, g)
            return carry
        return lax.fori_loop(0, 2, one, carry)
    lax.fori_loop(0, last_u, backward_unit, 0)

    def share(k, carry):
        j = chips - 1 - k
        chip = chip_of_slot(j)
        for core in (1 - c, c):
            rows = block_rows(2 * chip + core)
            part[rows, :] = dot_nn(grad_cols(rows), wqkvt_pad[...]).astype(BF16)
        dx_copy(1, j).start()

        @pl.when(k > 0)
        def _():
            join_partner(1, j + 1)

        for first in (1, 2):
            @pl.when(k == 2 * first - 1)
            def _():
                rs_first(1, first)
        return carry
    lax.fori_loop(0, chips, share, 0)
    join_partner(1, 0)

    def weight_block(u, carry):
        rs_ticks(1, u)
        rows = ds_of(u - 1, pair)
        cols_t = jnp.transpose(grad_cols(rows).astype(F32)).astype(BF16)
        dwqkvt_acc[...] += dot_nn(cols_t, n1_all[rows, :])
        return carry
    lax.fori_loop(1, chips + 1, weight_block, 0)

    dw2_ref[...] = dw2_acc[...].astype(BF16)
    dw1_ref[...] = jnp.transpose(dw1t_acc[...]).astype(BF16)
    dwo_ref[0] = dwo_acc[...].astype(BF16)
    dwqkvt_ref[:head, :] = dwqkvt_acc[:head, :].astype(BF16)
    dwqkvt_ref[head:, :] = dwqkvt_acc[2 * head:, :].astype(BF16)

    def final_piece(q, carry):
        rows = ds_of(q, piece)
        in_hat, in_rstd = ln_forward(x_ref[rows, :].astype(F32))
        dx_ref[rows, :] = (dh1[rows, :] + ln_backward(in_hat, in_rstd, gain1_ref[...], rs_last(1, q))).astype(BF16)
        return carry
    lax.fori_loop(0, 4, final_piece, 0)
    rs_sent(1)
    ag_sent(N1)
    ag_sent(EG)


def hand_over(arrays):
    count = len(arrays)

    def kernel(*refs):
        ins, outs, held, sems = refs[:count], refs[count:2 * count], refs[2 * count:3 * count], refs[3 * count]
        reads = [pltpu.make_async_copy(ins[k], held[k], sems.at[0, k]) for k in range(count)]
        writes = [pltpu.make_async_copy(held[k], outs[k], sems.at[1, k]) for k in range(count)]
        for read in reads:
            read.start()
        for read, write in zip(reads, writes):
            read.wait()
            write.start()
        for write in writes:
            write.wait()

    return pl.pallas_call(
        kernel,
        out_shape=tuple(jax.ShapeDtypeStruct(a.shape, a.dtype) for a in arrays),
        in_specs=[pl.BlockSpec(memory_space=pl.ANY)] * count,
        out_specs=tuple([pl.BlockSpec(memory_space=pl.ANY)] * count),
        scratch_shapes=[pltpu.VMEM(a.shape, a.dtype) for a in arrays] + [pltpu.SemaphoreType.DMA((2, count))],
    )(*arrays)


def solution(mesh):
    chips = mesh.shape['tp'] // 2
    row_spec = P(('dp', 'tp'), None)
    in_specs = (row_spec, row_spec, row_spec, P(None), P(None), P(None, 'tp'), P('tp', None, None), P(None, 'tp'), P('tp', None))
    out_specs = (row_spec, P('dp', 'tp'), P(('dp', 'tp'), None, None), P('dp', 'tp'), P(('dp', 'tp'), None))

    def device_step(in_rows, mid_rows, gout_rows, ln1_gain, ln2_gain, wqkv_loc, wout_loc, wfc1_loc, wfc2_loc):
        R, width = in_rows.shape
        head = wout_loc.shape[1]
        hidden = wfc1_loc.shape[1]
        tokens = 2 * chips * R
        half_ring = chips // 2
        vm = pltpu.VMEM
        dma = pltpu.SemaphoreType.DMA
        scratch = [
            vm((tokens, width), BF16), vm((tokens, width), BF16), vm((tokens, width), BF16), vm((tokens, width), BF16),
            vm((chips, R, width), BF16), vm((2, half_ring, 4, R // 4, width), BF16),
            vm((tokens, 2 * head), BF16), vm((2 * head, width), BF16), vm((4 * head, width), BF16), vm((tokens, 2 * head), BF16), vm((2 * head, tokens), BF16),
            vm((head, tokens), F32), vm((1, tokens), F32),
            vm((tokens, 2 * head), BF16), vm((tokens, 2 * head), F32),
            vm((hidden, width), F32), vm((hidden, width), F32), vm((head, width), F32), vm((4 * head, width), F32), vm((R, width), F32),
            dma((4, 2, half_ring, 2)), dma((4, 2, half_ring, 2)), dma((4, chips, 2)), dma((4, chips, 2)),
            dma((2, 2, half_ring, 4)), dma((2, 2, half_ring, 4)), dma((2, chips)), dma((2, chips)),
        ]
        grads = pl.pallas_call(
            lambda *refs: layer_kernel(chips, *refs),
            out_shape=(
                jax.ShapeDtypeStruct((R, width), BF16), jax.ShapeDtypeStruct((3 * head, width), BF16),
                jax.ShapeDtypeStruct((1, head, width), BF16), jax.ShapeDtypeStruct((width, hidden), BF16),
                jax.ShapeDtypeStruct((hidden, width), BF16)),
            in_specs=[pl.BlockSpec(memory_space=pltpu.VMEM)] * 9,
            out_specs=tuple([pl.BlockSpec(memory_space=pltpu.VMEM)] * 5),
            scratch_shapes=scratch,
            compiler_params=pltpu.CompilerParams(collective_id=0, has_side_effects=True, vmem_limit_bytes=67043328),
        )(in_rows, mid_rows, gout_rows, ln1_gain[None], ln2_gain[None], wqkv_loc.T, wout_loc, wfc1_loc, wfc2_loc)
        grad_in, grad_wqkvt, grad_wout, grad_wfc1, grad_wfc2 = hand_over(grads)
        return grad_in, grad_wqkvt.T, grad_wout, grad_wfc1, grad_wfc2

    return jax.shard_map(device_step, mesh=mesh, in_specs=in_specs, out_specs=out_specs, check_vma=False)
```

```python
import jax
import jax.numpy as jnp
from jax import lax
from jax.experimental import pallas as pl
from jax.experimental.pallas import tpu as pltpu
from jax.sharding import PartitionSpec as P

LN_EPS = 1e-5
GELU_COEF = 0.044715
GELU_SCALE = 0.7978845608028654
NEG = -1e30
F32 = jnp.float32
BF16 = jnp.bfloat16
MESH = pl.DeviceIdType.MESH
SIGN = (1, -1)
N2, DY, N1, EG = 0, 1, 2, 3


def ln_forward(rows):
    row_mean = jnp.mean(rows, axis=-1, keepdims=True)
    centered = rows - row_mean
    row_rstd = lax.rsqrt(jnp.mean(centered * centered, axis=-1, keepdims=True) + LN_EPS)
    return centered * row_rstd, row_rstd


def ln_backward(x_hat, row_rstd, ln_gain, grad_norm):
    grad_hat = grad_norm * ln_gain
    proj_one = jnp.mean(grad_hat, axis=-1, keepdims=True)
    proj_two = jnp.mean(grad_hat * x_hat, axis=-1, keepdims=True)
    return row_rstd * (grad_hat - proj_one - x_hat * proj_two)


def gelu_pair(pre_act):
    tanh_val = jnp.tanh(GELU_SCALE * (pre_act + GELU_COEF * pre_act * pre_act * pre_act))
    gelu_val = 0.5 * pre_act * (1.0 + tanh_val)
    gelu_der = 0.5 * (1.0 + tanh_val) + 0.5 * pre_act * (1.0 - tanh_val * tanh_val) * GELU_SCALE * (1.0 + 3.0 * GELU_COEF * pre_act * pre_act)
    return gelu_val, gelu_der


def dot_nt(a, b):
    return lax.dot_general(a, b, (((1,), (1,)), ((), ())), preferred_element_type=F32)


def dot_nn(a, b):
    return lax.dot_general(a, b, (((1,), (0,)), ((), ())), preferred_element_type=F32)


def ds_of(index, size):
    return pl.ds(pl.multiple_of(index * size, size), size)


def keep_mask(shape):
    return lax.broadcasted_iota(jnp.int32, shape, 0) <= lax.broadcasted_iota(jnp.int32, shape, 1)


def layer_kernel(chips, x_ref, h_ref, g_ref, gain1_ref, gain2_ref, wqkvt_ref, wo_ref, w1_ref, w2_ref,
                 dx_ref, dwqkvt_ref, dwo_ref, dw1_ref, dw2_ref,
                 n2_all, dy_all, n1_all, part, dbuf, rbuf, q_all, wot_pad, wqkvt_pad, kv_all, kvt_all, ot_all, lse_all,
                 dq_all, dkv_acc, dw1t_acc, dw2_acc, dwo_acc, dwqkvt_acc, dh1,
                 ag_send, ag_recv, dd_send, dd_recv, rs_send, rs_recv, dx_send, dx_recv):
    me = lax.axis_index('tp')
    z, c = lax.div(me, 2), lax.rem(me, 2)
    half_ring = chips // 2
    last_u = 2 * half_ring
    R, width = x_ref.shape
    H = R // 2
    piece = R // 4
    head = dwo_ref.shape[1]
    pair = 2 * R
    full = (n2_all, dy_all, n1_all, dy_all)

    def chip_at(offset):
        return lax.rem(z + offset + 2 * chips, chips)

    nbr = tuple(2 * chip_at(s) + c for s in SIGN)
    partner = 2 * z + 1 - c

    def half_rows(chip, core, h):
        return ds_of(2 * (2 * chip + core) + h, H)

    def piece_rows(chip, core, q):
        return ds_of(4 * (2 * chip + core) + q, piece)

    def block_rows(block):
        return ds_of(block, R)

    def ag_copy(a, d, s, h, src=None):
        dst = full[a].at[half_rows(chip_at(-SIGN[d] * (s - 1)), c, h)]
        return pltpu.make_async_remote_copy(dst if src is None else src, dst, ag_send.at[a, d, s - 1, h],
                                            ag_recv.at[a, d, s - 1, h], device_id={'tp': nbr[d]}, device_id_type=MESH)

    def ag_arrived(a, d, s, h):
        dst = full[a].at[half_rows(chip_at(-SIGN[d] * s), c, h)]
        pltpu.make_async_remote_copy(dst, dst, ag_send.at[a, d, s - 1, h],
                                     ag_recv.at[a, d, s - 1, h], device_id={'tp': nbr[d]}, device_id_type=MESH).wait_recv()

    def dd_copy(a, j, chip, core, h, src=None):
        dst = full[a].at[half_rows(chip, core, h)]
        return pltpu.make_async_remote_copy(dst if src is None else src, dst, dd_send.at[a, j, h], dd_recv.at[a, j, h],
                                            device_id={'tp': partner}, device_id_type=MESH)

    def slot_of(step, d):
        return jnp.where(step == 0, 0, jnp.minimum(2 * step - 1 + d, chips - 1))

    def chip_of_slot(j):
        away = lax.div(j + 1, 2)
        return chip_at(jnp.where(lax.rem(j, 2) == 1, -away, away))

    def dx_copy(r, j):
        chip = chip_of_slot(j)
        return pltpu.make_async_remote_copy(part.at[block_rows(2 * chip + 1 - c)], dbuf.at[chip], dx_send.at[r, j],
                                            dx_recv.at[r, j], device_id={'tp': partner}, device_id_type=MESH)

    def rs_copy(r, d, s, h):
        src = part.at[piece_rows(chip_at(SIGN[d] * (half_ring - s + 1)), c, h)]
        return pltpu.make_async_remote_copy(src, rbuf.at[d, s - 1, h], rs_send.at[r, d, s - 1, h],
                                            rs_recv.at[r, d, s - 1, h], device_id={'tp': nbr[d]}, device_id_type=MESH)

    def ag_begin(a, src=None, halves=(0, 1)):
        for h in halves:
            part_src = None if src is None else src.at[pl.ds(h * H, H)]
            dd_copy(a, 0, z, c, h, part_src).start()
            for d in (0, 1):
                ag_copy(a, d, 1, h, part_src).start()

    def ag_sent(a):
        for h in (0, 1):
            for d in (0, 1):
                for s in range(1, half_ring + 1):
                    if s < half_ring or h == d:
                        ag_copy(a, d, s, h).wait_send()
            for j in range(chips):
                dd_copy(a, j, chip_of_slot(j), c, h).wait_send()

    def ag_loop(arrays, before, compute, after):
        def body(u, carry):
            step, h = lax.div(u, 2), lax.rem(u, 2)
            s = step + 1

            @pl.when(u < last_u)
            def _():
                for a in arrays:
                    for d in (0, 1):
                        @pl.when((s < half_ring) | (h == d))
                        def _():
                            ag_arrived(a, d, s, h)
                            dd_copy(a, slot_of(s, d), chip_at(-SIGN[d] * s), c, h).start()

                            @pl.when((s < half_ring - 1) | ((s == half_ring - 1) & (h == d)))
                            def _():
                                ag_copy(a, d, s + 1, h).start()
            before(u)

            @pl.when((h == 0) | ((step > 0) & (step < half_ring)))
            def _():
                chip = chip_at((2 * h - 1) * step)
                for a in arrays:
                    for g in (0, 1):
                        dd_copy(a, slot_of(step, h), chip, 1 - c, g).wait_recv()
                compute(chip)
            after(u)
            return carry
        lax.fori_loop(0, last_u + 1, body, 0)

    def rs_first(r, s):
        for d in (0, 1):
            for q in (0, 1):
                rs_copy(r, d, s, (2 * d + q + 2 * (s - 1)) % 4).start()

    def rs_tick(r, k):
        s = 2 + lax.div(k + 2, 4)
        place = lax.rem(k + 2, 4)
        swapped = lax.rem(place + 2, 4)
        rising = jnp.where(place == 3, 3, lax.rem(place + 2, 3))
        order = (jnp.where(s == half_ring, place, jnp.where(s == half_ring - 1, rising, swapped)), place)
        for d in (0, 1):
            q = order[d]
            rs_copy(r, d, s - 1, q).wait_recv()
            rows = piece_rows(chip_at(SIGN[d] * (half_ring - s + 1)), c, q)
            part[rows, :] = (part[rows, :].astype(F32) + rbuf[d, s - 2, q].astype(F32)).astype(BF16)
        for d in (0, 1):
            rs_copy(r, d, s, order[d]).start()

    def rs_ticks(r, u):
        @pl.when(u <= last_u - 3)
        def _():
            rs_tick(r, 2 * u - 2)
            rs_tick(r, 2 * u - 1)

    def rs_last(r, q):
        for d in (0, 1):
            rs_copy(r, d, half_ring, q).wait_recv()
        own = part[piece_rows(z, c, q), :].astype(F32)
        return own + rbuf[0, half_ring - 1, q].astype(F32) + rbuf[1, half_ring - 1, q].astype(F32)

    def rs_sent(r):
        for d in (0, 1):
            for q in range(4):
                for s in range(1, half_ring + 1):
                    if s > 1 or q // 2 == d:
                        rs_copy(r, d, s, q).wait_send()
        for j in range(chips):
            dx_copy(r, j).wait_send()

    def join_partner(r, j):
        dx_copy(r, j).wait_recv()
        chip = chip_of_slot(j)
        rows = block_rows(2 * chip + c)
        part[rows, :] = (part[rows, :].astype(F32) + dbuf[chip].astype(F32)).astype(BF16)

    def mlp(chip):
        rows = ds_of(chip, pair)
        n2, dy = n2_all[rows, :], dy_all[rows, :]
        gelu_val, gelu_der = gelu_pair(dot_nn(n2, w1_ref[...]))
        grad_pre = dot_nt(dy, w2_ref[...]) * gelu_der
        dw2_acc[...] += dot_nn(jnp.transpose(gelu_val).astype(BF16), dy)
        dw1t_acc[...] += dot_nn(jnp.transpose(grad_pre).astype(BF16), n2)
        part[rows, :] = dot_nt(grad_pre.astype(BF16), w1_ref[...]).astype(BF16)

    def qkv(chip):
        rows = ds_of(chip, pair)
        cols = dot_nt(n1_all[rows, :], wqkvt_pad[...])
        q_all[rows, :] = cols[:, :2 * head].astype(BF16) * jnp.asarray(head ** -0.5, BF16)
        kv_all[rows, :] = cols[:, 2 * head:].astype(BF16)
        kvt_all[:, rows] = jnp.transpose(cols[:, 2 * head:]).astype(BF16)

    def attend(m):
        rows = ds_of(m, pair)
        queries = q_all[rows, :]

        def tile(t, carry, masked):
            top, total, acc = carry
            keys = ds_of(t, pair)
            s = dot_nt(kv_all[keys, :], queries)
            if masked:
                s = jnp.where(keep_mask(s.shape), s, NEG)
            new_top = jnp.maximum(top, jnp.max(s, axis=0, keepdims=True))
            p = jnp.exp(s - new_top)
            scale = jnp.exp(top - new_top)
            total = total * scale + jnp.sum(p, axis=0, keepdims=True)
            acc = acc * scale + dot_nn(kvt_all[head:, keys], p.astype(BF16))
            return new_top, total, acc

        init = (jnp.full((1, pair), NEG, F32), jnp.zeros((1, pair), F32), jnp.zeros((head, pair), F32))
        top, total, acc = tile(m, lax.fori_loop(0, m, lambda t, k: tile(t, k, False), init), True)
        ot_all[:, rows] = acc / total
        lse_all[:, rows] = top + jnp.log(total)

    def attend_grad(m, h):
        rows = (half_rows(m, 0, h), half_rows(m, 1, h))
        e_rows = jnp.concatenate([dy_all[k, :] for k in rows], axis=0)
        grads = dot_nt(e_rows, wot_pad[...]).astype(BF16)
        grads_t = jnp.transpose(grads.astype(F32))[head:]
        out_t = jnp.concatenate([ot_all[:, k] for k in rows], axis=1)
        dwo_acc[...] += dot_nn(out_t.astype(BF16), e_rows)
        row_dot = jnp.sum(grads_t * out_t, axis=0, keepdims=True)
        both = jnp.concatenate([q_all[k, :] for k in rows] + [grads], axis=0)
        lse = jnp.concatenate([lse_all[:, k] for k in rows], axis=1)

        def tile(t, dqt, masked):
            keys = ds_of(t, pair)
            sr = dot_nt(kv_all[keys, :], both)
            p = jnp.exp(sr[:, :R] - lse)
            if masked:
                query = lax.broadcasted_iota(jnp.int32, p.shape, 1)
                query = jnp.where(query < H, query, query + H) + h * H
                p = jnp.where(lax.broadcasted_iota(jnp.int32, p.shape, 0) <= query, p, 0.0)
            ds = (p * (sr[:, R:] - row_dot)).astype(BF16)
            dkv_acc[keys, :] += dot_nn(jnp.concatenate([ds, p.astype(BF16)], axis=1), both)
            return dqt + dot_nn(kvt_all[:head, keys], ds)

        dqt = lax.fori_loop(0, m, lambda t, k: tile(t, k, False), jnp.zeros((head, R), F32))
        dqt = tile(m, dqt, True) * (head ** -0.5)
        dq = jnp.transpose(jnp.concatenate([dqt, jnp.zeros_like(dqt)], axis=0)).astype(BF16)
        dq_all[rows[0], :] = dq[:H]
        dq_all[rows[1], :] = dq[H:]

    def grad_cols(rows):
        return jnp.concatenate([dq_all[rows, :], dkv_acc[rows, :].astype(BF16)], axis=1)

    barrier = pltpu.get_barrier_semaphore()
    for peer in nbr + (partner,):
        pl.semaphore_signal(barrier, inc=1, device_id={'tp': peer}, device_id_type=MESH)
    pl.semaphore_wait(barrier, 3)
    ag_begin(DY, g_ref)

    def norm_rows(k, carry):
        src = ds_of(k, piece)
        dst = ds_of((2 * z + c) * 4 + k, piece)
        for raw, gain, out in ((h_ref, gain2_ref, n2_all), (x_ref, gain1_ref, n1_all)):
            out[dst, :] = (ln_forward(raw[src, :].astype(F32))[0] * gain[...]).astype(BF16)
        dy_all[dst, :] = g_ref[src, :]
        return carry
    lax.fori_loop(0, 4, norm_rows, 0)
    for acc in (dw1t_acc, dw2_acc):
        acc[...] = jnp.zeros_like(acc)
    ag_begin(N2)
    wot_pad[:head, :] = jnp.zeros((head, width), BF16)
    wot_pad[head:, :] = wo_ref[0]
    wqkvt_pad[:head, :] = wqkvt_ref[:head, :]
    wqkvt_pad[head:2 * head, :] = jnp.zeros((head, width), BF16)
    wqkvt_pad[2 * head:, :] = wqkvt_ref[head:, :]
    for acc in (dwo_acc, dwqkvt_acc, dkv_acc):
        acc[...] = jnp.zeros_like(acc)

    def send_partner(u):
        step, sub = lax.div(u - 1, 2), lax.rem(u - 1, 2)

        @pl.when((u > 0) & ((sub == 0) | (step > 0)))
        def _():
            dx_copy(0, slot_of(step, sub)).start()

    def begin_n1(u):
        @pl.when(u == last_u - 3)
        def _():
            ag_begin(N1)

    ag_loop((DY, N2), send_partner, mlp, begin_n1)

    dx_pending = slot_of(half_ring, 0)

    def join_first(u):
        @pl.when(u == 0)
        def _():
            dx_copy(0, dx_pending).start()

        @pl.when((u > 0) & (u <= chips))
        def _():
            join_partner(0, chips - u)

    def begin_rs(u):
        @pl.when(u == last_u - 3)
        def _():
            ag_sent(N2)
            ag_sent(DY)
            rs_first(0, 1)
            rs_first(0, 2)

    ag_loop((N1,), join_first, qkv, begin_rs)

    def forward_chip(u, carry):
        rs_ticks(0, u)
        attend(chips - u)
        return carry
    lax.fori_loop(1, chips + 1, forward_chip, 0)

    def middle_piece(q, carry):
        rows = ds_of(q, piece)
        mid_hat, mid_rstd = ln_forward(h_ref[rows, :].astype(F32))
        grad = g_ref[rows, :].astype(F32) + ln_backward(mid_hat, mid_rstd, gain2_ref[...], rs_last(0, q))
        dh1[rows, :] = grad
        dy_all[piece_rows(z, c, q), :] = grad.astype(BF16)
        for h in (0, 1):
            @pl.when(q == 2 * h + 1)
            def _():
                ag_begin(EG, halves=(h,))
        return carry
    lax.fori_loop(0, 4, middle_piece, 0)
    rs_sent(0)

    def backward_unit(v, carry):
        s, h = 1 + lax.div(v, 2), lax.rem(v, 2)

        @pl.when(v < last_u - 1)
        def _():
            for d in (0, 1):
                g = jnp.where(s == half_ring, d, h)
                ag_arrived(EG, d, s, g)
                dd_copy(EG, slot_of(s, d), chip_at(-SIGN[d] * s), c, g).start()

                @pl.when((s < half_ring - 1) | ((s == half_ring - 1) & (h == d)))
                def _():
                    ag_copy(EG, d, s + 1, h).start()

        def one(sub, carry):
            ends = (v == 0) | (v == last_u - 1)
            step = jnp.where(v == 0, 0, jnp.where(v == last_u - 1, half_ring, 1 + lax.div(v - 1, 2)))
            side = jnp.where(ends, 0, sub)
            g = jnp.where(ends, sub, lax.rem(v + 1, 2))
            chip = chip_at((2 * side - 1) * step)
            dd_copy(EG, slot_of(step, side), chip, 1 - c, g).wait_recv()
            attend_grad(chip, g)
            return carry
        return lax.fori_loop(0, 2, one, carry)
    lax.fori_loop(0, last_u, backward_unit, 0)

    def share(k, carry):
        j = chips - 1 - k
        chip = chip_of_slot(j)
        for core in (1 - c, c):
            rows = block_rows(2 * chip + core)
            part[rows, :] = dot_nn(grad_cols(rows), wqkvt_pad[...]).astype(BF16)
        dx_copy(1, j).start()

        @pl.when(k > 0)
        def _():
            join_partner(1, j + 1)

        for first in (1, 2):
            @pl.when(k == 2 * first - 1)
            def _():
                rs_first(1, first)
        return carry
    lax.fori_loop(0, chips, share, 0)
    join_partner(1, 0)

    def weight_block(u, carry):
        rs_ticks(1, u)
        rows = ds_of(u - 1, pair)
        cols_t = jnp.transpose(grad_cols(rows).astype(F32)).astype(BF16)
        dwqkvt_acc[...] += dot_nn(cols_t, n1_all[rows, :])
        return carry
    lax.fori_loop(1, chips + 1, weight_block, 0)

    ag_sent(N1)
    ag_sent(EG)
    dw2_ref[...] = dw2_acc[...].astype(BF16)
    dw1_ref[...] = jnp.transpose(dw1t_acc[...]).astype(BF16)
    dwo_ref[0] = dwo_acc[...].astype(BF16)
    dwqkvt_ref[:head, :] = dwqkvt_acc[:head, :].astype(BF16)
    dwqkvt_ref[head:, :] = dwqkvt_acc[2 * head:, :].astype(BF16)

    def final_piece(q, carry):
        rows = ds_of(q, piece)
        in_hat, in_rstd = ln_forward(x_ref[rows, :].astype(F32))
        dx_ref[rows, :] = (dh1[rows, :] + ln_backward(in_hat, in_rstd, gain1_ref[...], rs_last(1, q))).astype(BF16)
        return carry
    lax.fori_loop(0, 4, final_piece, 0)
    rs_sent(1)


def hand_over(arrays):
    count = len(arrays)

    def kernel(*refs):
        ins, outs, held, sems = refs[:count], refs[count:2 * count], refs[2 * count:3 * count], refs[3 * count]
        reads = [pltpu.make_async_copy(ins[k], held[k], sems.at[0, k]) for k in range(count)]
        writes = [pltpu.make_async_copy(held[k], outs[k], sems.at[1, k]) for k in range(count)]
        for read in reads:
            read.start()
        for read, write in zip(reads, writes):
            read.wait()
            write.start()
        for write in writes:
            write.wait()

    return pl.pallas_call(
        kernel,
        out_shape=tuple(jax.ShapeDtypeStruct(a.shape, a.dtype) for a in arrays),
        in_specs=[pl.BlockSpec(memory_space=pl.ANY)] * count,
        out_specs=tuple([pl.BlockSpec(memory_space=pl.ANY)] * count),
        scratch_shapes=[pltpu.VMEM(a.shape, a.dtype) for a in arrays] + [pltpu.SemaphoreType.DMA((2, count))],
    )(*arrays)


def solution(mesh):
    chips = mesh.shape['tp'] // 2
    row_spec = P(('dp', 'tp'), None)
    in_specs = (row_spec, row_spec, row_spec, P(None), P(None), P(None, 'tp'), P('tp', None, None), P(None, 'tp'), P('tp', None))
    out_specs = (row_spec, P('dp', 'tp'), P(('dp', 'tp'), None, None), P('dp', 'tp'), P(('dp', 'tp'), None))

    def device_step(in_rows, mid_rows, gout_rows, ln1_gain, ln2_gain, wqkv_loc, wout_loc, wfc1_loc, wfc2_loc):
        R, width = in_rows.shape
        head = wout_loc.shape[1]
        hidden = wfc1_loc.shape[1]
        tokens = 2 * chips * R
        half_ring = chips // 2
        vm = pltpu.VMEM
        dma = pltpu.SemaphoreType.DMA
        scratch = [
            vm((tokens, width), BF16), vm((tokens, width), BF16), vm((tokens, width), BF16), vm((tokens, width), BF16),
            vm((chips, R, width), BF16), vm((2, half_ring, 4, R // 4, width), BF16),
            vm((tokens, 2 * head), BF16), vm((2 * head, width), BF16), vm((4 * head, width), BF16), vm((tokens, 2 * head), BF16), vm((2 * head, tokens), BF16),
            vm((head, tokens), F32), vm((1, tokens), F32),
            vm((tokens, 2 * head), BF16), vm((tokens, 2 * head), F32),
            vm((hidden, width), F32), vm((hidden, width), F32), vm((head, width), F32), vm((4 * head, width), F32), vm((R, width), F32),
            dma((4, 2, half_ring, 2)), dma((4, 2, half_ring, 2)), dma((4, chips, 2)), dma((4, chips, 2)),
            dma((2, 2, half_ring, 4)), dma((2, 2, half_ring, 4)), dma((2, chips)), dma((2, chips)),
        ]
        grads = pl.pallas_call(
            lambda *refs: layer_kernel(chips, *refs),
            out_shape=(
                jax.ShapeDtypeStruct((R, width), BF16), jax.ShapeDtypeStruct((3 * head, width), BF16),
                jax.ShapeDtypeStruct((1, head, width), BF16), jax.ShapeDtypeStruct((width, hidden), BF16),
                jax.ShapeDtypeStruct((hidden, width), BF16)),
            in_specs=[pl.BlockSpec(memory_space=pltpu.VMEM)] * 9,
            out_specs=tuple([pl.BlockSpec(memory_space=pltpu.VMEM)] * 5),
            scratch_shapes=scratch,
            compiler_params=pltpu.CompilerParams(collective_id=0, has_side_effects=True, vmem_limit_bytes=67043328),
        )(in_rows, mid_rows, gout_rows, ln1_gain[None], ln2_gain[None], wqkv_loc.T, wout_loc, wfc1_loc, wfc2_loc)
        grad_in, grad_wqkvt, grad_wout, grad_wfc1, grad_wfc2 = hand_over(grads)
        return grad_in, grad_wqkvt.T, grad_wout, grad_wfc1, grad_wfc2

    return jax.shard_map(device_step, mesh=mesh, in_specs=in_specs, out_specs=out_specs, check_vma=False)
```

```python
import jax
import jax.numpy as jnp
from jax import lax
from jax.experimental import pallas as pl
from jax.experimental.pallas import tpu as pltpu
from jax.sharding import PartitionSpec as P

LN_EPS = 1e-5
GELU_COEF = 0.044715
GELU_SCALE = 0.7978845608028654
NEG = -1e30
F32 = jnp.float32
BF16 = jnp.bfloat16
MESH = pl.DeviceIdType.MESH
SIGN = (1, -1)
N2, DY, N1, EG = 0, 1, 2, 3


def ln_forward(rows):
    row_mean = jnp.mean(rows, axis=-1, keepdims=True)
    centered = rows - row_mean
    row_rstd = lax.rsqrt(jnp.mean(centered * centered, axis=-1, keepdims=True) + LN_EPS)
    return centered * row_rstd, row_rstd


def ln_backward(x_hat, row_rstd, ln_gain, grad_norm):
    grad_hat = grad_norm * ln_gain
    proj_one = jnp.mean(grad_hat, axis=-1, keepdims=True)
    proj_two = jnp.mean(grad_hat * x_hat, axis=-1, keepdims=True)
    return row_rstd * (grad_hat - proj_one - x_hat * proj_two)


def gelu_pair(pre_act):
    tanh_val = jnp.tanh(GELU_SCALE * (pre_act + GELU_COEF * pre_act * pre_act * pre_act))
    gelu_val = 0.5 * pre_act * (1.0 + tanh_val)
    gelu_der = 0.5 * (1.0 + tanh_val) + 0.5 * pre_act * (1.0 - tanh_val * tanh_val) * GELU_SCALE * (1.0 + 3.0 * GELU_COEF * pre_act * pre_act)
    return gelu_val, gelu_der


def dot_nt(a, b):
    return lax.dot_general(a, b, (((1,), (1,)), ((), ())), preferred_element_type=F32)


def dot_nn(a, b):
    return lax.dot_general(a, b, (((1,), (0,)), ((), ())), preferred_element_type=F32)


def ds_of(index, size):
    return pl.ds(pl.multiple_of(index * size, size), size)


def keep_mask(shape):
    return lax.broadcasted_iota(jnp.int32, shape, 0) <= lax.broadcasted_iota(jnp.int32, shape, 1)


def layer_kernel(chips, g_hbm, h_hbm, x_hbm, gain1_ref, gain2_ref, wqkvt_hbm, wo_hbm, w1_hbm, w2_hbm,
                 dx_hbm, dwqkvt_hbm, dwo_hbm, dw1_hbm, dw2_hbm,
                 g_ref, h_ref, x_ref, wqkvt_ref, wo_ref, w1_ref, w2_ref, dx_ref, dwqkvt_ref, dwo_ref, dw1_ref, dw2_ref, in_sem, out_sem,
                 n2_all, dy_all, n1_all, part, dbuf, rbuf, q_all, wot_pad, wqkvt_pad, kv_all, kvt_all, ot_all, lse_all,
                 dq_all, dkv_acc, dw1t_acc, dw2_acc, dwo_acc, dwqkvt_acc, dh1,
                 ag_send, ag_recv, dd_send, dd_recv, rs_send, rs_recv, dx_send, dx_recv):
    me = lax.axis_index('tp')
    z, c = lax.div(me, 2), lax.rem(me, 2)
    half_ring = chips // 2
    last_u = 2 * half_ring
    R, width = x_hbm.shape
    H = R // 2
    piece = R // 4
    head = dwo_hbm.shape[1]
    pair = 2 * R
    full = (n2_all, dy_all, n1_all, dy_all)

    def chip_at(offset):
        return lax.rem(z + offset + 2 * chips, chips)

    nbr = tuple(2 * chip_at(s) + c for s in SIGN)
    partner = 2 * z + 1 - c

    def half_rows(chip, core, h):
        return ds_of(2 * (2 * chip + core) + h, H)

    def piece_rows(chip, core, q):
        return ds_of(4 * (2 * chip + core) + q, piece)

    def block_rows(block):
        return ds_of(block, R)

    def ag_copy(a, d, s, h, src=None):
        dst = full[a].at[half_rows(chip_at(-SIGN[d] * (s - 1)), c, h)]
        return pltpu.make_async_remote_copy(dst if src is None else src, dst, ag_send.at[a, d, s - 1, h],
                                            ag_recv.at[a, d, s - 1, h], device_id={'tp': nbr[d]}, device_id_type=MESH)

    def ag_arrived(a, d, s, h):
        dst = full[a].at[half_rows(chip_at(-SIGN[d] * s), c, h)]
        pltpu.make_async_remote_copy(dst, dst, ag_send.at[a, d, s - 1, h],
                                     ag_recv.at[a, d, s - 1, h], device_id={'tp': nbr[d]}, device_id_type=MESH).wait_recv()

    def dd_copy(a, j, chip, core, h, src=None):
        dst = full[a].at[half_rows(chip, core, h)]
        return pltpu.make_async_remote_copy(dst if src is None else src, dst, dd_send.at[a, j, h], dd_recv.at[a, j, h],
                                            device_id={'tp': partner}, device_id_type=MESH)

    def slot_of(step, d):
        return jnp.where(step == 0, 0, jnp.minimum(2 * step - 1 + d, chips - 1))

    def chip_of_slot(j):
        away = lax.div(j + 1, 2)
        return chip_at(jnp.where(lax.rem(j, 2) == 1, -away, away))

    def dx_copy(r, j):
        chip = chip_of_slot(j)
        return pltpu.make_async_remote_copy(part.at[block_rows(2 * chip + 1 - c)], dbuf.at[chip], dx_send.at[r, j],
                                            dx_recv.at[r, j], device_id={'tp': partner}, device_id_type=MESH)

    def rs_copy(r, d, s, h):
        src = part.at[piece_rows(chip_at(SIGN[d] * (half_ring - s + 1)), c, h)]
        return pltpu.make_async_remote_copy(src, rbuf.at[d, s - 1, h], rs_send.at[r, d, s - 1, h],
                                            rs_recv.at[r, d, s - 1, h], device_id={'tp': nbr[d]}, device_id_type=MESH)

    def ag_begin(a, src=None, halves=(0, 1)):
        for h in halves:
            part_src = None if src is None else src.at[pl.ds(h * H, H)]
            dd_copy(a, 0, z, c, h, part_src).start()
            for d in (0, 1):
                ag_copy(a, d, 1, h, part_src).start()

    def ag_sent(a):
        for h in (0, 1):
            for d in (0, 1):
                for s in range(1, half_ring + 1):
                    if s < half_ring or h == d:
                        ag_copy(a, d, s, h).wait_send()
            for j in range(chips):
                dd_copy(a, j, chip_of_slot(j), c, h).wait_send()

    def ag_loop(arrays, before, compute, after):
        def body(u, carry):
            step, h = lax.div(u, 2), lax.rem(u, 2)
            s = step + 1

            @pl.when(u < last_u)
            def _():
                for a in arrays:
                    for d in (0, 1):
                        @pl.when((s < half_ring) | (h == d))
                        def _():
                            ag_arrived(a, d, s, h)
                            dd_copy(a, slot_of(s, d), chip_at(-SIGN[d] * s), c, h).start()

                            @pl.when((s < half_ring - 1) | ((s == half_ring - 1) & (h == d)))
                            def _():
                                ag_copy(a, d, s + 1, h).start()
            before(u)

            @pl.when((h == 0) | ((step > 0) & (step < half_ring)))
            def _():
                chip = chip_at((2 * h - 1) * step)
                for a in arrays:
                    for g in (0, 1):
                        dd_copy(a, slot_of(step, h), chip, 1 - c, g).wait_recv()
                compute(chip)
            after(u)
            return carry
        lax.fori_loop(0, last_u + 1, body, 0)

    def rs_first(r, s):
        for d in (0, 1):
            for q in (0, 1):
                rs_copy(r, d, s, (2 * d + q + 2 * (s - 1)) % 4).start()

    def rs_tick(r, k):
        s = 2 + lax.div(k + 2, 4)
        place = lax.rem(k + 2, 4)
        swapped = lax.rem(place + 2, 4)
        rising = jnp.where(place == 3, 3, lax.rem(place + 2, 3))
        order = (jnp.where(s == half_ring, place, jnp.where(s == half_ring - 1, rising, swapped)), place)
        for d in (0, 1):
            q = order[d]
            rs_copy(r, d, s - 1, q).wait_recv()
            rows = piece_rows(chip_at(SIGN[d] * (half_ring - s + 1)), c, q)
            part[rows, :] = (part[rows, :].astype(F32) + rbuf[d, s - 2, q].astype(F32)).astype(BF16)
        for d in (0, 1):
            rs_copy(r, d, s, order[d]).start()

    def rs_ticks(r, u):
        @pl.when(u <= last_u - 3)
        def _():
            rs_tick(r, 2 * u - 2)
            rs_tick(r, 2 * u - 1)

    def rs_last(r, q):
        for d in (0, 1):
            rs_copy(r, d, half_ring, q).wait_recv()
        own = part[piece_rows(z, c, q), :].astype(F32)
        return own + rbuf[0, half_ring - 1, q].astype(F32) + rbuf[1, half_ring - 1, q].astype(F32)

    def rs_sent(r, steps):
        for d in (0, 1):
            for q in range(4):
                for s in steps:
                    if s > 1 or q // 2 == d:
                        rs_copy(r, d, s, q).wait_send()

    def dx_sent(r):
        for j in range(chips):
            dx_copy(r, j).wait_send()

    def join_partner(r, j):
        dx_copy(r, j).wait_recv()
        chip = chip_of_slot(j)
        rows = block_rows(2 * chip + c)
        part[rows, :] = (part[rows, :].astype(F32) + dbuf[chip].astype(F32)).astype(BF16)

    def mlp(chip):
        rows = ds_of(chip, pair)
        n2, dy = n2_all[rows, :], dy_all[rows, :]
        gelu_val, gelu_der = gelu_pair(dot_nn(n2, w1_ref[...]))
        grad_pre = dot_nt(dy, w2_ref[...]) * gelu_der
        dw2_acc[...] += dot_nn(jnp.transpose(gelu_val).astype(BF16), dy)
        dw1t_acc[...] += dot_nn(jnp.transpose(grad_pre).astype(BF16), n2)
        part[rows, :] = dot_nt(grad_pre.astype(BF16), w1_ref[...]).astype(BF16)

    def qkv(chip):
        rows = ds_of(chip, pair)
        cols = dot_nt(n1_all[rows, :], wqkvt_pad[...])
        q_all[rows, :] = cols[:, :2 * head].astype(BF16) * jnp.asarray(head ** -0.5, BF16)
        kv_all[rows, :] = cols[:, 2 * head:].astype(BF16)
        kvt_all[:, rows] = jnp.transpose(cols[:, 2 * head:]).astype(BF16)

    def attend(m):
        rows = ds_of(m, pair)
        queries = q_all[rows, :]

        def tile(t, carry, masked):
            top, total, acc = carry
            keys = ds_of(t, pair)
            s = dot_nt(kv_all[keys, :], queries)
            if masked:
                s = jnp.where(keep_mask(s.shape), s, NEG)
            new_top = jnp.maximum(top, jnp.max(s, axis=0, keepdims=True))
            p = jnp.exp(s - new_top)
            scale = jnp.exp(top - new_top)
            total = total * scale + jnp.sum(p, axis=0, keepdims=True)
            acc = acc * scale + dot_nn(kvt_all[head:, keys], p.astype(BF16))
            return new_top, total, acc

        init = (jnp.full((1, pair), NEG, F32), jnp.zeros((1, pair), F32), jnp.zeros((head, pair), F32))
        top, total, acc = tile(m, lax.fori_loop(0, m, lambda t, k: tile(t, k, False), init), True)
        ot_all[:, rows] = acc / total
        lse_all[:, rows] = top + jnp.log(total)

    def attend_grad(m, h):
        rows = (half_rows(m, 0, h), half_rows(m, 1, h))
        e_rows = jnp.concatenate([dy_all[k, :] for k in rows], axis=0)
        grads = dot_nt(e_rows, wot_pad[...]).astype(BF16)
        grads_t = jnp.transpose(grads.astype(F32))[head:]
        out_t = jnp.concatenate([ot_all[:, k] for k in rows], axis=1)
        dwo_acc[...] += dot_nn(out_t.astype(BF16), e_rows)
        row_dot = jnp.sum(grads_t * out_t, axis=0, keepdims=True)
        both = jnp.concatenate([q_all[k, :] for k in rows] + [grads], axis=0)
        lse = jnp.concatenate([lse_all[:, k] for k in rows], axis=1)

        def tile(t, dqt, masked):
            keys = ds_of(t, pair)
            sr = dot_nt(kv_all[keys, :], both)
            p = jnp.exp(sr[:, :R] - lse)
            if masked:
                query = lax.broadcasted_iota(jnp.int32, p.shape, 1)
                query = jnp.where(query < H, query, query + H) + h * H
                p = jnp.where(lax.broadcasted_iota(jnp.int32, p.shape, 0) <= query, p, 0.0)
            ds = (p * (sr[:, R:] - row_dot)).astype(BF16)
            dkv_acc[keys, :] += dot_nn(jnp.concatenate([ds, p.astype(BF16)], axis=1), both)
            return dqt + dot_nn(kvt_all[:head, keys], ds)

        dqt = lax.fori_loop(0, m, lambda t, k: tile(t, k, False), jnp.zeros((head, R), F32))
        dqt = tile(m, dqt, True) * (head ** -0.5)
        dq = jnp.transpose(jnp.concatenate([dqt, jnp.zeros_like(dqt)], axis=0)).astype(BF16)
        dq_all[rows[0], :] = dq[:H]
        dq_all[rows[1], :] = dq[H:]

    def grad_cols(rows):
        return jnp.concatenate([dq_all[rows, :], dkv_acc[rows, :].astype(BF16)], axis=1)

    loads = [pltpu.make_async_copy(src, dst, in_sem.at[k]) for k, (src, dst) in enumerate((
        (g_hbm, g_ref), (h_hbm, h_ref), (x_hbm, x_ref), (w1_hbm, w1_ref), (w2_hbm, w2_ref), (wqkvt_hbm, wqkvt_ref), (wo_hbm, wo_ref)))]
    barrier = pltpu.get_barrier_semaphore()
    for peer in nbr + (partner,):
        pl.semaphore_signal(barrier, inc=1, device_id={'tp': peer}, device_id_type=MESH)
    for load in loads:
        load.start()
    pl.semaphore_wait(barrier, 3)
    loads[0].wait()
    ag_begin(DY, g_ref)
    loads[1].wait()
    loads[2].wait()

    def norm_rows(k, carry):
        src = ds_of(k, piece)
        dst = ds_of((2 * z + c) * 4 + k, piece)
        for raw, gain, out in ((h_ref, gain2_ref, n2_all), (x_ref, gain1_ref, n1_all)):
            out[dst, :] = (ln_forward(raw[src, :].astype(F32))[0] * gain[...]).astype(BF16)
        dy_all[dst, :] = g_ref[src, :]
        return carry
    lax.fori_loop(0, 4, norm_rows, 0)
    for acc in (dw1t_acc, dw2_acc):
        acc[...] = jnp.zeros_like(acc)
    ag_begin(N2)
    for load in loads[3:]:
        load.wait()
    wot_pad[:head, :] = jnp.zeros((head, width), BF16)
    wot_pad[head:, :] = wo_ref[0]
    wqkvt_pad[:head, :] = wqkvt_ref[:head, :]
    wqkvt_pad[head:2 * head, :] = jnp.zeros((head, width), BF16)
    wqkvt_pad[2 * head:, :] = wqkvt_ref[head:, :]
    for acc in (dwo_acc, dwqkvt_acc, dkv_acc):
        acc[...] = jnp.zeros_like(acc)

    def send_partner(u):
        step, sub = lax.div(u - 1, 2), lax.rem(u - 1, 2)

        @pl.when((u > 0) & ((sub == 0) | (step > 0)))
        def _():
            dx_copy(0, slot_of(step, sub)).start()

    def begin_n1(u):
        @pl.when(u == last_u - 3)
        def _():
            ag_begin(N1)

    ag_loop((DY, N2), send_partner, mlp, begin_n1)

    dx_pending = slot_of(half_ring, 0)

    def join_first(u):
        @pl.when(u == 0)
        def _():
            dx_copy(0, dx_pending).start()

        @pl.when((u > 0) & (u <= chips))
        def _():
            join_partner(0, chips - u)

    def begin_rs(u):
        @pl.when(u == last_u - 3)
        def _():
            ag_sent(N2)
            ag_sent(DY)
            rs_first(0, 1)
            rs_first(0, 2)

    ag_loop((N1,), join_first, qkv, begin_rs)

    def forward_chip(u, carry):
        rs_ticks(0, u)
        attend(chips - u)
        return carry
    lax.fori_loop(1, chips + 1, forward_chip, 0)

    def middle_piece(q, carry):
        rows = ds_of(q, piece)
        mid_hat, mid_rstd = ln_forward(h_ref[rows, :].astype(F32))
        grad = g_ref[rows, :].astype(F32) + ln_backward(mid_hat, mid_rstd, gain2_ref[...], rs_last(0, q))
        dh1[rows, :] = grad
        dy_all[piece_rows(z, c, q), :] = grad.astype(BF16)
        for h in (0, 1):
            @pl.when(q == 2 * h + 1)
            def _():
                ag_begin(EG, halves=(h,))
        return carry
    lax.fori_loop(0, 4, middle_piece, 0)
    rs_sent(0, range(1, half_ring + 1))
    dx_sent(0)

    def backward_call(x, carry):
        v = lax.div(x - 1, 2)
        s, h = 1 + lax.div(v, 2), lax.rem(v, 2)

        @pl.when((lax.rem(x, 2) == 1) & (v < last_u - 1))
        def _():
            for d in (0, 1):
                g = jnp.where(s == half_ring, d, h)
                ag_arrived(EG, d, s, g)
                dd_copy(EG, slot_of(s, d), chip_at(-SIGN[d] * s), c, g).start()

                @pl.when((s < half_ring - 1) | ((s == half_ring - 1) & (h == d)))
                def _():
                    ag_copy(EG, d, s + 1, h).start()

        first, final = x < 2, x >= 2 * last_u - 2
        unit, side = lax.div(jnp.maximum(x - 2, 0), 2), lax.rem(x, 2)
        step = jnp.where(first, 0, jnp.where(final, half_ring, 1 + lax.div(unit, 2)))
        g = jnp.where(first | final, side, lax.rem(unit, 2))
        side = jnp.where(first | final, 0, side)
        chip = chip_at((2 * side - 1) * step)
        dd_copy(EG, slot_of(step, side), chip, 1 - c, g).wait_recv()
        attend_grad(chip, g)
        return carry
    lax.fori_loop(0, 2 * last_u, backward_call, 0)

    def share(k, carry):
        j = chips - 1 - k
        chip = chip_of_slot(j)
        for core in (1 - c, c):
            rows = block_rows(2 * chip + core)
            part[rows, :] = dot_nn(grad_cols(rows), wqkvt_pad[...]).astype(BF16)
        dx_copy(1, j).start()

        @pl.when(k > 0)
        def _():
            join_partner(1, j + 1)

        for first in (1, 2):
            @pl.when(k == 2 * first - 1)
            def _():
                rs_first(1, first)
        return carry
    lax.fori_loop(0, chips, share, 0)
    join_partner(1, 0)

    def weight_block(u, carry):
        rs_ticks(1, u)
        rows = ds_of(u - 1, pair)
        cols_t = jnp.transpose(grad_cols(rows).astype(F32)).astype(BF16)
        dwqkvt_acc[...] += dot_nn(cols_t, n1_all[rows, :])
        return carry
    lax.fori_loop(1, chips + 1, weight_block, 0)

    dw2_ref[...] = dw2_acc[...].astype(BF16)
    dw1_ref[...] = jnp.transpose(dw1t_acc[...]).astype(BF16)
    dwo_ref[0] = dwo_acc[...].astype(BF16)
    dwqkvt_ref[:head, :] = dwqkvt_acc[:head, :].astype(BF16)
    dwqkvt_ref[head:, :] = dwqkvt_acc[2 * head:, :].astype(BF16)
    ag_sent(N1)
    ag_sent(EG)
    stores = [pltpu.make_async_copy(src, dst, out_sem.at[k]) for k, (src, dst) in enumerate((
        (dw2_ref, dw2_hbm), (dw1_ref, dw1_hbm), (dwo_ref, dwo_hbm), (dwqkvt_ref, dwqkvt_hbm)))]
    for store in stores:
        store.start()
    dx_sent(1)
    rs_sent(1, range(1, half_ring))
    for store in stores:
        store.wait()

    def dx_store(q):
        rows = pl.ds(q * piece, piece)
        return pltpu.make_async_copy(dx_ref.at[rows], dx_hbm.at[rows], out_sem.at[4 + q])

    def final_piece(q, carry):
        rows = ds_of(q, piece)
        in_hat, in_rstd = ln_forward(x_ref[rows, :].astype(F32))
        dx_ref[rows, :] = (dh1[rows, :] + ln_backward(in_hat, in_rstd, gain1_ref[...], rs_last(1, q))).astype(BF16)

        @pl.when(q > 0)
        def _():
            dx_store(q - 1).start()
        return carry
    lax.fori_loop(0, 4, final_piece, 0)
    rs_sent(1, (half_ring,))
    dx_store(3).start()
    for q in range(4):
        dx_store(q).wait()


def hand_over(arrays):
    count = len(arrays)

    def kernel(*refs):
        ins, outs, held, sems = refs[:count], refs[count:2 * count], refs[2 * count:3 * count], refs[3 * count]
        moves = []
        for k in range(count):
            axis = len(arrays[k].shape) - 2
            size = arrays[k].shape[axis] // 2
            for h in (0, 1):
                at = (slice(None),) * axis + (pl.ds(h * size, size),)
                moves.append((pltpu.make_async_copy(ins[k].at[at], held[k].at[at], sems.at[0, k, h]),
                              pltpu.make_async_copy(held[k].at[at], outs[k].at[at], sems.at[1, k, h])))
        for read, _ in moves:
            read.start()
        for read, write in moves:
            read.wait()
            write.start()
        for _, write in moves:
            write.wait()

    return pl.pallas_call(
        kernel,
        out_shape=tuple(jax.ShapeDtypeStruct(a.shape, a.dtype) for a in arrays),
        in_specs=[pl.BlockSpec(memory_space=pl.ANY)] * count,
        out_specs=tuple([pl.BlockSpec(memory_space=pl.ANY)] * count),
        scratch_shapes=[pltpu.VMEM(a.shape, a.dtype) for a in arrays] + [pltpu.SemaphoreType.DMA((2, count, 2))],
    )(*arrays)


def solution(mesh):
    chips = mesh.shape['tp'] // 2
    row_spec = P(('dp', 'tp'), None)
    in_specs = (row_spec, row_spec, row_spec, P(None), P(None), P(None, 'tp'), P('tp', None, None), P(None, 'tp'), P('tp', None))
    out_specs = (row_spec, P('dp', 'tp'), P(('dp', 'tp'), None, None), P('dp', 'tp'), P(('dp', 'tp'), None))

    def device_step(in_rows, mid_rows, gout_rows, ln1_gain, ln2_gain, wqkv_loc, wout_loc, wfc1_loc, wfc2_loc):
        R, width = in_rows.shape
        head = wout_loc.shape[1]
        hidden = wfc1_loc.shape[1]
        tokens = 2 * chips * R
        half_ring = chips // 2
        vm = pltpu.VMEM
        hbm = pl.BlockSpec(memory_space=pl.ANY)
        vmem = pl.BlockSpec(memory_space=pltpu.VMEM)
        dma = pltpu.SemaphoreType.DMA
        outs = (
            jax.ShapeDtypeStruct((R, width), BF16), jax.ShapeDtypeStruct((3 * head, width), BF16),
            jax.ShapeDtypeStruct((1, head, width), BF16), jax.ShapeDtypeStruct((width, hidden), BF16),
            jax.ShapeDtypeStruct((hidden, width), BF16))
        wide = (in_rows, in_rows, in_rows, outs[1], wout_loc, wfc1_loc, wfc2_loc) + outs
        scratch = [vm(a.shape, BF16) for a in wide] + [dma((7,)), dma((8,))] + [
            vm((tokens, width), BF16), vm((tokens, width), BF16), vm((tokens, width), BF16), vm((tokens, width), BF16),
            vm((chips, R, width), BF16), vm((2, half_ring, 4, R // 4, width), BF16),
            vm((tokens, 2 * head), BF16), vm((2 * head, width), BF16), vm((4 * head, width), BF16), vm((tokens, 2 * head), BF16), vm((2 * head, tokens), BF16),
            vm((head, tokens), F32), vm((1, tokens), F32),
            vm((tokens, 2 * head), BF16), vm((tokens, 2 * head), F32),
            vm((hidden, width), F32), vm((hidden, width), F32), vm((head, width), F32), vm((4 * head, width), F32), vm((R, width), F32),
            dma((4, 2, half_ring, 2)), dma((4, 2, half_ring, 2)), dma((4, chips, 2)), dma((4, chips, 2)),
            dma((2, 2, half_ring, 4)), dma((2, 2, half_ring, 4)), dma((2, chips)), dma((2, chips)),
        ]
        grads = pl.pallas_call(
            lambda *refs: layer_kernel(chips, *refs),
            out_shape=outs,
            in_specs=[hbm, hbm, hbm, vmem, vmem, hbm, hbm, hbm, hbm],
            out_specs=(hbm,) * 5,
            scratch_shapes=scratch,
            compiler_params=pltpu.CompilerParams(collective_id=0, has_side_effects=True, vmem_limit_bytes=67043328),
        )(gout_rows, mid_rows, in_rows, ln1_gain[None], ln2_gain[None], wqkv_loc.T, wout_loc, wfc1_loc, wfc2_loc)
        grad_in, grad_wqkvt, grad_wout, grad_wfc1, grad_wfc2 = hand_over(grads)
        return grad_in, grad_wqkvt.T, grad_wout, grad_wfc1, grad_wfc2

    return jax.shard_map(device_step, mesh=mesh, in_specs=in_specs, out_specs=out_specs, check_vma=False)
```

```python
import jax
import jax.numpy as jnp
from jax import lax
from jax.experimental import pallas as pl
from jax.experimental.pallas import tpu as pltpu
from jax.sharding import PartitionSpec as P

LN_EPS = 1e-5
GELU_COEF = 0.044715
GELU_SCALE = 0.7978845608028654
NEG = -1e30
F32 = jnp.float32
BF16 = jnp.bfloat16
MESH = pl.DeviceIdType.MESH
SIGN = (1, -1)
N2, DY, N1, EG = 0, 1, 2, 3


def ln_forward(rows):
    row_mean = jnp.mean(rows, axis=-1, keepdims=True)
    centered = rows - row_mean
    row_rstd = lax.rsqrt(jnp.mean(centered * centered, axis=-1, keepdims=True) + LN_EPS)
    return centered * row_rstd, row_rstd


def ln_backward(x_hat, row_rstd, ln_gain, grad_norm):
    grad_hat = grad_norm * ln_gain
    proj_one = jnp.mean(grad_hat, axis=-1, keepdims=True)
    proj_two = jnp.mean(grad_hat * x_hat, axis=-1, keepdims=True)
    return row_rstd * (grad_hat - proj_one - x_hat * proj_two)


def gelu_pair(pre_act):
    tanh_val = jnp.tanh(GELU_SCALE * (pre_act + GELU_COEF * pre_act * pre_act * pre_act))
    gelu_val = 0.5 * pre_act * (1.0 + tanh_val)
    gelu_der = 0.5 * (1.0 + tanh_val) + 0.5 * pre_act * (1.0 - tanh_val * tanh_val) * GELU_SCALE * (1.0 + 3.0 * GELU_COEF * pre_act * pre_act)
    return gelu_val, gelu_der


def dot_nt(a, b):
    return lax.dot_general(a, b, (((1,), (1,)), ((), ())), preferred_element_type=F32)


def dot_nn(a, b):
    return lax.dot_general(a, b, (((1,), (0,)), ((), ())), preferred_element_type=F32)


def ds_of(index, size):
    return pl.ds(pl.multiple_of(index * size, size), size)


def keep_mask(shape):
    return lax.broadcasted_iota(jnp.int32, shape, 0) <= lax.broadcasted_iota(jnp.int32, shape, 1)


def layer_kernel(chips, g_hbm, h_hbm, x_hbm, gain1_ref, gain2_ref, wqkvt_hbm, wo_hbm, w1_hbm, w2_hbm,
                 dx_hbm, dwqkvt_hbm, dwo_hbm, dw1_hbm, dw2_hbm,
                 g_ref, h_ref, x_ref, wqkvt_ref, wo_ref, w1_ref, w2_ref, dx_ref, dwqkvt_ref, dwo_ref, dw1_ref, dw2_ref, in_sem, out_sem,
                 n2_all, dy_all, n1_all, part, dbuf, rbuf, q_all, wot_pad, wqkvt_pad, kv_all, kvt_all, ot_all, lse_all,
                 dq_all, dkv_acc, dw1t_acc, dw2_acc, dwo_acc, dwqkvt_acc, dh1,
                 ag_send, ag_recv, dd_send, dd_recv, rs_send, rs_recv, dx_send, dx_recv):
    me = lax.axis_index('tp')
    z, c = lax.div(me, 2), lax.rem(me, 2)
    half_ring = chips // 2
    last_u = 2 * half_ring
    R, width = x_hbm.shape
    H = R // 2
    piece = R // 4
    head = dwo_hbm.shape[1]
    pair = 2 * R
    full = (n2_all, dy_all, n1_all, dy_all)

    def chip_at(offset):
        return lax.rem(z + offset + 2 * chips, chips)

    nbr = tuple(2 * chip_at(s) + c for s in SIGN)
    partner = 2 * z + 1 - c

    def half_rows(chip, core, h):
        return ds_of(2 * (2 * chip + core) + h, H)

    def piece_rows(chip, core, q):
        return ds_of(4 * (2 * chip + core) + q, piece)

    def block_rows(block):
        return ds_of(block, R)

    def ag_copy(a, d, s, h, src=None):
        dst = full[a].at[half_rows(chip_at(-SIGN[d] * (s - 1)), c, h)]
        return pltpu.make_async_remote_copy(dst if src is None else src, dst, ag_send.at[a, d, s - 1, h],
                                            ag_recv.at[a, d, s - 1, h], device_id={'tp': nbr[d]}, device_id_type=MESH)

    def ag_arrived(a, d, s, h):
        dst = full[a].at[half_rows(chip_at(-SIGN[d] * s), c, h)]
        pltpu.make_async_remote_copy(dst, dst, ag_send.at[a, d, s - 1, h],
                                     ag_recv.at[a, d, s - 1, h], device_id={'tp': nbr[d]}, device_id_type=MESH).wait_recv()

    def dd_copy(a, j, chip, core, h, src=None):
        dst = full[a].at[half_rows(chip, core, h)]
        return pltpu.make_async_remote_copy(dst if src is None else src, dst, dd_send.at[a, j, h], dd_recv.at[a, j, h],
                                            device_id={'tp': partner}, device_id_type=MESH)

    def slot_of(step, d):
        return jnp.where(step == 0, 0, jnp.minimum(2 * step - 1 + d, chips - 1))

    def chip_of_slot(j):
        away = lax.div(j + 1, 2)
        return chip_at(jnp.where(lax.rem(j, 2) == 1, -away, away))

    def dx_copy(r, j):
        chip = chip_of_slot(j)
        return pltpu.make_async_remote_copy(part.at[block_rows(2 * chip + 1 - c)], dbuf.at[chip], dx_send.at[r, j],
                                            dx_recv.at[r, j], device_id={'tp': partner}, device_id_type=MESH)

    def rs_copy(r, d, s, h):
        src = part.at[piece_rows(chip_at(SIGN[d] * (half_ring - s + 1)), c, h)]
        return pltpu.make_async_remote_copy(src, rbuf.at[d, s - 1, h], rs_send.at[r, d, s - 1, h],
                                            rs_recv.at[r, d, s - 1, h], device_id={'tp': nbr[d]}, device_id_type=MESH)

    def ag_begin(a, src=None, halves=(0, 1)):
        for h in halves:
            part_src = None if src is None else src.at[pl.ds(h * H, H)]
            dd_copy(a, 0, z, c, h, part_src).start()
            for d in (0, 1):
                ag_copy(a, d, 1, h, part_src).start()

    def ag_sent(a):
        for h in (0, 1):
            for d in (0, 1):
                for s in range(1, half_ring + 1):
                    if s < half_ring or h == d:
                        ag_copy(a, d, s, h).wait_send()
            for j in range(chips):
                dd_copy(a, j, chip_of_slot(j), c, h).wait_send()

    def ag_loop(arrays, before, compute, after):
        def body(u, carry):
            step, h = lax.div(u, 2), lax.rem(u, 2)
            s = step + 1

            @pl.when(u < last_u)
            def _():
                for a in arrays:
                    for d in (0, 1):
                        @pl.when((s < half_ring) | (h == d))
                        def _():
                            ag_arrived(a, d, s, h)
                            dd_copy(a, slot_of(s, d), chip_at(-SIGN[d] * s), c, h).start()

                            @pl.when((s < half_ring - 1) | ((s == half_ring - 1) & (h == d)))
                            def _():
                                ag_copy(a, d, s + 1, h).start()
            before(u)

            @pl.when((h == 0) | ((step > 0) & (step < half_ring)))
            def _():
                chip = chip_at((2 * h - 1) * step)
                for a in arrays:
                    for g in (0, 1):
                        dd_copy(a, slot_of(step, h), chip, 1 - c, g).wait_recv()
                compute(chip)
            after(u)
            return carry
        lax.fori_loop(0, last_u + 1, body, 0)

    def rs_first(r, s):
        for d in (0, 1):
            for q in (0, 1):
                rs_copy(r, d, s, (2 * d + q + 2 * (s - 1)) % 4).start()

    def rs_tick(r, k):
        s = 2 + lax.div(k + 2, 4)
        place = lax.rem(k + 2, 4)
        swapped = lax.rem(place + 2, 4)
        rising = jnp.where(place == 3, 3, lax.rem(place + 2, 3))
        order = (jnp.where(s == half_ring, place, jnp.where(s == half_ring - 1, rising, swapped)), place)
        for d in (0, 1):
            q = order[d]
            rs_copy(r, d, s - 1, q).wait_recv()
            rows = piece_rows(chip_at(SIGN[d] * (half_ring - s + 1)), c, q)
            part[rows, :] = (part[rows, :].astype(F32) + rbuf[d, s - 2, q].astype(F32)).astype(BF16)
        for d in (0, 1):
            rs_copy(r, d, s, order[d]).start()

    def rs_ticks(r, u):
        @pl.when(u <= last_u - 3)
        def _():
            rs_tick(r, 2 * u - 2)
            rs_tick(r, 2 * u - 1)

    def rs_last(r, q):
        for d in (0, 1):
            rs_copy(r, d, half_ring, q).wait_recv()
        own = part[piece_rows(z, c, q), :].astype(F32)
        return own + rbuf[0, half_ring - 1, q].astype(F32) + rbuf[1, half_ring - 1, q].astype(F32)

    def rs_sent(r, steps):
        for d in (0, 1):
            for q in range(4):
                for s in steps:
                    if s > 1 or q // 2 == d:
                        rs_copy(r, d, s, q).wait_send()

    def dx_sent(r):
        for j in range(chips):
            dx_copy(r, j).wait_send()

    def join_partner(r, j):
        dx_copy(r, j).wait_recv()
        chip = chip_of_slot(j)
        rows = block_rows(2 * chip + c)
        part[rows, :] = (part[rows, :].astype(F32) + dbuf[chip].astype(F32)).astype(BF16)

    def mlp(chip):
        rows = ds_of(chip, pair)
        n2, dy = n2_all[rows, :], dy_all[rows, :]
        gelu_val, gelu_der = gelu_pair(dot_nn(n2, w1_ref[...]))
        grad_pre = dot_nt(dy, w2_ref[...]) * gelu_der
        dw2_acc[...] += dot_nn(jnp.transpose(gelu_val).astype(BF16), dy)
        dw1t_acc[...] += dot_nn(jnp.transpose(grad_pre).astype(BF16), n2)
        part[rows, :] = dot_nt(grad_pre.astype(BF16), w1_ref[...]).astype(BF16)

    def qkv(chip):
        rows = ds_of(chip, pair)
        cols = dot_nt(n1_all[rows, :], wqkvt_pad[...])
        q_all[rows, :] = cols[:, :2 * head].astype(BF16) * jnp.asarray(head ** -0.5, BF16)
        kv_all[rows, :] = cols[:, 2 * head:].astype(BF16)
        kvt_all[:, rows] = jnp.transpose(cols[:, 2 * head:]).astype(BF16)

    def attend(m):
        rows = ds_of(m, pair)
        queries = q_all[rows, :]

        def tile(t, carry, masked):
            top, total, acc = carry
            keys = ds_of(t, pair)
            s = dot_nt(kv_all[keys, :], queries)
            if masked:
                s = jnp.where(keep_mask(s.shape), s, NEG)
            new_top = jnp.maximum(top, jnp.max(s, axis=0, keepdims=True))
            p = jnp.exp(s - new_top)
            scale = jnp.exp(top - new_top)
            total = total * scale + jnp.sum(p, axis=0, keepdims=True)
            acc = acc * scale + dot_nn(kvt_all[head:, keys], p.astype(BF16))
            return new_top, total, acc

        init = (jnp.full((1, pair), NEG, F32), jnp.zeros((1, pair), F32), jnp.zeros((head, pair), F32))
        top, total, acc = tile(m, lax.fori_loop(0, m, lambda t, k: tile(t, k, False), init), True)
        ot_all[:, rows] = acc / total
        lse_all[:, rows] = top + jnp.log(total)

    def attend_grad(m, h=None):
        rows = (ds_of(m, pair),) if h is None else (half_rows(m, 0, h), half_rows(m, 1, h))
        count = pair if h is None else R
        e_rows = jnp.concatenate([dy_all[k, :] for k in rows], axis=0)
        grads = dot_nt(e_rows, wot_pad[...]).astype(BF16)
        grads_t = jnp.transpose(grads.astype(F32))[head:]
        out_t = jnp.concatenate([ot_all[:, k] for k in rows], axis=1)
        row_dot = jnp.sum(grads_t * out_t, axis=0, keepdims=True)
        both = jnp.concatenate([q_all[k, :] for k in rows] + [grads], axis=0)
        lse = jnp.concatenate([lse_all[:, k] for k in rows], axis=1)

        def tile(t, dqt, masked):
            keys = ds_of(t, pair)
            sr = dot_nt(kv_all[keys, :], both)
            p = jnp.exp(sr[:, :count] - lse)
            if masked:
                query = lax.broadcasted_iota(jnp.int32, p.shape, 1)
                if h is not None:
                    query = jnp.where(query < H, query, query + H) + h * H
                p = jnp.where(lax.broadcasted_iota(jnp.int32, p.shape, 0) <= query, p, 0.0)
            ds = (p * (sr[:, count:] - row_dot)).astype(BF16)
            dkv_acc[keys, :] += dot_nn(jnp.concatenate([ds, p.astype(BF16)], axis=1), both)
            return dqt + dot_nn(kvt_all[:head, keys], ds)

        dqt = lax.fori_loop(0, m, lambda t, k: tile(t, k, False), jnp.zeros((head, count), F32))
        dqt = tile(m, dqt, True) * (head ** -0.5)
        dq = jnp.transpose(jnp.concatenate([dqt, jnp.zeros_like(dqt)], axis=0)).astype(BF16)
        for k, place in enumerate(rows):
            dq_all[place, :] = dq[k * H:(k + 1) * H] if len(rows) > 1 else dq

    def grad_cols(rows):
        return jnp.concatenate([dq_all[rows, :], dkv_acc[rows, :].astype(BF16)], axis=1)

    loads = [pltpu.make_async_copy(src, dst, in_sem.at[k]) for k, (src, dst) in enumerate((
        (g_hbm, g_ref), (h_hbm, h_ref), (x_hbm, x_ref), (w1_hbm, w1_ref), (w2_hbm, w2_ref), (wqkvt_hbm, wqkvt_ref), (wo_hbm, wo_ref)))]
    barrier = pltpu.get_barrier_semaphore()
    for peer in nbr + (partner,):
        pl.semaphore_signal(barrier, inc=1, device_id={'tp': peer}, device_id_type=MESH)
    for load in loads:
        load.start()
    pl.semaphore_wait(barrier, 3)
    loads[0].wait()
    ag_begin(DY, g_ref)
    loads[1].wait()
    loads[2].wait()

    def norm_rows(k, carry):
        src = ds_of(k, piece)
        dst = ds_of((2 * z + c) * 4 + k, piece)
        for raw, gain, out in ((h_ref, gain2_ref, n2_all), (x_ref, gain1_ref, n1_all)):
            out[dst, :] = (ln_forward(raw[src, :].astype(F32))[0] * gain[...]).astype(BF16)
        dy_all[dst, :] = g_ref[src, :]
        return carry
    lax.fori_loop(0, 4, norm_rows, 0)
    for acc in (dw1t_acc, dw2_acc):
        acc[...] = jnp.zeros_like(acc)
    ag_begin(N2)
    for load in loads[3:]:
        load.wait()
    wot_pad[:head, :] = jnp.zeros((head, width), BF16)
    wot_pad[head:, :] = wo_ref[0]
    wqkvt_pad[:head, :] = wqkvt_ref[:head, :]
    wqkvt_pad[head:2 * head, :] = jnp.zeros((head, width), BF16)
    wqkvt_pad[2 * head:, :] = wqkvt_ref[head:, :]
    for acc in (dwo_acc, dwqkvt_acc, dkv_acc):
        acc[...] = jnp.zeros_like(acc)

    def send_partner(u):
        step, sub = lax.div(u - 1, 2), lax.rem(u - 1, 2)

        @pl.when((u > 0) & ((sub == 0) | (step > 0)))
        def _():
            dx_copy(0, slot_of(step, sub)).start()

    def begin_n1(u):
        @pl.when(u == last_u - 3)
        def _():
            ag_begin(N1)

    ag_loop((DY, N2), send_partner, mlp, begin_n1)

    dx_pending = slot_of(half_ring, 0)

    def join_first(u):
        @pl.when(u == 0)
        def _():
            dx_copy(0, dx_pending).start()

        @pl.when((u > 0) & (u <= chips))
        def _():
            join_partner(0, chips - u)

    def begin_rs(u):
        @pl.when(u == last_u - 3)
        def _():
            ag_sent(N2)
            ag_sent(DY)
            rs_first(0, 1)
            rs_first(0, 2)

    ag_loop((N1,), join_first, qkv, begin_rs)

    def forward_chip(u, carry):
        rs_ticks(0, u)
        attend(chips - u)
        return carry
    lax.fori_loop(1, chips + 1, forward_chip, 0)

    def middle_piece(q, carry):
        rows = ds_of(q, piece)
        mid_hat, mid_rstd = ln_forward(h_ref[rows, :].astype(F32))
        grad = g_ref[rows, :].astype(F32) + ln_backward(mid_hat, mid_rstd, gain2_ref[...], rs_last(0, q))
        dh1[rows, :] = grad
        dy_all[piece_rows(z, c, q), :] = grad.astype(BF16)
        for h in (0, 1):
            @pl.when(q == 2 * h + 1)
            def _():
                ag_begin(EG, halves=(h,))
        return carry
    lax.fori_loop(0, 4, middle_piece, 0)
    rs_sent(0, range(1, half_ring + 1))
    dx_sent(0)

    def e_tick(v):
        s, h = 1 + lax.div(v, 2), lax.rem(v, 2)
        for d in (0, 1):
            g = jnp.where(s == half_ring, d, h)
            ag_arrived(EG, d, s, g)
            dd_copy(EG, slot_of(s, d), chip_at(-SIGN[d] * s), c, g).start()

            @pl.when((s < half_ring - 1) | ((s == half_ring - 1) & (h == d)))
            def _():
                ag_copy(EG, d, s + 1, h).start()

    def backward_call(x, carry):
        @pl.when((lax.rem(x, 2) == 1) & (x < 2 * last_u - 3))
        def _():
            e_tick(lax.div(x - 1, 2))

        unit, side = lax.div(jnp.maximum(x - 2, 0), 2), lax.rem(x, 2)
        step = jnp.where(x < 2, 0, 1 + lax.div(unit, 2))
        g = jnp.where(x < 2, side, lax.rem(unit, 2))
        side = jnp.where(x < 2, 0, side)
        chip = chip_at((2 * side - 1) * step)
        dd_copy(EG, slot_of(step, side), chip, 1 - c, g).wait_recv()
        attend_grad(chip, g)
        return carry
    lax.fori_loop(0, 2 * last_u - 2, backward_call, 0)
    e_tick(jnp.int32(last_u - 2))
    last_chip = chip_at(half_ring)
    for g in (0, 1):
        dd_copy(EG, chips - 1, last_chip, 1 - c, g).wait_recv()
    attend_grad(last_chip)

    def share(k, carry):
        j = chips - 1 - k
        chip = chip_of_slot(j)
        for core in (1 - c, c):
            rows = block_rows(2 * chip + core)
            part[rows, :] = dot_nn(grad_cols(rows), wqkvt_pad[...]).astype(BF16)
        dx_copy(1, j).start()

        @pl.when(k > 0)
        def _():
            join_partner(1, j + 1)

        for first in (1, 2):
            @pl.when(k == 2 * first - 1)
            def _():
                rs_first(1, first)
        return carry
    lax.fori_loop(0, chips, share, 0)
    join_partner(1, 0)

    def weight_block(u, carry):
        rs_ticks(1, u)
        rows = ds_of(u - 1, pair)
        cols_t = jnp.transpose(grad_cols(rows).astype(F32)).astype(BF16)
        dwqkvt_acc[...] += dot_nn(cols_t, n1_all[rows, :])
        dwo_acc[...] += dot_nn(ot_all[:, rows].astype(BF16), dy_all[rows, :])
        return carry
    lax.fori_loop(1, chips + 1, weight_block, 0)

    dw2_ref[...] = dw2_acc[...].astype(BF16)
    dw1_ref[...] = jnp.transpose(dw1t_acc[...]).astype(BF16)
    dwo_ref[0] = dwo_acc[...].astype(BF16)
    dwqkvt_ref[:head, :] = dwqkvt_acc[:head, :].astype(BF16)
    dwqkvt_ref[head:, :] = dwqkvt_acc[2 * head:, :].astype(BF16)
    ag_sent(N1)
    ag_sent(EG)
    stores = [pltpu.make_async_copy(src, dst, out_sem.at[k]) for k, (src, dst) in enumerate((
        (dw2_ref, dw2_hbm), (dw1_ref, dw1_hbm), (dwo_ref, dwo_hbm), (dwqkvt_ref, dwqkvt_hbm)))]
    for store in stores:
        store.start()
    dx_sent(1)
    rs_sent(1, range(1, half_ring))
    for store in stores:
        store.wait()

    def dx_store(q):
        rows = pl.ds(q * piece, piece)
        return pltpu.make_async_copy(dx_ref.at[rows], dx_hbm.at[rows], out_sem.at[4 + q])

    def final_piece(q, carry):
        rows = ds_of(q, piece)
        in_hat, in_rstd = ln_forward(x_ref[rows, :].astype(F32))
        dx_ref[rows, :] = (dh1[rows, :] + ln_backward(in_hat, in_rstd, gain1_ref[...], rs_last(1, q))).astype(BF16)

        @pl.when(q > 0)
        def _():
            dx_store(q - 1).start()
        return carry
    lax.fori_loop(0, 4, final_piece, 0)
    rs_sent(1, (half_ring,))
    dx_store(3).start()
    for q in range(4):
        dx_store(q).wait()


def hand_over(arrays):
    count = len(arrays)

    def kernel(*refs):
        ins, outs, held, sems = refs[:count], refs[count:2 * count], refs[2 * count:3 * count], refs[3 * count]
        moves = []
        for k in range(count):
            axis = len(arrays[k].shape) - 2
            size = arrays[k].shape[axis] // 2
            for h in (0, 1):
                at = (slice(None),) * axis + (pl.ds(h * size, size),)
                moves.append((pltpu.make_async_copy(ins[k].at[at], held[k].at[at], sems.at[0, k, h]),
                              pltpu.make_async_copy(held[k].at[at], outs[k].at[at], sems.at[1, k, h])))
        for read, _ in moves:
            read.start()
        for read, write in moves:
            read.wait()
            write.start()
        for _, write in moves:
            write.wait()

    return pl.pallas_call(
        kernel,
        out_shape=tuple(jax.ShapeDtypeStruct(a.shape, a.dtype) for a in arrays),
        in_specs=[pl.BlockSpec(memory_space=pl.ANY)] * count,
        out_specs=tuple([pl.BlockSpec(memory_space=pl.ANY)] * count),
        scratch_shapes=[pltpu.VMEM(a.shape, a.dtype) for a in arrays] + [pltpu.SemaphoreType.DMA((2, count, 2))],
    )(*arrays)


def solution(mesh):
    chips = mesh.shape['tp'] // 2
    row_spec = P(('dp', 'tp'), None)
    in_specs = (row_spec, row_spec, row_spec, P(None), P(None), P(None, 'tp'), P('tp', None, None), P(None, 'tp'), P('tp', None))
    out_specs = (row_spec, P('dp', 'tp'), P(('dp', 'tp'), None, None), P('dp', 'tp'), P(('dp', 'tp'), None))

    def device_step(in_rows, mid_rows, gout_rows, ln1_gain, ln2_gain, wqkv_loc, wout_loc, wfc1_loc, wfc2_loc):
        R, width = in_rows.shape
        head = wout_loc.shape[1]
        hidden = wfc1_loc.shape[1]
        tokens = 2 * chips * R
        half_ring = chips // 2
        vm = pltpu.VMEM
        hbm = pl.BlockSpec(memory_space=pl.ANY)
        vmem = pl.BlockSpec(memory_space=pltpu.VMEM)
        dma = pltpu.SemaphoreType.DMA
        outs = (
            jax.ShapeDtypeStruct((R, width), BF16), jax.ShapeDtypeStruct((3 * head, width), BF16),
            jax.ShapeDtypeStruct((1, head, width), BF16), jax.ShapeDtypeStruct((width, hidden), BF16),
            jax.ShapeDtypeStruct((hidden, width), BF16))
        wide = (in_rows, in_rows, in_rows, outs[1], wout_loc, wfc1_loc, wfc2_loc) + outs
        scratch = [vm(a.shape, BF16) for a in wide] + [dma((7,)), dma((8,))] + [
            vm((tokens, width), BF16), vm((tokens, width), BF16), vm((tokens, width), BF16), vm((tokens, width), BF16),
            vm((chips, R, width), BF16), vm((2, half_ring, 4, R // 4, width), BF16),
            vm((tokens, 2 * head), BF16), vm((2 * head, width), BF16), vm((4 * head, width), BF16), vm((tokens, 2 * head), BF16), vm((2 * head, tokens), BF16),
            vm((head, tokens), F32), vm((1, tokens), F32),
            vm((tokens, 2 * head), BF16), vm((tokens, 2 * head), F32),
            vm((hidden, width), F32), vm((hidden, width), F32), vm((head, width), F32), vm((4 * head, width), F32), vm((R, width), F32),
            dma((4, 2, half_ring, 2)), dma((4, 2, half_ring, 2)), dma((4, chips, 2)), dma((4, chips, 2)),
            dma((2, 2, half_ring, 4)), dma((2, 2, half_ring, 4)), dma((2, chips)), dma((2, chips)),
        ]
        grads = pl.pallas_call(
            lambda *refs: layer_kernel(chips, *refs),
            out_shape=outs,
            in_specs=[hbm, hbm, hbm, vmem, vmem, hbm, hbm, hbm, hbm],
            out_specs=(hbm,) * 5,
            scratch_shapes=scratch,
            compiler_params=pltpu.CompilerParams(collective_id=0, has_side_effects=True, vmem_limit_bytes=67043328),
        )(gout_rows, mid_rows, in_rows, ln1_gain[None], ln2_gain[None], wqkv_loc.T, wout_loc, wfc1_loc, wfc2_loc)
        grad_in, grad_wqkvt, grad_wout, grad_wfc1, grad_wfc2 = hand_over(grads)
        return grad_in, grad_wqkvt.T, grad_wout, grad_wfc1, grad_wfc2

    return jax.shard_map(device_step, mesh=mesh, in_specs=in_specs, out_specs=out_specs, check_vma=False)
```

```python
import jax
import jax.numpy as jnp
from jax import lax
from jax.experimental import pallas as pl
from jax.experimental.pallas import tpu as pltpu
from jax.sharding import PartitionSpec as P

LN_EPS = 1e-5
GELU_COEF = 0.044715
GELU_SCALE = 0.7978845608028654
NEG = -1e30
F32 = jnp.float32
BF16 = jnp.bfloat16
MESH = pl.DeviceIdType.MESH
SIGN = (1, -1)
N2, DY, N1, EG = 0, 1, 2, 3


def ln_forward(rows):
    row_mean = jnp.mean(rows, axis=-1, keepdims=True)
    centered = rows - row_mean
    row_rstd = lax.rsqrt(jnp.mean(centered * centered, axis=-1, keepdims=True) + LN_EPS)
    return centered * row_rstd, row_rstd


def ln_backward(x_hat, row_rstd, ln_gain, grad_norm):
    grad_hat = grad_norm * ln_gain
    proj_one = jnp.mean(grad_hat, axis=-1, keepdims=True)
    proj_two = jnp.mean(grad_hat * x_hat, axis=-1, keepdims=True)
    return row_rstd * (grad_hat - proj_one - x_hat * proj_two)


def gelu_pair(pre_act):
    tanh_val = jnp.tanh(GELU_SCALE * (pre_act + GELU_COEF * pre_act * pre_act * pre_act))
    gelu_val = 0.5 * pre_act * (1.0 + tanh_val)
    gelu_der = 0.5 * (1.0 + tanh_val) + 0.5 * pre_act * (1.0 - tanh_val * tanh_val) * GELU_SCALE * (1.0 + 3.0 * GELU_COEF * pre_act * pre_act)
    return gelu_val, gelu_der


def dot_nt(a, b):
    return lax.dot_general(a, b, (((1,), (1,)), ((), ())), preferred_element_type=F32)


def dot_nn(a, b):
    return lax.dot_general(a, b, (((1,), (0,)), ((), ())), preferred_element_type=F32)


def ds_of(index, size):
    return pl.ds(pl.multiple_of(index * size, size), size)


def keep_mask(shape):
    return lax.broadcasted_iota(jnp.int32, shape, 0) <= lax.broadcasted_iota(jnp.int32, shape, 1)


def layer_kernel(chips, g_hbm, h_hbm, x_hbm, gain1_ref, gain2_ref, wqkvt_hbm, wo_hbm, w1_hbm, w2_hbm,
                 dx_hbm, dwqkvt_hbm, dwo_hbm, dw1_hbm, dw2_hbm,
                 g_ref, h_ref, x_ref, wqkvt_ref, wo_ref, w1_ref, w2_ref, dx_ref, dwqkvt_ref, dwo_ref, dw1_ref, dw2_ref, in_sem, out_sem,
                 n2_all, dy_all, n1_all, part, dbuf, rbuf, q_all, wot_pad, wqkvt_pad, kv_all, kvt_all, ot_all, lse_all,
                 dq_all, dkv_acc, dw1t_acc, dw2_acc, dwo_acc, dwqkvt_acc, dh1,
                 ag_send, ag_recv, dd_send, dd_recv, rs_send, rs_recv, dx_send, dx_recv):
    me = lax.axis_index('tp')
    z, c = lax.div(me, 2), lax.rem(me, 2)
    half_ring = chips // 2
    last_u = 2 * half_ring
    R, width = x_hbm.shape
    H = R // 2
    piece = R // 4
    head = dwo_hbm.shape[1]
    pair = 2 * R
    full = (n2_all, dy_all, n1_all, dy_all)

    def chip_at(offset):
        return lax.rem(z + offset + 2 * chips, chips)

    nbr = tuple(2 * chip_at(s) + c for s in SIGN)
    partner = 2 * z + 1 - c

    def half_rows(chip, core, h):
        return ds_of(2 * (2 * chip + core) + h, H)

    def piece_rows(chip, core, q):
        return ds_of(4 * (2 * chip + core) + q, piece)

    def block_rows(block):
        return ds_of(block, R)

    def ag_copy(a, d, s, h, src=None):
        dst = full[a].at[half_rows(chip_at(-SIGN[d] * (s - 1)), c, h)]
        return pltpu.make_async_remote_copy(dst if src is None else src, dst, ag_send.at[a, d, s - 1, h],
                                            ag_recv.at[a, d, s - 1, h], device_id={'tp': nbr[d]}, device_id_type=MESH)

    def ag_arrived(a, d, s, h):
        dst = full[a].at[half_rows(chip_at(-SIGN[d] * s), c, h)]
        pltpu.make_async_remote_copy(dst, dst, ag_send.at[a, d, s - 1, h],
                                     ag_recv.at[a, d, s - 1, h], device_id={'tp': nbr[d]}, device_id_type=MESH).wait_recv()

    def dd_copy(a, j, chip, core, h, src=None):
        dst = full[a].at[half_rows(chip, core, h)]
        return pltpu.make_async_remote_copy(dst if src is None else src, dst, dd_send.at[a, j, h], dd_recv.at[a, j, h],
                                            device_id={'tp': partner}, device_id_type=MESH)

    def slot_of(step, d):
        return jnp.where(step == 0, 0, jnp.minimum(2 * step - 1 + d, chips - 1))

    def chip_of_slot(j):
        away = lax.div(j + 1, 2)
        return chip_at(jnp.where(lax.rem(j, 2) == 1, -away, away))

    def dx_copy(r, j):
        chip = chip_of_slot(j)
        return pltpu.make_async_remote_copy(part.at[block_rows(2 * chip + 1 - c)], dbuf.at[chip], dx_send.at[r, j],
                                            dx_recv.at[r, j], device_id={'tp': partner}, device_id_type=MESH)

    def rs_copy(r, d, s, h):
        src = part.at[piece_rows(chip_at(SIGN[d] * (half_ring - s + 1)), c, h)]
        return pltpu.make_async_remote_copy(src, rbuf.at[d, s - 1, h], rs_send.at[r, d, s - 1, h],
                                            rs_recv.at[r, d, s - 1, h], device_id={'tp': nbr[d]}, device_id_type=MESH)

    def ag_begin(a, src=None, halves=(0, 1)):
        for h in halves:
            part_src = None if src is None else src.at[pl.ds(h * H, H)]
            dd_copy(a, 0, z, c, h, part_src).start()
            for d in (0, 1):
                ag_copy(a, d, 1, h, part_src).start()

    def ag_sent(a):
        for h in (0, 1):
            for d in (0, 1):
                for s in range(1, half_ring + 1):
                    if s < half_ring or h == d:
                        ag_copy(a, d, s, h).wait_send()
            for j in range(chips):
                dd_copy(a, j, chip_of_slot(j), c, h).wait_send()

    def ag_loop(arrays, before, compute, after):
        def body(u, carry):
            step, h = lax.div(u, 2), lax.rem(u, 2)
            s = step + 1

            @pl.when(u < last_u)
            def _():
                for a in arrays:
                    for d in (0, 1):
                        @pl.when((s < half_ring) | (h == d))
                        def _():
                            ag_arrived(a, d, s, h)
                            dd_copy(a, slot_of(s, d), chip_at(-SIGN[d] * s), c, h).start()

                            @pl.when((s < half_ring - 1) | ((s == half_ring - 1) & (h == d)))
                            def _():
                                ag_copy(a, d, s + 1, h).start()
            before(u)

            @pl.when((h == 0) | ((step > 0) & (step < half_ring)))
            def _():
                chip = chip_at((2 * h - 1) * step)
                for a in arrays:
                    for g in (0, 1):
                        dd_copy(a, slot_of(step, h), chip, 1 - c, g).wait_recv()
                compute(chip)
            after(u)
            return carry
        lax.fori_loop(0, last_u + 1, body, 0)

    def rs_first(r, s):
        for d in (0, 1):
            for q in (0, 1):
                rs_copy(r, d, s, (2 * d + q + 2 * (s - 1)) % 4).start()

    def rs_tick(r, k):
        s = 2 + lax.div(k + 2, 4)
        place = lax.rem(k + 2, 4)
        swapped = lax.rem(place + 2, 4)
        rising = jnp.where(place == 3, 3, lax.rem(place + 2, 3))
        order = (jnp.where(s == half_ring, place, jnp.where(s == half_ring - 1, rising, swapped)), place)
        for d in (0, 1):
            q = order[d]
            rs_copy(r, d, s - 1, q).wait_recv()
            rows = piece_rows(chip_at(SIGN[d] * (half_ring - s + 1)), c, q)
            part[rows, :] = (part[rows, :].astype(F32) + rbuf[d, s - 2, q].astype(F32)).astype(BF16)
        for d in (0, 1):
            rs_copy(r, d, s, order[d]).start()

    def rs_ticks(r, u):
        @pl.when(u <= last_u - 3)
        def _():
            rs_tick(r, 2 * u - 2)
            rs_tick(r, 2 * u - 1)

    def rs_last(r, q):
        for d in (0, 1):
            rs_copy(r, d, half_ring, q).wait_recv()
        own = part[piece_rows(z, c, q), :].astype(F32)
        return own + rbuf[0, half_ring - 1, q].astype(F32) + rbuf[1, half_ring - 1, q].astype(F32)

    def rs_sent(r, steps):
        for d in (0, 1):
            for q in range(4):
                for s in steps:
                    if s > 1 or q // 2 == d:
                        rs_copy(r, d, s, q).wait_send()

    def dx_sent(r):
        for j in range(chips):
            dx_copy(r, j).wait_send()

    def join_partner(r, j):
        dx_copy(r, j).wait_recv()
        chip = chip_of_slot(j)
        rows = block_rows(2 * chip + c)
        part[rows, :] = (part[rows, :].astype(F32) + dbuf[chip].astype(F32)).astype(BF16)

    def mlp(chip):
        rows = ds_of(chip, pair)
        n2, dy = n2_all[rows, :], dy_all[rows, :]
        gelu_val, gelu_der = gelu_pair(dot_nn(n2, w1_ref[...]))
        grad_pre = dot_nt(dy, w2_ref[...]) * gelu_der
        dw2_acc[...] += dot_nn(jnp.transpose(gelu_val).astype(BF16), dy)
        dw1t_acc[...] += dot_nn(jnp.transpose(grad_pre).astype(BF16), n2)
        part[rows, :] = dot_nt(grad_pre.astype(BF16), w1_ref[...]).astype(BF16)

    def qkv(chip):
        rows = ds_of(chip, pair)
        cols = dot_nt(n1_all[rows, :], wqkvt_pad[...])
        q_all[rows, :] = cols[:, :2 * head].astype(BF16) * jnp.asarray(head ** -0.5, BF16)
        kv_all[rows, :] = cols[:, 2 * head:].astype(BF16)
        kvt_all[:, rows] = jnp.transpose(cols[:, 2 * head:]).astype(BF16)

    def attend(m):
        rows = ds_of(m, pair)
        queries = q_all[rows, :]

        def tile(t, carry, masked):
            top, total, acc = carry
            keys = ds_of(t, pair)
            s = dot_nt(kv_all[keys, :], queries)
            if masked:
                s = jnp.where(keep_mask(s.shape), s, NEG)
            new_top = jnp.maximum(top, jnp.max(s, axis=0, keepdims=True))
            p = jnp.exp(s - new_top)
            scale = jnp.exp(top - new_top)
            total = total * scale + jnp.sum(p, axis=0, keepdims=True)
            acc = acc * scale + dot_nn(kvt_all[head:, keys], p.astype(BF16))
            return new_top, total, acc

        init = (jnp.full((1, pair), NEG, F32), jnp.zeros((1, pair), F32), jnp.zeros((head, pair), F32))
        top, total, acc = tile(m, lax.fori_loop(0, m, lambda t, k: tile(t, k, False), init), True)
        ot_all[:, rows] = acc / total
        lse_all[:, rows] = top + jnp.log(total)

    def attend_grad(m, h=None):
        rows = (ds_of(m, pair),) if h is None else (half_rows(m, 0, h), half_rows(m, 1, h))
        count = pair if h is None else R
        e_rows = jnp.concatenate([dy_all[k, :] for k in rows], axis=0)
        grads = dot_nt(e_rows, wot_pad[...]).astype(BF16)
        grads_t = jnp.transpose(grads.astype(F32))[head:]
        out_t = jnp.concatenate([ot_all[:, k] for k in rows], axis=1)
        row_dot = jnp.sum(grads_t * out_t, axis=0, keepdims=True)
        both = jnp.concatenate([q_all[k, :] for k in rows] + [grads], axis=0)
        lse = jnp.concatenate([lse_all[:, k] for k in rows], axis=1)

        def tile(t, dqt, masked, size=pair):
            keys = ds_of(t, size)
            sr = dot_nt(kv_all[keys, :], both)
            p = jnp.exp(sr[:, :count] - lse)
            if masked:
                query = lax.broadcasted_iota(jnp.int32, p.shape, 1)
                if h is not None:
                    query = jnp.where(query < H, query, query + H) + h * H
                p = jnp.where(lax.broadcasted_iota(jnp.int32, p.shape, 0) <= query, p, 0.0)
            ds = (p * (sr[:, count:] - row_dot)).astype(BF16)
            dkv_acc[keys, :] += dot_nn(jnp.concatenate([ds, p.astype(BF16)], axis=1), both)
            return dqt + dot_nn(kvt_all[:head, keys], ds)

        dqt = jnp.zeros((head, count), F32)
        done = 0
        if h is not None:
            twos = lax.div(m, 2)
            dqt = lax.fori_loop(0, twos, lambda t, k: tile(t, k, False, 2 * pair), dqt)
            done = 2 * twos
        dqt = lax.fori_loop(done, m, lambda t, k: tile(t, k, False), dqt)
        dqt = tile(m, dqt, True) * (head ** -0.5)
        dq = jnp.transpose(jnp.concatenate([dqt, jnp.zeros_like(dqt)], axis=0)).astype(BF16)
        for k, place in enumerate(rows):
            dq_all[place, :] = dq[k * H:(k + 1) * H] if len(rows) > 1 else dq

    def grad_cols(rows):
        return jnp.concatenate([dq_all[rows, :], dkv_acc[rows, :].astype(BF16)], axis=1)

    loads = [pltpu.make_async_copy(src, dst, in_sem.at[k]) for k, (src, dst) in enumerate((
        (g_hbm, g_ref), (h_hbm, h_ref), (x_hbm, x_ref), (w1_hbm, w1_ref), (w2_hbm, w2_ref), (wqkvt_hbm, wqkvt_ref), (wo_hbm, wo_ref)))]
    barrier = pltpu.get_barrier_semaphore()
    for peer in nbr + (partner,):
        pl.semaphore_signal(barrier, inc=1, device_id={'tp': peer}, device_id_type=MESH)
    for load in loads:
        load.start()
    pl.semaphore_wait(barrier, 3)
    loads[0].wait()
    ag_begin(DY, g_ref)
    loads[1].wait()
    loads[2].wait()

    def norm_rows(k, carry):
        src = ds_of(k, piece)
        dst = ds_of((2 * z + c) * 4 + k, piece)
        for raw, gain, out in ((h_ref, gain2_ref, n2_all), (x_ref, gain1_ref, n1_all)):
            out[dst, :] = (ln_forward(raw[src, :].astype(F32))[0] * gain[...]).astype(BF16)
        dy_all[dst, :] = g_ref[src, :]
        return carry
    lax.fori_loop(0, 4, norm_rows, 0)
    for acc in (dw1t_acc, dw2_acc):
        acc[...] = jnp.zeros_like(acc)
    ag_begin(N2)
    for load in loads[3:]:
        load.wait()
    wot_pad[:head, :] = jnp.zeros((head, width), BF16)
    wot_pad[head:, :] = wo_ref[0]
    wqkvt_pad[:head, :] = wqkvt_ref[:head, :]
    wqkvt_pad[head:2 * head, :] = jnp.zeros((head, width), BF16)
    wqkvt_pad[2 * head:, :] = wqkvt_ref[head:, :]
    for acc in (dwo_acc, dwqkvt_acc, dkv_acc):
        acc[...] = jnp.zeros_like(acc)

    def send_partner(u):
        step, sub = lax.div(u - 1, 2), lax.rem(u - 1, 2)

        @pl.when((u > 0) & ((sub == 0) | (step > 0)))
        def _():
            dx_copy(0, slot_of(step, sub)).start()

    def begin_n1(u):
        @pl.when(u == last_u - 3)
        def _():
            ag_begin(N1)

    ag_loop((DY, N2), send_partner, mlp, begin_n1)

    dx_pending = slot_of(half_ring, 0)

    def join_first(u):
        @pl.when(u == 0)
        def _():
            dx_copy(0, dx_pending).start()

        @pl.when((u > 0) & (u <= chips))
        def _():
            join_partner(0, chips - u)

    def begin_rs(u):
        @pl.when(u == last_u - 3)
        def _():
            ag_sent(N2)
            ag_sent(DY)
            rs_first(0, 1)
            rs_first(0, 2)

    ag_loop((N1,), join_first, qkv, begin_rs)

    def forward_chip(u, carry):
        rs_ticks(0, u)
        attend(chips - u)
        return carry
    lax.fori_loop(1, chips + 1, forward_chip, 0)

    def middle_piece(q, carry):
        rows = ds_of(q, piece)
        mid_hat, mid_rstd = ln_forward(h_ref[rows, :].astype(F32))
        grad = g_ref[rows, :].astype(F32) + ln_backward(mid_hat, mid_rstd, gain2_ref[...], rs_last(0, q))
        dh1[rows, :] = grad
        dy_all[piece_rows(z, c, q), :] = grad.astype(BF16)
        for h in (0, 1):
            @pl.when(q == 2 * h + 1)
            def _():
                ag_begin(EG, halves=(h,))
        return carry
    lax.fori_loop(0, 4, middle_piece, 0)
    rs_sent(0, range(1, half_ring + 1))
    dx_sent(0)

    def e_tick(v):
        s, h = 1 + lax.div(v, 2), lax.rem(v, 2)
        for d in (0, 1):
            g = jnp.where(s == half_ring, d, h)
            ag_arrived(EG, d, s, g)
            dd_copy(EG, slot_of(s, d), chip_at(-SIGN[d] * s), c, g).start()

            @pl.when((s < half_ring - 1) | ((s == half_ring - 1) & (h == d)))
            def _():
                ag_copy(EG, d, s + 1, h).start()

    def backward_call(x, carry):
        @pl.when((lax.rem(x, 2) == 1) & (x < 2 * last_u - 3))
        def _():
            e_tick(lax.div(x - 1, 2))

        unit, side = lax.div(jnp.maximum(x - 2, 0), 2), lax.rem(x, 2)
        step = jnp.where(x < 2, 0, 1 + lax.div(unit, 2))
        g = jnp.where(x < 2, side, lax.rem(unit, 2))
        side = jnp.where(x < 2, 0, side)
        chip = chip_at((2 * side - 1) * step)
        dd_copy(EG, slot_of(step, side), chip, 1 - c, g).wait_recv()
        attend_grad(chip, g)
        return carry
    lax.fori_loop(0, 2 * last_u - 2, backward_call, 0)
    e_tick(jnp.int32(last_u - 2))
    last_chip = chip_at(half_ring)
    for g in (0, 1):
        dd_copy(EG, chips - 1, last_chip, 1 - c, g).wait_recv()
    attend_grad(last_chip)

    def share(k, carry):
        j = chips - 1 - k
        chip = chip_of_slot(j)
        for core in (1 - c, c):
            rows = block_rows(2 * chip + core)
            part[rows, :] = dot_nn(grad_cols(rows), wqkvt_pad[...]).astype(BF16)
        dx_copy(1, j).start()

        @pl.when(k > 0)
        def _():
            join_partner(1, j + 1)

        for first in (1, 2):
            @pl.when(k == 2 * first - 1)
            def _():
                rs_first(1, first)
        return carry
    lax.fori_loop(0, chips, share, 0)
    join_partner(1, 0)

    def weight_block(u, carry):
        rs_ticks(1, u)
        rows = ds_of(u - 1, pair)
        cols_t = jnp.transpose(grad_cols(rows).astype(F32)).astype(BF16)
        dwqkvt_acc[...] += dot_nn(cols_t, n1_all[rows, :])
        dwo_acc[...] += dot_nn(ot_all[:, rows].astype(BF16), dy_all[rows, :])
        return carry
    lax.fori_loop(1, chips + 1, weight_block, 0)

    dw2_ref[...] = dw2_acc[...].astype(BF16)
    dw1_ref[...] = jnp.transpose(dw1t_acc[...]).astype(BF16)
    dwo_ref[0] = dwo_acc[...].astype(BF16)
    dwqkvt_ref[:head, :] = dwqkvt_acc[:head, :].astype(BF16)
    dwqkvt_ref[head:, :] = dwqkvt_acc[2 * head:, :].astype(BF16)
    ag_sent(N1)
    ag_sent(EG)
    stores = [pltpu.make_async_copy(src, dst, out_sem.at[k]) for k, (src, dst) in enumerate((
        (dw2_ref, dw2_hbm), (dw1_ref, dw1_hbm), (dwo_ref, dwo_hbm), (dwqkvt_ref, dwqkvt_hbm)))]
    for store in stores:
        store.start()
    dx_sent(1)
    rs_sent(1, range(1, half_ring))
    for store in stores:
        store.wait()

    def dx_store(q):
        rows = pl.ds(q * piece, piece)
        return pltpu.make_async_copy(dx_ref.at[rows], dx_hbm.at[rows], out_sem.at[4 + q])

    def final_piece(q, carry):
        rows = ds_of(q, piece)
        in_hat, in_rstd = ln_forward(x_ref[rows, :].astype(F32))
        dx_ref[rows, :] = (dh1[rows, :] + ln_backward(in_hat, in_rstd, gain1_ref[...], rs_last(1, q))).astype(BF16)

        @pl.when(q > 0)
        def _():
            dx_store(q - 1).start()
        return carry
    lax.fori_loop(0, 4, final_piece, 0)
    rs_sent(1, (half_ring,))
    dx_store(3).start()
    for q in range(4):
        dx_store(q).wait()


def hand_over(arrays):
    count = len(arrays)

    def kernel(*refs):
        ins, outs, held, sems = refs[:count], refs[count:2 * count], refs[2 * count:3 * count], refs[3 * count]
        moves = []
        for k in range(count):
            axis = len(arrays[k].shape) - 2
            size = arrays[k].shape[axis] // 2
            for h in (0, 1):
                at = (slice(None),) * axis + (pl.ds(h * size, size),)
                moves.append((pltpu.make_async_copy(ins[k].at[at], held[k].at[at], sems.at[0, k, h]),
                              pltpu.make_async_copy(held[k].at[at], outs[k].at[at], sems.at[1, k, h])))
        for read, _ in moves:
            read.start()
        for read, write in moves:
            read.wait()
            write.start()
        for _, write in moves:
            write.wait()

    return pl.pallas_call(
        kernel,
        out_shape=tuple(jax.ShapeDtypeStruct(a.shape, a.dtype) for a in arrays),
        in_specs=[pl.BlockSpec(memory_space=pl.ANY)] * count,
        out_specs=tuple([pl.BlockSpec(memory_space=pl.ANY)] * count),
        scratch_shapes=[pltpu.VMEM(a.shape, a.dtype) for a in arrays] + [pltpu.SemaphoreType.DMA((2, count, 2))],
    )(*arrays)


def solution(mesh):
    chips = mesh.shape['tp'] // 2
    row_spec = P(('dp', 'tp'), None)
    in_specs = (row_spec, row_spec, row_spec, P(None), P(None), P(None, 'tp'), P('tp', None, None), P(None, 'tp'), P('tp', None))
    out_specs = (row_spec, P('dp', 'tp'), P(('dp', 'tp'), None, None), P('dp', 'tp'), P(('dp', 'tp'), None))

    def device_step(in_rows, mid_rows, gout_rows, ln1_gain, ln2_gain, wqkv_loc, wout_loc, wfc1_loc, wfc2_loc):
        R, width = in_rows.shape
        head = wout_loc.shape[1]
        hidden = wfc1_loc.shape[1]
        tokens = 2 * chips * R
        half_ring = chips // 2
        vm = pltpu.VMEM
        hbm = pl.BlockSpec(memory_space=pl.ANY)
        vmem = pl.BlockSpec(memory_space=pltpu.VMEM)
        dma = pltpu.SemaphoreType.DMA
        outs = (
            jax.ShapeDtypeStruct((R, width), BF16), jax.ShapeDtypeStruct((3 * head, width), BF16),
            jax.ShapeDtypeStruct((1, head, width), BF16), jax.ShapeDtypeStruct((width, hidden), BF16),
            jax.ShapeDtypeStruct((hidden, width), BF16))
        wide = (in_rows, in_rows, in_rows, outs[1], wout_loc, wfc1_loc, wfc2_loc) + outs
        scratch = [vm(a.shape, BF16) for a in wide] + [dma((7,)), dma((8,))] + [
            vm((tokens, width), BF16), vm((tokens, width), BF16), vm((tokens, width), BF16), vm((tokens, width), BF16),
            vm((chips, R, width), BF16), vm((2, half_ring, 4, R // 4, width), BF16),
            vm((tokens, 2 * head), BF16), vm((2 * head, width), BF16), vm((4 * head, width), BF16), vm((tokens, 2 * head), BF16), vm((2 * head, tokens), BF16),
            vm((head, tokens), F32), vm((1, tokens), F32),
            vm((tokens, 2 * head), BF16), vm((tokens, 2 * head), F32),
            vm((hidden, width), F32), vm((hidden, width), F32), vm((head, width), F32), vm((4 * head, width), F32), vm((R, width), F32),
            dma((4, 2, half_ring, 2)), dma((4, 2, half_ring, 2)), dma((4, chips, 2)), dma((4, chips, 2)),
            dma((2, 2, half_ring, 4)), dma((2, 2, half_ring, 4)), dma((2, chips)), dma((2, chips)),
        ]
        grads = pl.pallas_call(
            lambda *refs: layer_kernel(chips, *refs),
            out_shape=outs,
            in_specs=[hbm, hbm, hbm, vmem, vmem, hbm, hbm, hbm, hbm],
            out_specs=(hbm,) * 5,
            scratch_shapes=scratch,
            compiler_params=pltpu.CompilerParams(collective_id=0, has_side_effects=True, vmem_limit_bytes=67043328),
        )(gout_rows, mid_rows, in_rows, ln1_gain[None], ln2_gain[None], wqkv_loc.T, wout_loc, wfc1_loc, wfc2_loc)
        grad_in, grad_wqkvt, grad_wout, grad_wfc1, grad_wfc2 = hand_over(grads)
        return grad_in, grad_wqkvt.T, grad_wout, grad_wfc1, grad_wfc2

    return jax.shard_map(device_step, mesh=mesh, in_specs=in_specs, out_specs=out_specs, check_vma=False)
```

```python
import jax
import jax.numpy as jnp
from jax import lax
from jax.experimental import pallas as pl
from jax.experimental.pallas import tpu as pltpu
from jax.sharding import PartitionSpec as P

LN_EPS = 1e-5
GELU_COEF = 0.044715
GELU_SCALE = 0.7978845608028654
NEG = -1e30
F32 = jnp.float32
BF16 = jnp.bfloat16
MESH = pl.DeviceIdType.MESH
SIGN = (1, -1)
N2, DY, N1, EG = 0, 1, 2, 3


def ln_forward(rows):
    row_mean = jnp.mean(rows, axis=-1, keepdims=True)
    centered = rows - row_mean
    row_rstd = lax.rsqrt(jnp.mean(centered * centered, axis=-1, keepdims=True) + LN_EPS)
    return centered * row_rstd, row_rstd


def ln_backward(x_hat, row_rstd, ln_gain, grad_norm):
    grad_hat = grad_norm * ln_gain
    proj_one = jnp.mean(grad_hat, axis=-1, keepdims=True)
    proj_two = jnp.mean(grad_hat * x_hat, axis=-1, keepdims=True)
    return row_rstd * (grad_hat - proj_one - x_hat * proj_two)


def gelu_pair(pre_act):
    tanh_val = jnp.tanh(GELU_SCALE * (pre_act + GELU_COEF * pre_act * pre_act * pre_act))
    gelu_val = 0.5 * pre_act * (1.0 + tanh_val)
    gelu_der = 0.5 * (1.0 + tanh_val) + 0.5 * pre_act * (1.0 - tanh_val * tanh_val) * GELU_SCALE * (1.0 + 3.0 * GELU_COEF * pre_act * pre_act)
    return gelu_val, gelu_der


def dot_nt(a, b):
    return lax.dot_general(a, b, (((1,), (1,)), ((), ())), preferred_element_type=F32)


def dot_nn(a, b):
    return lax.dot_general(a, b, (((1,), (0,)), ((), ())), preferred_element_type=F32)


def ds_of(index, size):
    return pl.ds(pl.multiple_of(index * size, size), size)


def keep_mask(shape):
    return lax.broadcasted_iota(jnp.int32, shape, 0) <= lax.broadcasted_iota(jnp.int32, shape, 1)


def layer_kernel(chips, g_hbm, h_hbm, x_hbm, gain1_ref, gain2_ref, wqkvt_hbm, wo_hbm, w1_hbm, w2_hbm,
                 dx_hbm, dwqkvt_hbm, dwo_hbm, dw1_hbm, dw2_hbm,
                 g_ref, h_ref, x_ref, wqkvt_ref, wo_ref, w1_ref, w2_ref, dx_ref, dwqkvt_ref, dwo_ref, dw1_ref, dw2_ref, in_sem, out_sem,
                 n2_all, dy_all, n1_all, part, dbuf, rbuf, q_all, wot_pad, wqkvt_pad, kv_all, kvt_all, ot_all, lse_all,
                 dq_all, dkv_acc, dw1t_acc, dw2_acc, dwo_acc, dwqkvt_acc, dh1,
                 ag_send, ag_recv, dd_send, dd_recv, rs_send, rs_recv, dx_send, dx_recv):
    me = lax.axis_index('tp')
    z, c = lax.div(me, 2), lax.rem(me, 2)
    half_ring = chips // 2
    last_u = 2 * half_ring
    R, width = x_hbm.shape
    H = R // 2
    piece = R // 4
    head = dwo_hbm.shape[1]
    pair = 2 * R
    full = (n2_all, dy_all, n1_all, dy_all)

    def chip_at(offset):
        return lax.rem(z + offset + 2 * chips, chips)

    nbr = tuple(2 * chip_at(s) + c for s in SIGN)
    partner = 2 * z + 1 - c

    def half_rows(chip, core, h):
        return ds_of(2 * (2 * chip + core) + h, H)

    def piece_rows(chip, core, q):
        return ds_of(4 * (2 * chip + core) + q, piece)

    def block_rows(block):
        return ds_of(block, R)

    def ag_copy(a, d, s, h, src=None):
        dst = full[a].at[half_rows(chip_at(-SIGN[d] * (s - 1)), c, h)]
        return pltpu.make_async_remote_copy(dst if src is None else src, dst, ag_send.at[a, d, s - 1, h],
                                            ag_recv.at[a, d, s - 1, h], device_id={'tp': nbr[d]}, device_id_type=MESH)

    def ag_arrived(a, d, s, h):
        dst = full[a].at[half_rows(chip_at(-SIGN[d] * s), c, h)]
        pltpu.make_async_remote_copy(dst, dst, ag_send.at[a, d, s - 1, h],
                                     ag_recv.at[a, d, s - 1, h], device_id={'tp': nbr[d]}, device_id_type=MESH).wait_recv()

    def dd_copy(a, j, chip, core, h, src=None):
        dst = full[a].at[half_rows(chip, core, h)]
        return pltpu.make_async_remote_copy(dst if src is None else src, dst, dd_send.at[a, j, h], dd_recv.at[a, j, h],
                                            device_id={'tp': partner}, device_id_type=MESH)

    def slot_of(step, d):
        return jnp.where(step == 0, 0, jnp.minimum(2 * step - 1 + d, chips - 1))

    def chip_of_slot(j):
        away = lax.div(j + 1, 2)
        return chip_at(jnp.where(lax.rem(j, 2) == 1, -away, away))

    def dx_copy(r, j):
        chip = chip_of_slot(j)
        return pltpu.make_async_remote_copy(part.at[block_rows(2 * chip + 1 - c)], dbuf.at[chip], dx_send.at[r, j],
                                            dx_recv.at[r, j], device_id={'tp': partner}, device_id_type=MESH)

    def rs_copy(r, d, s, h):
        src = part.at[piece_rows(chip_at(SIGN[d] * (half_ring - s + 1)), c, h)]
        return pltpu.make_async_remote_copy(src, rbuf.at[d, s - 1, h], rs_send.at[r, d, s - 1, h],
                                            rs_recv.at[r, d, s - 1, h], device_id={'tp': nbr[d]}, device_id_type=MESH)

    def ag_begin(a, src=None, halves=(0, 1)):
        for h in halves:
            part_src = None if src is None else src.at[pl.ds(h * H, H)]
            dd_copy(a, 0, z, c, h, part_src).start()
            for d in (0, 1):
                ag_copy(a, d, 1, h, part_src).start()

    def ag_sent(a):
        for h in (0, 1):
            for d in (0, 1):
                for s in range(1, half_ring + 1):
                    if s < half_ring or h == d:
                        ag_copy(a, d, s, h).wait_send()
            for j in range(chips):
                dd_copy(a, j, chip_of_slot(j), c, h).wait_send()

    def ag_loop(arrays, before, compute, after):
        def body(u, carry):
            step, h = lax.div(u, 2), lax.rem(u, 2)
            s = step + 1

            @pl.when(u < last_u)
            def _():
                for a in arrays:
                    for d in (0, 1):
                        @pl.when((s < half_ring) | (h == d))
                        def _():
                            ag_arrived(a, d, s, h)
                            dd_copy(a, slot_of(s, d), chip_at(-SIGN[d] * s), c, h).start()

                            @pl.when((s < half_ring - 1) | ((s == half_ring - 1) & (h == d)))
                            def _():
                                ag_copy(a, d, s + 1, h).start()
            before(u)

            @pl.when((h == 0) | ((step > 0) & (step < half_ring)))
            def _():
                chip = chip_at((2 * h - 1) * step)
                for a in arrays:
                    for g in (0, 1):
                        dd_copy(a, slot_of(step, h), chip, 1 - c, g).wait_recv()
                compute(chip)
            after(u)
            return carry
        lax.fori_loop(0, last_u + 1, body, 0)

    def rs_first(r, s):
        for d in (0, 1):
            for q in (0, 1):
                rs_copy(r, d, s, (2 * d + q + 2 * (s - 1)) % 4).start()

    def rs_tick(r, k):
        s = 2 + lax.div(k + 2, 4)
        place = lax.rem(k + 2, 4)
        swapped = lax.rem(place + 2, 4)
        rising = jnp.where(place == 3, 3, lax.rem(place + 2, 3))
        order = (jnp.where(s == half_ring, place, jnp.where(s == half_ring - 1, rising, swapped)), place)
        for d in (0, 1):
            q = order[d]
            rs_copy(r, d, s - 1, q).wait_recv()
            rows = piece_rows(chip_at(SIGN[d] * (half_ring - s + 1)), c, q)
            part[rows, :] = (part[rows, :].astype(F32) + rbuf[d, s - 2, q].astype(F32)).astype(BF16)
        for d in (0, 1):
            rs_copy(r, d, s, order[d]).start()

    def rs_ticks(r, u):
        @pl.when(u <= last_u - 3)
        def _():
            rs_tick(r, 2 * u - 2)
            rs_tick(r, 2 * u - 1)

    def rs_last(r, q):
        for d in (0, 1):
            rs_copy(r, d, half_ring, q).wait_recv()
        own = part[piece_rows(z, c, q), :].astype(F32)
        return own + rbuf[0, half_ring - 1, q].astype(F32) + rbuf[1, half_ring - 1, q].astype(F32)

    def rs_sent(r, steps):
        for d in (0, 1):
            for q in range(4):
                for s in steps:
                    if s > 1 or q // 2 == d:
                        rs_copy(r, d, s, q).wait_send()

    def dx_sent(r):
        for j in range(chips):
            dx_copy(r, j).wait_send()

    def join_partner(r, j):
        dx_copy(r, j).wait_recv()
        chip = chip_of_slot(j)
        rows = block_rows(2 * chip + c)
        part[rows, :] = (part[rows, :].astype(F32) + dbuf[chip].astype(F32)).astype(BF16)

    def mlp(chip):
        rows = ds_of(chip, pair)
        n2, dy = n2_all[rows, :], dy_all[rows, :]
        gelu_val, gelu_der = gelu_pair(dot_nn(n2, w1_ref[...]))
        grad_pre = dot_nt(dy, w2_ref[...]) * gelu_der
        dw2_acc[...] += dot_nn(jnp.transpose(gelu_val).astype(BF16), dy)
        dw1t_acc[...] += dot_nn(jnp.transpose(grad_pre).astype(BF16), n2)
        part[rows, :] = dot_nt(grad_pre.astype(BF16), w1_ref[...]).astype(BF16)

    def qkv(chip):
        rows = ds_of(chip, pair)
        cols = dot_nt(n1_all[rows, :], wqkvt_pad[...])
        q_all[rows, :] = cols[:, :2 * head].astype(BF16) * jnp.asarray(head ** -0.5, BF16)
        kv_all[rows, :] = cols[:, 2 * head:].astype(BF16)
        kvt_all[:, rows] = jnp.transpose(cols[:, 2 * head:]).astype(BF16)

    def attend(m):
        rows = ds_of(m, pair)
        queries = q_all[rows, :]

        def tile(t, carry, masked):
            top, total, acc = carry
            keys = ds_of(t, pair)
            s = dot_nt(kv_all[keys, :], queries)
            if masked:
                s = jnp.where(keep_mask(s.shape), s, NEG)
            new_top = jnp.maximum(top, jnp.max(s, axis=0, keepdims=True))
            p = jnp.exp(s - new_top)
            scale = jnp.exp(top - new_top)
            total = total * scale + jnp.sum(p, axis=0, keepdims=True)
            acc = acc * scale + dot_nn(kvt_all[head:, keys], p.astype(BF16))
            return new_top, total, acc

        init = (jnp.full((1, pair), NEG, F32), jnp.zeros((1, pair), F32), jnp.zeros((head, pair), F32))
        top, total, acc = tile(m, lax.fori_loop(0, m, lambda t, k: tile(t, k, False), init), True)
        ot_all[:, rows] = acc / total
        lse_all[:, rows] = top + jnp.log(total)

    def attend_grad(m, h=None):
        rows = (ds_of(m, pair),) if h is None else (half_rows(m, 0, h), half_rows(m, 1, h))
        count = pair if h is None else R
        e_rows = jnp.concatenate([dy_all[k, :] for k in rows], axis=0)
        grads = dot_nt(e_rows, wot_pad[...]).astype(BF16)
        grads_t = jnp.transpose(grads.astype(F32))[head:]
        out_t = jnp.concatenate([ot_all[:, k] for k in rows], axis=1)
        row_dot = jnp.sum(grads_t * out_t, axis=0, keepdims=True)
        both = jnp.concatenate([q_all[k, :] for k in rows] + [grads], axis=0)
        lse = jnp.concatenate([lse_all[:, k] for k in rows], axis=1)

        def tile(t, dqt, masked, size=pair):
            keys = ds_of(t, size)
            sr = dot_nt(kv_all[keys, :], both)
            p = jnp.exp(sr[:, :count] - lse)
            if masked:
                query = lax.broadcasted_iota(jnp.int32, p.shape, 1)
                if h is not None:
                    query = jnp.where(query < H, query, query + H) + h * H
                p = jnp.where(lax.broadcasted_iota(jnp.int32, p.shape, 0) <= query, p, 0.0)
            ds = (p * (sr[:, count:] - row_dot)).astype(BF16)
            dkv_acc[keys, :] += dot_nn(jnp.concatenate([ds, p.astype(BF16)], axis=1), both)
            return dqt + dot_nn(kvt_all[:head, keys], ds)

        dqt = jnp.zeros((head, count), F32)
        done = 0
        if h is not None:
            twos = lax.div(m, 2)
            dqt = lax.fori_loop(0, twos, lambda t, k: tile(t, k, False, 2 * pair), dqt)
            done = 2 * twos
        dqt = lax.fori_loop(done, m, lambda t, k: tile(t, k, False), dqt)
        dqt = tile(m, dqt, True) * (head ** -0.5)
        dq = jnp.transpose(jnp.concatenate([dqt, jnp.zeros_like(dqt)], axis=0)).astype(BF16)
        for k, place in enumerate(rows):
            dq_all[place, :] = dq[k * H:(k + 1) * H] if len(rows) > 1 else dq

    def grad_cols(rows):
        return jnp.concatenate([dq_all[rows, :], dkv_acc[rows, :].astype(BF16)], axis=1)

    loads = [pltpu.make_async_copy(src, dst, in_sem.at[k]) for k, (src, dst) in enumerate((
        (g_hbm, g_ref), (h_hbm, h_ref), (x_hbm, x_ref), (w1_hbm, w1_ref), (w2_hbm, w2_ref), (wqkvt_hbm, wqkvt_ref), (wo_hbm, wo_ref)))]
    barrier = pltpu.get_barrier_semaphore()
    for peer in nbr + (partner,):
        pl.semaphore_signal(barrier, inc=1, device_id={'tp': peer}, device_id_type=MESH)
    for load in loads:
        load.start()
    pl.semaphore_wait(barrier, 3)
    loads[0].wait()
    ag_begin(DY, g_ref)
    loads[1].wait()
    loads[2].wait()

    def norm_rows(k, carry):
        src = ds_of(k, piece)
        dst = ds_of((2 * z + c) * 4 + k, piece)
        for raw, gain, out in ((h_ref, gain2_ref, n2_all), (x_ref, gain1_ref, n1_all)):
            out[dst, :] = (ln_forward(raw[src, :].astype(F32))[0] * gain[...]).astype(BF16)
        dy_all[dst, :] = g_ref[src, :]
        return carry
    lax.fori_loop(0, 4, norm_rows, 0)
    for acc in (dw1t_acc, dw2_acc):
        acc[...] = jnp.zeros_like(acc)
    ag_begin(N2)
    for load in loads[3:]:
        load.wait()
    wot_pad[:head, :] = jnp.zeros((head, width), BF16)
    wot_pad[head:, :] = wo_ref[0]
    wqkvt_pad[:head, :] = wqkvt_ref[:head, :]
    wqkvt_pad[head:2 * head, :] = jnp.zeros((head, width), BF16)
    wqkvt_pad[2 * head:, :] = wqkvt_ref[head:, :]
    for acc in (dwo_acc, dwqkvt_acc, dkv_acc):
        acc[...] = jnp.zeros_like(acc)

    def send_partner(u):
        step, sub = lax.div(u - 1, 2), lax.rem(u - 1, 2)

        @pl.when((u > 0) & ((sub == 0) | (step > 0)))
        def _():
            dx_copy(0, slot_of(step, sub)).start()

    def begin_n1(u):
        @pl.when(u == last_u - 3)
        def _():
            ag_begin(N1)

    ag_loop((DY, N2), send_partner, mlp, begin_n1)

    dx_pending = slot_of(half_ring, 0)

    def join_first(u):
        @pl.when(u == 0)
        def _():
            dx_copy(0, dx_pending).start()

        @pl.when((u > 0) & (u <= chips))
        def _():
            join_partner(0, chips - u)

    def begin_rs(u):
        @pl.when(u == last_u - 3)
        def _():
            ag_sent(N2)
            ag_sent(DY)
            rs_first(0, 1)
            rs_first(0, 2)

    ag_loop((N1,), join_first, qkv, begin_rs)

    def forward_chip(u, carry):
        rs_ticks(0, u)
        attend(chips - u)
        return carry
    lax.fori_loop(1, chips + 1, forward_chip, 0)

    def middle_piece(q, carry):
        rows = ds_of(q, piece)
        mid_hat, mid_rstd = ln_forward(h_ref[rows, :].astype(F32))
        grad = g_ref[rows, :].astype(F32) + ln_backward(mid_hat, mid_rstd, gain2_ref[...], rs_last(0, q))
        dh1[rows, :] = grad
        dy_all[piece_rows(z, c, q), :] = grad.astype(BF16)
        for h in (0, 1):
            @pl.when(q == 2 * h + 1)
            def _():
                ag_begin(EG, halves=(h,))
        return carry
    lax.fori_loop(0, 4, middle_piece, 0)
    rs_sent(0, range(1, half_ring + 1))
    dx_sent(0)

    def e_tick(v):
        s, h = 1 + lax.div(v, 2), lax.rem(v, 2)
        for d in (0, 1):
            g = jnp.where(s == half_ring, d, h)
            ag_arrived(EG, d, s, g)
            dd_copy(EG, slot_of(s, d), chip_at(-SIGN[d] * s), c, g).start()

            @pl.when((s < half_ring - 1) | ((s == half_ring - 1) & (h == d)))
            def _():
                ag_copy(EG, d, s + 1, h).start()

    def backward_call(x, carry):
        late = 2 * last_u - 6

        @pl.when(((lax.rem(x, 2) == 1) & (x < 2 * last_u - 3) & (x != late - 1)) | (x == late))
        def _():
            e_tick(lax.div(x - 1, 2))

        unit, side = lax.div(jnp.maximum(x - 2, 0), 2), lax.rem(x, 2)
        step = jnp.where(x < 2, 0, 1 + lax.div(unit, 2))
        g = jnp.where(x < 2, side, lax.rem(unit, 2))
        side = jnp.where(x < 2, 0, side)
        chip = chip_at((2 * side - 1) * step)
        dd_copy(EG, slot_of(step, side), chip, 1 - c, g).wait_recv()
        attend_grad(chip, g)
        return carry
    lax.fori_loop(0, 2 * last_u - 2, backward_call, 0)
    e_tick(jnp.int32(last_u - 2))
    last_chip = chip_at(half_ring)
    for g in (0, 1):
        dd_copy(EG, chips - 1, last_chip, 1 - c, g).wait_recv()
    attend_grad(last_chip)

    def share(k, carry):
        j = chips - 1 - k
        chip = chip_of_slot(j)
        for core in (1 - c, c):
            rows = block_rows(2 * chip + core)
            part[rows, :] = dot_nn(grad_cols(rows), wqkvt_pad[...]).astype(BF16)
        dx_copy(1, j).start()

        @pl.when(k > 0)
        def _():
            join_partner(1, j + 1)

        for first in (1, 2):
            @pl.when(k == 2 * first - 1)
            def _():
                rs_first(1, first)
        return carry
    lax.fori_loop(0, chips, share, 0)
    join_partner(1, 0)

    def weight_block(u, carry):
        rs_ticks(1, u)
        rows = ds_of(u - 1, pair)
        cols_t = jnp.transpose(grad_cols(rows).astype(F32)).astype(BF16)
        dwqkvt_acc[...] += dot_nn(cols_t, n1_all[rows, :])
        dwo_acc[...] += dot_nn(ot_all[:, rows].astype(BF16), dy_all[rows, :])
        return carry
    lax.fori_loop(1, chips + 1, weight_block, 0)

    dw2_ref[...] = dw2_acc[...].astype(BF16)
    dw1_ref[...] = jnp.transpose(dw1t_acc[...]).astype(BF16)
    dwo_ref[0] = dwo_acc[...].astype(BF16)
    dwqkvt_ref[:head, :] = dwqkvt_acc[:head, :].astype(BF16)
    dwqkvt_ref[head:, :] = dwqkvt_acc[2 * head:, :].astype(BF16)
    ag_sent(N1)
    ag_sent(EG)
    stores = [pltpu.make_async_copy(src, dst, out_sem.at[k]) for k, (src, dst) in enumerate((
        (dw2_ref, dw2_hbm), (dw1_ref, dw1_hbm), (dwo_ref, dwo_hbm), (dwqkvt_ref, dwqkvt_hbm)))]
    for store in stores:
        store.start()
    dx_sent(1)
    rs_sent(1, range(1, half_ring))
    for store in stores:
        store.wait()

    def dx_store(q):
        rows = pl.ds(q * piece, piece)
        return pltpu.make_async_copy(dx_ref.at[rows], dx_hbm.at[rows], out_sem.at[4 + q])

    def final_piece(q, carry):
        rows = ds_of(q, piece)
        in_hat, in_rstd = ln_forward(x_ref[rows, :].astype(F32))
        dx_ref[rows, :] = (dh1[rows, :] + ln_backward(in_hat, in_rstd, gain1_ref[...], rs_last(1, q))).astype(BF16)

        @pl.when(q > 0)
        def _():
            dx_store(q - 1).start()
        return carry
    lax.fori_loop(0, 4, final_piece, 0)
    rs_sent(1, (half_ring,))
    dx_store(3).start()
    for q in range(4):
        dx_store(q).wait()


def hand_over(arrays):
    count = len(arrays)

    def kernel(*refs):
        ins, outs, held, sems = refs[:count], refs[count:2 * count], refs[2 * count:3 * count], refs[3 * count]
        moves = []
        for k in range(count):
            axis = len(arrays[k].shape) - 2
            size = arrays[k].shape[axis] // 2
            for h in (0, 1):
                at = (slice(None),) * axis + (pl.ds(h * size, size),)
                moves.append((pltpu.make_async_copy(ins[k].at[at], held[k].at[at], sems.at[0, k, h]),
                              pltpu.make_async_copy(held[k].at[at], outs[k].at[at], sems.at[1, k, h])))
        for read, _ in moves:
            read.start()
        for read, write in moves:
            read.wait()
            write.start()
        for _, write in moves:
            write.wait()

    return pl.pallas_call(
        kernel,
        out_shape=tuple(jax.ShapeDtypeStruct(a.shape, a.dtype) for a in arrays),
        in_specs=[pl.BlockSpec(memory_space=pl.ANY)] * count,
        out_specs=tuple([pl.BlockSpec(memory_space=pl.ANY)] * count),
        scratch_shapes=[pltpu.VMEM(a.shape, a.dtype) for a in arrays] + [pltpu.SemaphoreType.DMA((2, count, 2))],
    )(*arrays)


def solution(mesh):
    chips = mesh.shape['tp'] // 2
    row_spec = P(('dp', 'tp'), None)
    in_specs = (row_spec, row_spec, row_spec, P(None), P(None), P(None, 'tp'), P('tp', None, None), P(None, 'tp'), P('tp', None))
    out_specs = (row_spec, P('dp', 'tp'), P(('dp', 'tp'), None, None), P('dp', 'tp'), P(('dp', 'tp'), None))

    def device_step(in_rows, mid_rows, gout_rows, ln1_gain, ln2_gain, wqkv_loc, wout_loc, wfc1_loc, wfc2_loc):
        R, width = in_rows.shape
        head = wout_loc.shape[1]
        hidden = wfc1_loc.shape[1]
        tokens = 2 * chips * R
        half_ring = chips // 2
        vm = pltpu.VMEM
        hbm = pl.BlockSpec(memory_space=pl.ANY)
        vmem = pl.BlockSpec(memory_space=pltpu.VMEM)
        dma = pltpu.SemaphoreType.DMA
        outs = (
            jax.ShapeDtypeStruct((R, width), BF16), jax.ShapeDtypeStruct((3 * head, width), BF16),
            jax.ShapeDtypeStruct((1, head, width), BF16), jax.ShapeDtypeStruct((width, hidden), BF16),
            jax.ShapeDtypeStruct((hidden, width), BF16))
        wide = (in_rows, in_rows, in_rows, outs[1], wout_loc, wfc1_loc, wfc2_loc) + outs
        scratch = [vm(a.shape, BF16) for a in wide] + [dma((7,)), dma((8,))] + [
            vm((tokens, width), BF16), vm((tokens, width), BF16), vm((tokens, width), BF16), vm((tokens, width), BF16),
            vm((chips, R, width), BF16), vm((2, half_ring, 4, R // 4, width), BF16),
            vm((tokens, 2 * head), BF16), vm((2 * head, width), BF16), vm((4 * head, width), BF16), vm((tokens, 2 * head), BF16), vm((2 * head, tokens), BF16),
            vm((head, tokens), F32), vm((1, tokens), F32),
            vm((tokens, 2 * head), BF16), vm((tokens, 2 * head), F32),
            vm((hidden, width), F32), vm((hidden, width), F32), vm((head, width), F32), vm((4 * head, width), F32), vm((R, width), F32),
            dma((4, 2, half_ring, 2)), dma((4, 2, half_ring, 2)), dma((4, chips, 2)), dma((4, chips, 2)),
            dma((2, 2, half_ring, 4)), dma((2, 2, half_ring, 4)), dma((2, chips)), dma((2, chips)),
        ]
        grads = pl.pallas_call(
            lambda *refs: layer_kernel(chips, *refs),
            out_shape=outs,
            in_specs=[hbm, hbm, hbm, vmem, vmem, hbm, hbm, hbm, hbm],
            out_specs=(hbm,) * 5,
            scratch_shapes=scratch,
            compiler_params=pltpu.CompilerParams(collective_id=0, has_side_effects=True, vmem_limit_bytes=67043328),
        )(gout_rows, mid_rows, in_rows, ln1_gain[None], ln2_gain[None], wqkv_loc.T, wout_loc, wfc1_loc, wfc2_loc)
        grad_in, grad_wqkvt, grad_wout, grad_wfc1, grad_wfc2 = hand_over(grads)
        return grad_in, grad_wqkvt.T, grad_wout, grad_wfc1, grad_wfc2

    return jax.shard_map(device_step, mesh=mesh, in_specs=in_specs, out_specs=out_specs, check_vma=False)
```
